16 devices in a mesh: data: 2 (over y, z), expert: 8 (over x, core).
Axes of the slice: x: 4, y: 2, z: 1, core: 2. Of those that a mesh axis runs over, the one named last changes fastest.
The devices are a block of a 4x4x8 slice.
Arguments:
- token_rows: bfloat16 [2048, 2048], P(('data', 'expert')), parts along dimension 0
- expert_ids: int32 [2048, 6], P(('data', 'expert')), parts along dimension 0
- gate_weights: float32 [2048, 6], P(('data', 'expert')), parts along dimension 0
- w_in: bfloat16 [64, 2048, 1408], P('expert')
- w_out: bfloat16 [64, 1408, 2048], P('expert')
Outputs:
- output: bfloat16 [2048, 2048], P(('data', 'expert')), parts along dimension 0
There are 2 independent parts. The reference program is written for one: setup_inputs(seed, part) draws one part's arguments, and reference() takes and returns one part's arrays. A program takes and returns all parts, laid end to end along the dimension named above; an argument that names none is the same for every part.
All inputs are finite; a program needn't handle non-finite values.
Results may differ from the reference program's by a relative error of at most 0.001.
Values are sent between devices in bfloat16 or wider.
A program may use at most 768 MiB of HBM per device.

```python
import math
import jax
import jax.numpy as jnp
from jax import lax

TOKENS_DEV = 128
GROUP_DEVS = 8
MODEL_DIM = 2048
HIDDEN_DIM = 1408
EXPERTS = 64
TOP_K = 6

TOKENS = TOKENS_DEV * GROUP_DEVS
MEAN_LOAD = TOKENS_DEV * TOP_K // EXPERTS
CAPACITY = TOKENS * TOP_K // EXPERTS
POP_SPREAD = MEAN_LOAD // 2
DEV_SPREAD = MEAN_LOAD // 4


def draw_routing(key):
    key_order, key_pop, key_dev, key_tok, key_col = jax.random.split(key, 5)
    expert_order = jax.random.permutation(key_order, EXPERTS)
    pop_bias = jax.random.randint(key_pop, (EXPERTS,), 0, POP_SPREAD + 1)
    pop_bias = pop_bias.at[0].set(POP_SPREAD).at[1].set(0)
    dev_bias = jax.random.randint(key_dev, (GROUP_DEVS, EXPERTS), 0, DEV_SPREAD + 1)
    dev_bias = dev_bias.at[:, 0].set(DEV_SPREAD).at[:, 1].set(0)
    pair_load = MEAN_LOAD + (pop_bias - jnp.roll(pop_bias, -1))[None, :] + dev_bias - jnp.roll(dev_bias, -1, axis=1)
    run_ends = jnp.cumsum(pair_load, axis=1)
    positions = jnp.arange(TOKENS_DEV * TOP_K, dtype=jnp.int32)

    def find_run(row_ends):
        return jnp.searchsorted(row_ends, positions, side="right")

    run_index = jax.vmap(find_run)(run_ends)
    labels = expert_order[run_index].reshape(GROUP_DEVS, TOP_K, TOKENS_DEV)
    choices = jnp.swapaxes(labels, 1, 2)

    def token_order(sub_key):
        return jax.random.permutation(sub_key, TOKENS_DEV)

    tok_perm = jax.vmap(token_order)(jax.random.split(key_tok, GROUP_DEVS))
    choices = jnp.take_along_axis(choices, tok_perm[:, :, None], axis=1)
    choices = jax.random.permutation(key_col, choices, axis=2, independent=True)
    return choices.reshape(TOKENS, TOP_K).astype(jnp.int32)


def draw_matrices(key, fan_in, fan_out):
    def one_matrix(sub_key):
        return (jax.random.normal(sub_key, (fan_in, fan_out), jnp.float32) / math.sqrt(fan_in)).astype(jnp.bfloat16)
    return lax.map(one_matrix, jax.random.split(key, EXPERTS))


def setup_inputs(seed: int = 0, part: int = 0) -> dict:
    root = jax.random.key(seed)
    part_key = jax.random.fold_in(root, part)
    key_route, key_rows, key_gate = jax.random.split(part_key, 3)
    key_up, key_down = jax.random.split(jax.random.fold_in(root, 1000003), 2)
    token_rows = jax.random.normal(key_rows, (TOKENS, MODEL_DIM), jnp.float32).astype(jnp.bfloat16)
    gate_weights = jax.random.uniform(key_gate, (TOKENS, TOP_K), jnp.float32, 0.5, 1.5) / math.sqrt(TOP_K)
    return {"token_rows": token_rows, "expert_ids": draw_routing(key_route), "gate_weights": gate_weights, "w_in": draw_matrices(key_up, MODEL_DIM, HIDDEN_DIM), "w_out": draw_matrices(key_down, HIDDEN_DIM, MODEL_DIM)}


def expert_ffn(operands):
    rows, up_weight, down_weight = operands
    hidden = jax.nn.gelu(jnp.dot(rows, up_weight, preferred_element_type=jnp.float32)).astype(jnp.bfloat16)
    return jnp.dot(hidden, down_weight, preferred_element_type=jnp.float32).astype(jnp.bfloat16)


def reference(token_rows, expert_ids, gate_weights, w_in, w_out):
    pairs = TOP_K * TOKENS
    flat_ids = expert_ids.T.reshape(pairs)
    sort_order = jnp.argsort(flat_ids, stable=True)
    position = jnp.zeros((pairs,), jnp.int32).at[sort_order].set(jnp.arange(pairs, dtype=jnp.int32))
    counts = jnp.bincount(flat_ids, length=EXPERTS)
    seg_start = jnp.cumsum(counts) - counts
    slot = position - seg_start[flat_ids]
    keep = slot < CAPACITY
    slot_safe = jnp.where(keep, slot, CAPACITY)
    buffer = jnp.zeros((EXPERTS, CAPACITY, MODEL_DIM), token_rows.dtype).at[flat_ids, slot_safe].set(jnp.tile(token_rows, (TOP_K, 1)), mode="drop")
    outputs = lax.map(expert_ffn, (buffer, w_in, w_out))
    weight = jnp.where(keep, gate_weights.T.reshape(pairs), 0.0).reshape(TOP_K, TOKENS)
    slot_read = jnp.minimum(slot, CAPACITY - 1).reshape(TOP_K, TOKENS)

    def add_choice(total, pieces):
        choice_weight, choice_ids, choice_slot = pieces
        return total + choice_weight[:, None] * outputs[choice_ids, choice_slot].astype(jnp.float32), None

    mixed, _ = lax.scan(add_choice, token_rows.astype(jnp.float32), (weight, flat_ids.reshape(TOP_K, TOKENS), slot_read))
    return mixed.astype(jnp.bfloat16)
```

```python
import functools

import jax
import jax.numpy as jnp
from jax import lax
from jax.experimental import pallas as pl
from jax.experimental.pallas import tpu as pltpu
from jax.sharding import PartitionSpec as P

MESH = pl.DeviceIdType.MESH
F32 = jnp.float32
BF16 = jnp.bfloat16
AXIS = "expert"
LANES = 128
IN_BLOCKS = 4
IN_DEPTH = 1
OUT_COLS = 256
OUT_DEPTH = 3
BIG_BF16 = 3.3895313892515355e38

OWN_R, OWN_L, OWN_P, RELAY_R, RELAY_L, FWD_L, FWD_R, FWD_A, FWD_B = range(9)
PART, FAR_R, FAR_L, NEAR_R, NEAR_L, MIX_R, MIX_L = range(7)


def body(n, capacity, ids_ref, gate_ref, x_hbm, w_in, w_out, out_hbm,
         ids_all, gates_all, x_all, pick, packed, mix, xg, acc, hid, obuf,
         part_send, part_recv, total, far_recv, fin_recv, out_buf, win_buf, wout_buf,
         meta_ssem, meta_rsem, d_ssem, d_rsem, r_ssem, r_rsem, x_sem, win_sem, wout_sem, out_sem):
    top_k, tokens = ids_ref.shape
    local_e, model, hidden = w_in.shape
    chips = n // 2
    kc_n = model // IN_BLOCKS
    oc_n = model // OUT_COLS
    slots = local_e * capacity

    me = lax.axis_index(AXIS)
    core = lax.rem(me, 2)
    chip = me // 2
    buddy = me + 1 - 2 * core
    other = 1 - core
    c_right = lax.rem(chip + 1, chips)
    c_far = lax.rem(chip + 2, chips)
    c_left = lax.rem(chip + 3, chips)

    def dev(c, k):
        return 2 * c + k

    right = dev(c_right, core)
    left = dev(c_left, core)

    def win_copy(e, kc):
        slot = lax.rem(kc, IN_DEPTH) * local_e + e
        return pltpu.make_async_copy(
            w_in.at[e, pl.ds(kc * kc_n, kc_n), :], win_buf.at[slot], win_sem.at[slot])

    def wout_copy(e, oc):
        slot = lax.rem(oc, OUT_DEPTH) * local_e + e
        return pltpu.make_async_copy(
            w_out.at[e, :, pl.ds(oc * OUT_COLS, OUT_COLS)], wout_buf.at[slot], wout_sem.at[slot])

    def x_rows(kc, d):
        return x_all.at[kc, pl.ds(d * tokens, tokens), :]

    def x_half(kc, d, h):
        half = tokens // 2
        return x_all.at[kc, pl.ds(d * tokens + h * half, half), :]

    def x_copy(kc):
        return pltpu.make_async_copy(
            x_hbm.at[:, pl.ds(kc * kc_n, kc_n)], x_rows(kc, me), x_sem.at[kc])

    for kc in range(IN_BLOCKS):
        x_copy(kc).start()

    @pl.loop(0, IN_DEPTH)
    def _(kc):
        @pl.loop(0, local_e)
        def _(e):
            win_copy(e, kc).start()

    @pl.loop(0, OUT_DEPTH)
    def _(oc):
        @pl.loop(0, local_e)
        def _(e):
            wout_copy(e, oc).start()

    barrier = pltpu.get_barrier_semaphore()
    for d in range(1, n):
        pl.semaphore_signal(barrier, inc=1, device_id={AXIS: lax.rem(me + d, n)}, device_id_type=MESH)
    pl.semaphore_wait(barrier, n - 1)

    def meta_copies(d):
        to = lax.rem(me + d, n)
        return (
            pltpu.make_async_remote_copy(
                src_ref=ids_ref, dst_ref=ids_all.at[me], send_sem=meta_ssem.at[0, d], recv_sem=meta_rsem.at[0, d],
                device_id={AXIS: to}, device_id_type=MESH),
            pltpu.make_async_remote_copy(
                src_ref=gate_ref, dst_ref=gates_all.at[me], send_sem=meta_ssem.at[1, d], recv_sem=meta_rsem.at[1, d],
                device_id={AXIS: to}, device_id_type=MESH),
        )

    for d in range(1, n):
        for c in meta_copies(d):
            c.start()
    ids_all[me] = ids_ref[...]
    gates_all[me] = gate_ref[...]

    def dcopy(kind, kc, ref, to):
        return pltpu.make_async_remote_copy(
            src_ref=ref, dst_ref=ref, send_sem=d_ssem.at[kind, kc], recv_sem=d_rsem.at[kind, kc],
            device_id={AXIS: to}, device_id_type=MESH)

    far = dev(c_far, core)

    def d_sent(kind, kc):
        if kind == OWN_R:
            return dcopy(kind, kc, x_rows(kc, me), right)
        if kind == OWN_L:
            return dcopy(kind, kc, x_rows(kc, me), left)
        if kind == OWN_P:
            return dcopy(kind, kc, x_rows(kc, me), buddy)
        if kind == RELAY_R:
            return dcopy(kind, kc, x_half(kc, left, 0), right)
        if kind == RELAY_L:
            return dcopy(kind, kc, x_half(kc, right, 1), left)
        if kind == FWD_L:
            return dcopy(kind, kc, x_rows(kc, left), buddy)
        if kind == FWD_R:
            return dcopy(kind, kc, x_rows(kc, right), buddy)
        if kind == FWD_A:
            return dcopy(kind, kc, x_half(kc, far, 0), buddy)
        return dcopy(kind, kc, x_half(kc, far, 1), buddy)

    def d_got(kind, kc):
        if kind == OWN_R:
            ref = x_rows(kc, left)
        elif kind == OWN_L:
            ref = x_rows(kc, right)
        elif kind == OWN_P:
            ref = x_rows(kc, buddy)
        elif kind == RELAY_R:
            ref = x_half(kc, far, 0)
        elif kind == RELAY_L:
            ref = x_half(kc, far, 1)
        elif kind == FWD_L:
            ref = x_rows(kc, dev(c_left, other))
        elif kind == FWD_R:
            ref = x_rows(kc, dev(c_right, other))
        elif kind == FWD_A:
            ref = x_half(kc, dev(c_far, other), 0)
        else:
            ref = x_half(kc, dev(c_far, other), 1)
        return dcopy(kind, kc, ref, buddy)

    def send_own(kc):
        x_copy(kc).wait()
        for kind in (OWN_R, OWN_L, OWN_P):
            d_sent(kind, kc).start()

    def stage1(kc):
        d_got(OWN_R, kc).wait_recv()
        d_sent(RELAY_R, kc).start()
        d_sent(FWD_L, kc).start()
        d_got(OWN_L, kc).wait_recv()
        d_sent(RELAY_L, kc).start()
        d_sent(FWD_R, kc).start()

    def stage2(kc):
        d_got(RELAY_R, kc).wait_recv()
        d_sent(FWD_A, kc).start()
        d_got(RELAY_L, kc).wait_recv()
        d_sent(FWD_B, kc).start()

    def stage3(kc):
        for kind in (OWN_P, FWD_L, FWD_R, FWD_A, FWD_B):
            d_got(kind, kc).wait_recv()

    send_own(0)
    send_own(1)

    for d in range(1, n):
        for c in meta_copies(d):
            c.wait_recv()

    sub = lax.broadcasted_iota(jnp.int32, (local_e, tokens), 0) + me * local_e
    hit = {}
    for b in range(n):
        for j in range(top_k):
            hit[b, j] = jnp.where(ids_all[b, j:j + 1, :] == sub, 1.0, 0.0).astype(F32)
    hits = jnp.concatenate([hit[b, j] for b in range(n) for j in range(top_k)], axis=0).astype(BF16)
    t_from = lax.broadcasted_iota(jnp.int32, (tokens, tokens), 0)
    t_to = lax.broadcasted_iota(jnp.int32, (tokens, tokens), 1)
    earlier = jnp.where(t_from < t_to, 1.0, 0.0).astype(BF16)
    ones = jnp.full((tokens, tokens), 1.0, BF16)
    within = jnp.dot(hits, earlier, preferred_element_type=F32)
    sums = jnp.dot(hits, ones, preferred_element_type=F32)
    running = jnp.zeros((local_e, tokens), F32)
    rank = [jnp.zeros((local_e, tokens), F32) for _ in range(n)]
    for j in range(top_k):
        for b in range(n):
            at = (b * top_k + j) * local_e
            rank[b] = rank[b] + hit[b, j] * (running + within[at:at + local_e])
            running = running + sums[at:at + local_e]
    slot_row = lax.broadcasted_iota(jnp.int32, (capacity, tokens), 0).astype(F32)
    for b in range(n):
        has = jnp.zeros((local_e, tokens), F32)
        gate = jnp.zeros((local_e, tokens), F32)
        for j in range(top_k):
            has = has + hit[b, j]
            gate = gate + hit[b, j] * gates_all[b, j:j + 1, :]
        slot = jnp.where((has > 0.0) & (rank[b] < capacity), rank[b], -1.0)
        g1 = jnp.minimum(gate, BIG_BF16).astype(BF16).astype(F32)
        g2 = (gate - g1).astype(BF16).astype(F32)
        g3 = gate - g1 - g2
        packed[b] = jnp.concatenate([slot, g1, g2, g3], axis=0)
        for e in range(local_e):
            pick[e * capacity:(e + 1) * capacity, b * tokens:(b + 1) * tokens] = jnp.where(
                slot[e:e + 1, :] == slot_row, 1.0, 0.0).astype(BF16)

    stage1(0)
    if IN_BLOCKS > 2:
        send_own(2)

    lane = lax.broadcasted_iota(jnp.int32, (tokens, LANES), 1)

    @pl.loop(0, n)
    def _(b):
        row = pl.multiple_of((lax.rem(b, 2) * chips + b // 2) * tokens, tokens)
        cols = jnp.concatenate(
            [packed[b], jnp.zeros((LANES - 4 * local_e, tokens), F32)], axis=0).T
        for tile in range(slots // LANES):
            first = tile * LANES // capacity
            last = (tile * LANES + LANES - 1) // capacity
            col = lane + tile * LANES

            def per_lane(k):
                out = cols[:, k * local_e + first:k * local_e + first + 1]
                out = jnp.broadcast_to(out, (tokens, LANES))
                for e in range(first + 1, last + 1):
                    nxt = cols[:, k * local_e + e:k * local_e + e + 1]
                    out = jnp.where(col >= e * capacity, nxt, out)
                return out

            rel = col - first * capacity
            for e in range(first + 1, last + 1):
                rel = jnp.where(col >= e * capacity, col - e * capacity, rel)
            sel = per_lane(0) == rel.astype(F32)
            for k in range(3):
                mix[k, pl.ds(row, tokens), tile * LANES:(tile + 1) * LANES] = jnp.where(
                    sel, per_lane(k + 1), 0.0).astype(BF16)

    for kc in range(IN_BLOCKS):
        if kc + 1 < IN_BLOCKS:
            stage1(kc + 1)
            if kc + 3 < IN_BLOCKS:
                send_own(kc + 3)
        stage2(kc)
        stage3(kc)
        xg[...] = jnp.dot(pick[...], x_all[kc], preferred_element_type=F32).astype(BF16).reshape(local_e, capacity, kc_n)

        @pl.loop(0, local_e)
        def _(e):
            win_copy(e, kc).wait()
            slot = (kc % IN_DEPTH) * local_e + e
            up = jnp.dot(xg[e], win_buf[slot], preferred_element_type=F32)
            if kc > 0:
                up = up + acc[e]
            if kc + 1 < IN_BLOCKS:
                acc[e] = up
            else:
                hid[e] = jax.nn.gelu(up).astype(BF16)
            if kc + IN_DEPTH < IN_BLOCKS:
                win_copy(e, kc + IN_DEPTH).start()

    for kc in range(IN_BLOCKS):
        for kind in range(9):
            d_sent(kind, kc).wait_send()
    for d in range(1, n):
        for c in meta_copies(d):
            c.wait_send()

    def rcopy(kind, oc, src, dst, to):
        return pltpu.make_async_remote_copy(
            src_ref=src, dst_ref=dst, send_sem=r_ssem.at[kind, oc], recv_sem=r_rsem.at[kind, oc],
            device_id={AXIS: to}, device_id_type=MESH)

    def r_copy(kind, oc):
        if kind == PART:
            return rcopy(kind, oc, part_send.at[lax.rem(oc, 2)], part_recv.at[oc], buddy)
        if kind == FAR_R:
            return rcopy(kind, oc, total.at[oc, c_far, 0], far_recv.at[oc, 0], right)
        if kind == FAR_L:
            return rcopy(kind, oc, total.at[oc, c_far, 1], far_recv.at[oc, 1], left)
        if kind == NEAR_R:
            return rcopy(kind, oc, total.at[oc, c_right, 1], fin_recv.at[oc, 0, 1], right)
        if kind == NEAR_L:
            return rcopy(kind, oc, total.at[oc, c_left, 0], fin_recv.at[oc, 1, 0], left)
        if kind == MIX_R:
            return rcopy(kind, oc, total.at[oc, c_right, 0], fin_recv.at[oc, 0, 0], right)
        return rcopy(kind, oc, total.at[oc, c_left, 1], fin_recv.at[oc, 1, 1], left)

    rows = chips * tokens
    half = OUT_COLS // 2
    step_rows = rows // 2

    def partial(rail, dst):
        @pl.loop(0, rows // step_rows)
        def _(i):
            at = pl.multiple_of(rail * rows + i * step_rows, step_rows)
            val = jnp.dot(mix[0, pl.ds(at, step_rows), :], obuf[...], preferred_element_type=F32)
            val += jnp.dot(mix[1, pl.ds(at, step_rows), :], obuf[...], preferred_element_type=F32)
            val += jnp.dot(mix[2, pl.ds(at, step_rows), :], obuf[...], preferred_element_type=F32)
            for t in range(step_rows // tokens):
                for h in range(2):
                    dst[i * (step_rows // tokens) + t, h] = val[
                        t * tokens:(t + 1) * tokens, h * half:(h + 1) * half]

    def out_copy(oc):
        return pltpu.make_async_copy(
            out_buf.at[oc], out_hbm.at[:, pl.ds(oc * OUT_COLS, OUT_COLS)], out_sem.at[oc])

    def finish_far(oc):
        r_copy(FAR_R, oc).wait_recv()
        total[oc, c_right, 0] = total[oc, c_right, 0] + far_recv[oc, 0]
        r_copy(MIX_R, oc).start()
        r_copy(FAR_L, oc).wait_recv()
        total[oc, c_left, 1] = total[oc, c_left, 1] + far_recv[oc, 1]
        r_copy(MIX_L, oc).start()

    per_in = kc_n // OUT_COLS

    def finish(oc):
        for kind in (NEAR_R, NEAR_L, MIX_R, MIX_L):
            r_copy(kind, oc).wait_recv()
        for h in range(2):
            at = pl.multiple_of(lax.rem(oc, per_in) * OUT_COLS + h * half, half)
            x_own = x_all[oc // per_in, pl.ds(pl.multiple_of(me * tokens, tokens), tokens), pl.ds(at, half)]
            val = total[oc, chip, h] + fin_recv[oc, 0, h] + fin_recv[oc, 1, h]
            out_buf[oc, :, h * half:(h + 1) * half] = (x_own.astype(F32) + val).astype(BF16)
        out_copy(oc).start()

    @pl.loop(0, oc_n)
    def _(oc):
        @pl.loop(0, local_e)
        def _(e):
            wout_copy(e, oc).wait()
            slot = lax.rem(oc, OUT_DEPTH) * local_e + e
            val = jnp.dot(hid[e], wout_buf[slot], preferred_element_type=F32)
            obuf[pl.ds(pl.multiple_of(e * capacity, capacity), capacity), :] = val.astype(BF16)

            @pl.when(oc + OUT_DEPTH < oc_n)
            def _():
                wout_copy(e, oc + OUT_DEPTH).start()

        @pl.when(oc >= 2)
        def _():
            r_copy(PART, oc - 2).wait_send()

        partial(other, part_send.at[lax.rem(oc, 2)])
        r_copy(PART, oc).start()
        partial(core, total.at[oc])
        r_copy(PART, oc).wait_recv()
        total[oc] = total[oc] + part_recv[oc]
        for kind in (FAR_R, FAR_L, NEAR_R, NEAR_L):
            r_copy(kind, oc).start()

        @pl.when(oc >= 1)
        def _():
            finish_far(oc - 1)

        @pl.when(oc >= 2)
        def _():
            finish(oc - 2)

    finish_far(oc_n - 1)
    finish(oc_n - 2)
    finish(oc_n - 1)

    for oc in range(oc_n):
        out_copy(oc).wait()
        for kind in range(7):
            if kind != PART or oc >= oc_n - 2:
                r_copy(kind, oc).wait_send()


def solution(mesh):
    n = mesh.shape[AXIS]
    row_spec = P(("data", AXIS), None)
    weight_spec = P(AXIS, None, None)

    def device_step(token_rows, expert_ids, gate_weights, w_in, w_out):
        tokens, top_k = expert_ids.shape
        local_e, model, hidden = w_in.shape
        capacity = n * tokens * top_k // (n * local_e)
        slots = local_e * capacity
        chips = n // 2
        kc_n = model // IN_BLOCKS
        oc_n = model // OUT_COLS
        half = OUT_COLS // 2
        vmem = pl.BlockSpec(memory_space=pltpu.VMEM)
        hbm = pl.BlockSpec(memory_space=pl.ANY)
        dma = pltpu.SemaphoreType.DMA
        return pl.pallas_call(
            functools.partial(body, n, capacity),
            out_shape=jax.ShapeDtypeStruct((tokens, model), BF16),
            in_specs=[vmem, vmem, hbm, hbm, hbm],
            out_specs=hbm,
            scratch_shapes=[
                pltpu.VMEM((n, top_k, tokens), jnp.int32),
                pltpu.VMEM((n, top_k, tokens), F32),
                pltpu.VMEM((IN_BLOCKS, n * tokens, kc_n), BF16),
                pltpu.VMEM((slots, n * tokens), BF16),
                pltpu.VMEM((n, 4 * local_e, tokens), F32),
                pltpu.VMEM((3, n * tokens, slots), BF16),
                pltpu.VMEM((local_e, capacity, kc_n), BF16),
                pltpu.VMEM((local_e, capacity, hidden), F32),
                pltpu.VMEM((local_e, capacity, hidden), BF16),
                pltpu.VMEM((slots, OUT_COLS), BF16),
                pltpu.VMEM((2, chips, 2, tokens, half), F32),
                pltpu.VMEM((oc_n, chips, 2, tokens, half), F32),
                pltpu.VMEM((oc_n, chips, 2, tokens, half), F32),
                pltpu.VMEM((oc_n, 2, tokens, half), F32),
                pltpu.VMEM((oc_n, 2, 2, tokens, half), F32),
                pltpu.VMEM((oc_n, tokens, OUT_COLS), BF16),
                pltpu.VMEM((IN_DEPTH * local_e, kc_n, hidden), BF16),
                pltpu.VMEM((OUT_DEPTH * local_e, hidden, OUT_COLS), BF16),
                dma((2, n)), dma((2, n)),
                dma((9, IN_BLOCKS)), dma((9, IN_BLOCKS)),
                dma((7, oc_n)), dma((7, oc_n)),
                dma((IN_BLOCKS,)),
                dma((IN_DEPTH * local_e,)),
                dma((OUT_DEPTH * local_e,)),
                dma((oc_n,)),
            ],
            compiler_params=pltpu.CompilerParams(
                collective_id=0, has_side_effects=True, vmem_limit_bytes=67043328),
        )(expert_ids.T, gate_weights.T, token_rows, w_in, w_out)

    return jax.shard_map(device_step, mesh=mesh, in_specs=(row_spec, row_spec, row_spec, weight_spec, weight_spec),
                         out_specs=row_spec, check_vma=False)
```

```python
import functools

import jax
import jax.numpy as jnp
from jax import lax
from jax.experimental import pallas as pl
from jax.experimental.pallas import tpu as pltpu
from jax.sharding import PartitionSpec as P

MESH = pl.DeviceIdType.MESH
F32 = jnp.float32
BF16 = jnp.bfloat16
AXIS = "expert"
LANES = 128
IN_BLOCKS = 8
IN_DEPTH = 3
OUT_COLS = 256
OUT_DEPTH = 2
AHEAD = 3
BIG_BF16 = 3.3895313892515355e38

OWN_R, OWN_L, OWN_P, RELAY_R, RELAY_L, FWD_L, FWD_R, FWD_A, FWD_B = range(9)
PART, FAR_R, FAR_L, NEAR_R, NEAR_L, MIX_R, MIX_L = range(7)


def body(n, capacity, ids_hbm, gate_hbm, x_hbm, w_in, w_out, out_hbm,
         ids_all, gates_all, x_all, pick, packed, mix, xg, acc, hid, obuf0, obuf1,
         part_send, part_recv, total, far_recv, fin_recv, out_buf, win_buf, wout_buf,
         meta_ssem, meta_rsem, d_ssem, d_rsem, r_ssem, r_rsem, x_sem, win_sem, wout_sem, out_sem, own_sem):
    top_k, tokens = ids_hbm.shape
    local_e, model, hidden = w_in.shape
    chips = n // 2
    kc_n = model // IN_BLOCKS
    oc_n = model // OUT_COLS
    slots = local_e * capacity

    me = lax.axis_index(AXIS)
    core = lax.rem(me, 2)
    chip = me // 2
    buddy = me + 1 - 2 * core
    other = 1 - core
    c_right = lax.rem(chip + 1, chips)
    c_far = lax.rem(chip + 2, chips)
    c_left = lax.rem(chip + 3, chips)

    def dev(c, k):
        return 2 * c + k

    right = dev(c_right, core)
    left = dev(c_left, core)

    def win_copy(e, kc):
        slot = lax.rem(kc, IN_DEPTH) * local_e + e
        return pltpu.make_async_copy(
            w_in.at[e, pl.ds(kc * kc_n, kc_n), :], win_buf.at[slot], win_sem.at[slot])

    def wout_copy(e, oc):
        slot = lax.rem(oc, OUT_DEPTH) * local_e + e
        return pltpu.make_async_copy(
            w_out.at[e, :, pl.ds(oc * OUT_COLS, OUT_COLS)], wout_buf.at[slot], wout_sem.at[slot])

    def x_rows(kc, d):
        return x_all.at[kc, pl.ds(d * tokens, tokens), :]

    def x_half(kc, d, h):
        half = tokens // 2
        return x_all.at[kc, pl.ds(d * tokens + h * half, half), :]

    def x_copy(kc):
        return pltpu.make_async_copy(
            x_hbm.at[:, pl.ds(kc * kc_n, kc_n)], x_rows(kc, me), x_sem.at[kc])

    barrier = pltpu.get_barrier_semaphore()
    for d in range(1, n):
        pl.semaphore_signal(barrier, inc=1, device_id={AXIS: lax.rem(me + d, n)}, device_id_type=MESH)

    own_meta = (
        pltpu.make_async_copy(ids_hbm, ids_all.at[me], own_sem.at[0]),
        pltpu.make_async_copy(gate_hbm, gates_all.at[me], own_sem.at[1]),
    )
    for c in own_meta:
        c.start()
    for kc in range(IN_BLOCKS):
        x_copy(kc).start()

    @pl.loop(0, IN_DEPTH)
    def _(kc):
        for e in range(local_e):
            win_copy(e, kc).start()

    @pl.loop(0, OUT_DEPTH)
    def _(oc):
        for e in range(local_e):
            wout_copy(e, oc).start()

    with jax.named_scope("barrier"):
        pl.semaphore_wait(barrier, n - 1)
        for c in own_meta:
            c.wait()

    def meta_copies(d):
        to = lax.rem(me + d, n)
        return (
            pltpu.make_async_remote_copy(
                src_ref=ids_all.at[me], dst_ref=ids_all.at[me], send_sem=meta_ssem.at[0, d], recv_sem=meta_rsem.at[0, d],
                device_id={AXIS: to}, device_id_type=MESH),
            pltpu.make_async_remote_copy(
                src_ref=gates_all.at[me], dst_ref=gates_all.at[me], send_sem=meta_ssem.at[1, d], recv_sem=meta_rsem.at[1, d],
                device_id={AXIS: to}, device_id_type=MESH),
        )

    for d in range(1, n):
        for c in meta_copies(d):
            c.start()

    def dcopy(kind, kc, ref, to):
        return pltpu.make_async_remote_copy(
            src_ref=ref, dst_ref=ref, send_sem=d_ssem.at[kind, kc], recv_sem=d_rsem.at[kind, kc],
            device_id={AXIS: to}, device_id_type=MESH)

    far = dev(c_far, core)

    def d_sent(kind, kc):
        if kind == OWN_R:
            return dcopy(kind, kc, x_rows(kc, me), right)
        if kind == OWN_L:
            return dcopy(kind, kc, x_rows(kc, me), left)
        if kind == OWN_P:
            return dcopy(kind, kc, x_rows(kc, me), buddy)
        if kind == RELAY_R:
            return dcopy(kind, kc, x_half(kc, left, 0), right)
        if kind == RELAY_L:
            return dcopy(kind, kc, x_half(kc, right, 1), left)
        if kind == FWD_L:
            return dcopy(kind, kc, x_rows(kc, left), buddy)
        if kind == FWD_R:
            return dcopy(kind, kc, x_rows(kc, right), buddy)
        if kind == FWD_A:
            return dcopy(kind, kc, x_half(kc, far, 0), buddy)
        return dcopy(kind, kc, x_half(kc, far, 1), buddy)

    def d_got(kind, kc):
        if kind == OWN_R:
            ref = x_rows(kc, left)
        elif kind == OWN_L:
            ref = x_rows(kc, right)
        elif kind == OWN_P:
            ref = x_rows(kc, buddy)
        elif kind == RELAY_R:
            ref = x_half(kc, far, 0)
        elif kind == RELAY_L:
            ref = x_half(kc, far, 1)
        elif kind == FWD_L:
            ref = x_rows(kc, dev(c_left, other))
        elif kind == FWD_R:
            ref = x_rows(kc, dev(c_right, other))
        elif kind == FWD_A:
            ref = x_half(kc, dev(c_far, other), 0)
        else:
            ref = x_half(kc, dev(c_far, other), 1)
        return dcopy(kind, kc, ref, buddy)

    def send_own(kc):
        x_copy(kc).wait()
        for kind in (OWN_R, OWN_L, OWN_P):
            d_sent(kind, kc).start()

    def stage1(kc):
        d_got(OWN_R, kc).wait_recv()
        d_sent(RELAY_R, kc).start()
        d_sent(FWD_L, kc).start()
        d_got(OWN_L, kc).wait_recv()
        d_sent(RELAY_L, kc).start()
        d_sent(FWD_R, kc).start()

    def stage2(kc):
        d_got(RELAY_R, kc).wait_recv()
        d_sent(FWD_A, kc).start()
        d_got(RELAY_L, kc).wait_recv()
        d_sent(FWD_B, kc).start()

    def stage3(kc):
        for kind in (OWN_P, FWD_L, FWD_R, FWD_A, FWD_B):
            d_got(kind, kc).wait_recv()

    with jax.named_scope("own"):
        for kc in range(AHEAD):
            send_own(kc)

    with jax.named_scope("meta_wait"):
        for d in range(1, n):
            for c in meta_copies(d):
                c.wait_recv()

    sub = lax.broadcasted_iota(jnp.int32, (local_e, tokens), 0) + me * local_e
    hit = {}
    for b in range(n):
        for j in range(top_k):
            hit[b, j] = jnp.where(ids_all[b, j:j + 1, :] == sub, 1.0, 0.0).astype(F32)
    hits = jnp.concatenate([hit[b, j] for b in range(n) for j in range(top_k)], axis=0).astype(BF16)
    t_from = lax.broadcasted_iota(jnp.int32, (tokens, tokens), 0)
    t_to = lax.broadcasted_iota(jnp.int32, (tokens, tokens), 1)
    earlier = jnp.where(t_from < t_to, 1.0, 0.0).astype(BF16)
    ones = jnp.full((tokens, tokens), 1.0, BF16)
    within = jnp.dot(hits, earlier, preferred_element_type=F32)
    sums = jnp.dot(hits, ones, preferred_element_type=F32)
    running = jnp.zeros((local_e, tokens), F32)
    rank = [jnp.zeros((local_e, tokens), F32) for _ in range(n)]
    for j in range(top_k):
        for b in range(n):
            at = (b * top_k + j) * local_e
            rank[b] = rank[b] + hit[b, j] * (running + within[at:at + local_e])
            running = running + sums[at:at + local_e]
    slot_row = lax.broadcasted_iota(jnp.int32, (capacity, tokens), 0).astype(F32)
    for b in range(n):
        has = jnp.zeros((local_e, tokens), F32)
        gate = jnp.zeros((local_e, tokens), F32)
        for j in range(top_k):
            has = has + hit[b, j]
            gate = gate + hit[b, j] * gates_all[b, j:j + 1, :]
        slot = jnp.where((has > 0.0) & (rank[b] < capacity), rank[b], -1.0)
        g1 = jnp.minimum(gate, BIG_BF16).astype(BF16).astype(F32)
        g2 = (gate - g1).astype(BF16).astype(F32)
        g3 = gate - g1 - g2
        packed[b] = jnp.concatenate([slot, g1, g2, g3], axis=0)
        for e in range(local_e):
            pick[e * capacity:(e + 1) * capacity, b * tokens:(b + 1) * tokens] = jnp.where(
                slot[e:e + 1, :] == slot_row, 1.0, 0.0).astype(BF16)

    acc[...] = jnp.zeros_like(acc)
    with jax.named_scope("s1"):
        stage1(0)
        send_own(AHEAD)

    lane = lax.broadcasted_iota(jnp.int32, (tokens, LANES), 1)

    def mix_rows(b):
        row = pl.multiple_of((lax.rem(b, 2) * chips + b // 2) * tokens, tokens)
        cols = jnp.concatenate(
            [packed[b], jnp.zeros((LANES - 4 * local_e, tokens), F32)], axis=0).T
        for tile in range(slots // LANES):
            first = tile * LANES // capacity
            last = (tile * LANES + LANES - 1) // capacity
            col = lane + tile * LANES

            def per_lane(k):
                out = cols[:, k * local_e + first:k * local_e + first + 1]
                out = jnp.broadcast_to(out, (tokens, LANES))
                for e in range(first + 1, last + 1):
                    nxt = cols[:, k * local_e + e:k * local_e + e + 1]
                    out = jnp.where(col >= e * capacity, nxt, out)
                return out

            rel = col - first * capacity
            for e in range(first + 1, last + 1):
                rel = jnp.where(col >= e * capacity, col - e * capacity, rel)
            sel = per_lane(0) == rel.astype(F32)
            for k in range(3):
                mix[k, pl.ds(row, tokens), tile * LANES:(tile + 1) * LANES] = jnp.where(
                    sel, per_lane(k + 1), 0.0).astype(BF16)

    def gather(kc):
        xg[...] = jnp.dot(pick[...], x_all[kc], preferred_element_type=F32).astype(BF16).reshape(local_e, capacity, kc_n)

    def win_at(e, kc):
        return lax.rem(kc, IN_DEPTH) * local_e + e

    mix_step = n // IN_BLOCKS

    @pl.loop(0, IN_BLOCKS - 1)
    def _(kc):
        with jax.named_scope("s1"):
            stage1(kc + 1)

            @pl.when(kc + 1 + AHEAD < IN_BLOCKS)
            def _():
                send_own(kc + 1 + AHEAD)

        with jax.named_scope("mix"):
            for i in range(mix_step):
                mix_rows(kc * mix_step + i)
        with jax.named_scope("s2"):
            stage2(kc)
        with jax.named_scope("s3"):
            stage3(kc)
        with jax.named_scope("up"):
            gather(kc)
            for e in range(local_e):
                win_copy(e, kc).wait()
            for e in range(local_e):
                acc[e] = acc[e] + jnp.dot(xg[e], win_buf[win_at(e, kc)], preferred_element_type=F32)

            @pl.when(kc + IN_DEPTH < IN_BLOCKS)
            def _():
                for e in range(local_e):
                    win_copy(e, kc + IN_DEPTH).start()

    last = IN_BLOCKS - 1
    with jax.named_scope("mix"):
        for i in range(mix_step):
            mix_rows(last * mix_step + i)
    with jax.named_scope("s2"):
        stage2(last)
    with jax.named_scope("s3"):
        stage3(last)
    with jax.named_scope("up_last"):
        gather(last)
        for e in range(local_e):
            win_copy(e, last).wait()
        for e in range(local_e):
            up = acc[e] + jnp.dot(xg[e], win_buf[win_at(e, last)], preferred_element_type=F32)
            hid[e] = jax.nn.gelu(up).astype(BF16)

    with jax.named_scope("up_done"):
      for kc in range(IN_BLOCKS):
        for kind in range(9):
            d_sent(kind, kc).wait_send()
    for d in range(1, n):
        for c in meta_copies(d):
            c.wait_send()

    def rcopy(kind, oc, src, dst, to):
        return pltpu.make_async_remote_copy(
            src_ref=src, dst_ref=dst, send_sem=r_ssem.at[kind, oc], recv_sem=r_rsem.at[kind, oc],
            device_id={AXIS: to}, device_id_type=MESH)

    def r_copy(kind, oc):
        if kind == PART:
            return rcopy(kind, oc, part_send.at[lax.rem(oc, 2)], part_recv.at[oc], buddy)
        if kind == FAR_R:
            return rcopy(kind, oc, total.at[oc, c_far, 0], far_recv.at[oc, 0], right)
        if kind == FAR_L:
            return rcopy(kind, oc, total.at[oc, c_far, 1], far_recv.at[oc, 1], left)
        if kind == NEAR_R:
            return rcopy(kind, oc, total.at[oc, c_right, 1], fin_recv.at[oc, 0, 1], right)
        if kind == NEAR_L:
            return rcopy(kind, oc, total.at[oc, c_left, 0], fin_recv.at[oc, 1, 0], left)
        if kind == MIX_R:
            return rcopy(kind, oc, total.at[oc, c_right, 0], fin_recv.at[oc, 0, 0], right)
        return rcopy(kind, oc, total.at[oc, c_left, 1], fin_recv.at[oc, 1, 1], left)

    rows = chips * tokens
    half = OUT_COLS // 2

    def partial(rail, obuf, dst):
        at = pl.multiple_of(rail * rows, rows)
        val = jnp.dot(mix[0, pl.ds(at, rows), :], obuf[...], preferred_element_type=F32)
        val += jnp.dot(mix[1, pl.ds(at, rows), :], obuf[...], preferred_element_type=F32)
        val += jnp.dot(mix[2, pl.ds(at, rows), :], obuf[...], preferred_element_type=F32)
        for t in range(chips):
            for h in range(2):
                dst[t, h] = val[t * tokens:(t + 1) * tokens, h * half:(h + 1) * half]

    def out_copy(oc):
        return pltpu.make_async_copy(
            out_buf.at[oc], out_hbm.at[:, pl.ds(oc * OUT_COLS, OUT_COLS)], out_sem.at[oc])

    def finish_far(oc):
        r_copy(FAR_R, oc).wait_recv()
        total[oc, c_right, 0] = total[oc, c_right, 0] + far_recv[oc, 0]
        r_copy(MIX_R, oc).start()
        r_copy(FAR_L, oc).wait_recv()
        total[oc, c_left, 1] = total[oc, c_left, 1] + far_recv[oc, 1]
        r_copy(MIX_L, oc).start()

    per_in = kc_n // OUT_COLS

    def finish(oc):
        for kind in (NEAR_R, NEAR_L, MIX_R, MIX_L):
            r_copy(kind, oc).wait_recv()
        for h in range(2):
            at = pl.multiple_of(lax.rem(oc, per_in) * OUT_COLS + h * half, half)
            x_own = x_all[oc // per_in, pl.ds(pl.multiple_of(me * tokens, tokens), tokens), pl.ds(at, half)]
            val = total[oc, chip, h] + fin_recv[oc, 0, h] + fin_recv[oc, 1, h]
            out_buf[oc, :, h * half:(h + 1) * half] = (x_own.astype(F32) + val).astype(BF16)
        out_copy(oc).start()

    def down(oc, obuf):
        for e in range(local_e):
            wout_copy(e, oc).wait()
        for e in range(local_e):
            val = jnp.dot(hid[e], wout_buf[lax.rem(oc, OUT_DEPTH) * local_e + e], preferred_element_type=F32)
            obuf[e * capacity:(e + 1) * capacity, :] = val.astype(BF16)

    def refill(oc):
        for e in range(local_e):
            wout_copy(e, oc).start()

    def step(oc, now, nxt, peeled):
        with jax.named_scope("partA"):
            if peeled:
                r_copy(PART, oc - 2).wait_send()
            else:
                @pl.when(oc >= 2)
                def _():
                    r_copy(PART, oc - 2).wait_send()
            partial(other, now, part_send.at[lax.rem(oc, 2)])
            r_copy(PART, oc).start()
        with jax.named_scope("partB"):
            partial(core, now, total.at[oc])
        if nxt is not None:
            with jax.named_scope("down"):
                down(oc + 1, nxt)
                if not peeled:
                    @pl.when(oc + 1 + OUT_DEPTH < oc_n)
                    def _():
                        refill(oc + 1 + OUT_DEPTH)
        with jax.named_scope("part_wait"):
            r_copy(PART, oc).wait_recv()
        total[oc] = total[oc] + part_recv[oc]
        for kind in (FAR_R, FAR_L, NEAR_R, NEAR_L):
            r_copy(kind, oc).start()
        if peeled:
            with jax.named_scope("far"):
                finish_far(oc - 1)
            with jax.named_scope("fin"):
                finish(oc - 2)
        else:
            @pl.when(oc >= 1)
            def _():
                with jax.named_scope("far"):
                    finish_far(oc - 1)

            @pl.when(oc >= 2)
            def _():
                with jax.named_scope("fin"):
                    finish(oc - 2)

    down(0, obuf0)
    refill(OUT_DEPTH)

    @pl.loop(0, oc_n // 2 - 1)
    def _(i):
        step(2 * i, obuf0, obuf1, False)
        step(2 * i + 1, obuf1, obuf0, False)

    step(oc_n - 2, obuf0, obuf1, True)
    step(oc_n - 1, obuf1, None, True)

    with jax.named_scope("far_t"):
        finish_far(oc_n - 1)
    with jax.named_scope("fin_t1"):
        finish(oc_n - 2)
    with jax.named_scope("fin_t2"):
        finish(oc_n - 1)
    drain = jax.named_scope("drain")
    drain.__enter__()

    for oc in range(oc_n):
        out_copy(oc).wait()
        for kind in range(7):
            if kind != PART or oc >= oc_n - 2:
                r_copy(kind, oc).wait_send()
    drain.__exit__(None, None, None)


def solution(mesh):
    n = mesh.shape[AXIS]
    row_spec = P(("data", AXIS), None)
    weight_spec = P(AXIS, None, None)

    def device_step(token_rows, expert_ids, gate_weights, w_in, w_out):
        tokens, top_k = expert_ids.shape
        local_e, model, hidden = w_in.shape
        capacity = n * tokens * top_k // (n * local_e)
        slots = local_e * capacity
        chips = n // 2
        kc_n = model // IN_BLOCKS
        oc_n = model // OUT_COLS
        half = OUT_COLS // 2
        hbm = pl.BlockSpec(memory_space=pl.ANY)
        dma = pltpu.SemaphoreType.DMA
        return pl.pallas_call(
            functools.partial(body, n, capacity),
            out_shape=jax.ShapeDtypeStruct((tokens, model), BF16),
            in_specs=[hbm, hbm, hbm, hbm, hbm],
            out_specs=hbm,
            scratch_shapes=[
                pltpu.VMEM((n, top_k, tokens), jnp.int32),
                pltpu.VMEM((n, top_k, tokens), F32),
                pltpu.VMEM((IN_BLOCKS, n * tokens, kc_n), BF16),
                pltpu.VMEM((slots, n * tokens), BF16),
                pltpu.VMEM((n, 4 * local_e, tokens), F32),
                pltpu.VMEM((3, n * tokens, slots), BF16),
                pltpu.VMEM((local_e, capacity, kc_n), BF16),
                pltpu.VMEM((local_e, capacity, hidden), F32),
                pltpu.VMEM((local_e, capacity, hidden), BF16),
                pltpu.VMEM((slots, OUT_COLS), BF16),
                pltpu.VMEM((slots, OUT_COLS), BF16),
                pltpu.VMEM((2, chips, 2, tokens, half), F32),
                pltpu.VMEM((oc_n, chips, 2, tokens, half), F32),
                pltpu.VMEM((oc_n, chips, 2, tokens, half), F32),
                pltpu.VMEM((oc_n, 2, tokens, half), F32),
                pltpu.VMEM((oc_n, 2, 2, tokens, half), F32),
                pltpu.VMEM((oc_n, tokens, OUT_COLS), BF16),
                pltpu.VMEM((IN_DEPTH * local_e, kc_n, hidden), BF16),
                pltpu.VMEM((OUT_DEPTH * local_e, hidden, OUT_COLS), BF16),
                dma((2, n)), dma((2, n)),
                dma((9, IN_BLOCKS)), dma((9, IN_BLOCKS)),
                dma((7, oc_n)), dma((7, oc_n)),
                dma((IN_BLOCKS,)),
                dma((IN_DEPTH * local_e,)),
                dma((OUT_DEPTH * local_e,)),
                dma((oc_n,)),
                dma((2,)),
            ],
            compiler_params=pltpu.CompilerParams(
                collective_id=0, has_side_effects=True, vmem_limit_bytes=67043328),
        )(expert_ids.T, gate_weights.T, token_rows, w_in, w_out)

    return jax.shard_map(device_step, mesh=mesh, in_specs=(row_spec, row_spec, row_spec, weight_spec, weight_spec),
                         out_specs=row_spec, check_vma=False)
```

```python
import functools

import jax
import jax.numpy as jnp
from jax import lax
from jax.experimental import pallas as pl
from jax.experimental.pallas import tpu as pltpu
from jax.sharding import PartitionSpec as P

MESH = pl.DeviceIdType.MESH
F32 = jnp.float32
BF16 = jnp.bfloat16
AXIS = "expert"
LANES = 128
IN_BLOCKS = 8
IN_DEPTH = 3
OUT_COLS = 256
OUT_DEPTH = 2
AHEAD = 3
BIG_BF16 = 3.3895313892515355e38

OWN_R, OWN_L, OWN_P, RELAY_R, RELAY_L, FWD_L, FWD_R, FWD_A, FWD_B = range(9)
PART, FAR_R, FAR_L, NEAR_R, NEAR_L, MIX_R, MIX_L = range(7)


def body(n, capacity, ids_hbm, gate_hbm, x_hbm, w_in, w_out, out_hbm,
         ids_all, gates_all, x_all, pick, packed, mix, xg, acc, hid, obuf0, obuf1,
         part_send, part_recv, total, far_recv, fin_recv, out_buf, win_buf, wout_buf,
         meta_ssem, meta_rsem, d_ssem, d_rsem, r_ssem, r_rsem, x_sem, win_sem, wout_sem, out_sem, own_sem):
    top_k, tokens = ids_hbm.shape
    local_e, model, hidden = w_in.shape
    chips = n // 2
    kc_n = model // IN_BLOCKS
    oc_n = model // OUT_COLS
    slots = local_e * capacity

    me = lax.axis_index(AXIS)
    core = lax.rem(me, 2)
    chip = me // 2
    buddy = me + 1 - 2 * core
    other = 1 - core
    c_right = lax.rem(chip + 1, chips)
    c_far = lax.rem(chip + 2, chips)
    c_left = lax.rem(chip + 3, chips)

    def dev(c, k):
        return 2 * c + k

    right = dev(c_right, core)
    left = dev(c_left, core)

    def alone(fn):
        pl.when(me >= 0)(fn)

    def win_copy(e, kc):
        slot = lax.rem(kc, IN_DEPTH) * local_e + e
        return pltpu.make_async_copy(
            w_in.at[e, pl.ds(kc * kc_n, kc_n), :], win_buf.at[slot], win_sem.at[slot])

    def wout_copy(e, oc):
        slot = lax.rem(oc, OUT_DEPTH) * local_e + e
        return pltpu.make_async_copy(
            w_out.at[e, :, pl.ds(oc * OUT_COLS, OUT_COLS)], wout_buf.at[slot], wout_sem.at[slot])

    def x_rows(kc, d):
        return x_all.at[kc, pl.ds(d * tokens, tokens), :]

    def x_half(kc, d, h):
        half = tokens // 2
        return x_all.at[kc, pl.ds(d * tokens + h * half, half), :]

    def x_copy(kc):
        return pltpu.make_async_copy(
            x_hbm.at[:, pl.ds(kc * kc_n, kc_n)], x_rows(kc, me), x_sem.at[kc])

    barrier = pltpu.get_barrier_semaphore()
    for d in range(1, n):
        pl.semaphore_signal(barrier, inc=1, device_id={AXIS: lax.rem(me + d, n)}, device_id_type=MESH)

    own_meta = (
        pltpu.make_async_copy(ids_hbm, ids_all.at[me], own_sem.at[0]),
        pltpu.make_async_copy(gate_hbm, gates_all.at[me], own_sem.at[1]),
    )
    for c in own_meta:
        c.start()
    for kc in range(IN_BLOCKS):
        x_copy(kc).start()

    @pl.loop(0, IN_DEPTH)
    def _(kc):
        for e in range(local_e):
            win_copy(e, kc).start()

    @pl.loop(0, OUT_DEPTH)
    def _(oc):
        for e in range(local_e):
            wout_copy(e, oc).start()

    with jax.named_scope("barrier"):
        pl.semaphore_wait(barrier, n - 1)
        for c in own_meta:
            c.wait()

    def meta_copies(d):
        to = lax.rem(me + d, n)
        return (
            pltpu.make_async_remote_copy(
                src_ref=ids_all.at[me], dst_ref=ids_all.at[me], send_sem=meta_ssem.at[0, d], recv_sem=meta_rsem.at[0, d],
                device_id={AXIS: to}, device_id_type=MESH),
            pltpu.make_async_remote_copy(
                src_ref=gates_all.at[me], dst_ref=gates_all.at[me], send_sem=meta_ssem.at[1, d], recv_sem=meta_rsem.at[1, d],
                device_id={AXIS: to}, device_id_type=MESH),
        )

    for d in range(1, n):
        for c in meta_copies(d):
            c.start()

    def dcopy(kind, kc, ref, to):
        return pltpu.make_async_remote_copy(
            src_ref=ref, dst_ref=ref, send_sem=d_ssem.at[kind, kc], recv_sem=d_rsem.at[kind, kc],
            device_id={AXIS: to}, device_id_type=MESH)

    far = dev(c_far, core)

    def d_sent(kind, kc):
        if kind == OWN_R:
            return dcopy(kind, kc, x_rows(kc, me), right)
        if kind == OWN_L:
            return dcopy(kind, kc, x_rows(kc, me), left)
        if kind == OWN_P:
            return dcopy(kind, kc, x_rows(kc, me), buddy)
        if kind == RELAY_R:
            return dcopy(kind, kc, x_half(kc, left, 0), right)
        if kind == RELAY_L:
            return dcopy(kind, kc, x_half(kc, right, 1), left)
        if kind == FWD_L:
            return dcopy(kind, kc, x_rows(kc, left), buddy)
        if kind == FWD_R:
            return dcopy(kind, kc, x_rows(kc, right), buddy)
        if kind == FWD_A:
            return dcopy(kind, kc, x_half(kc, far, 0), buddy)
        return dcopy(kind, kc, x_half(kc, far, 1), buddy)

    def d_got(kind, kc):
        if kind == OWN_R:
            ref = x_rows(kc, left)
        elif kind == OWN_L:
            ref = x_rows(kc, right)
        elif kind == OWN_P:
            ref = x_rows(kc, buddy)
        elif kind == RELAY_R:
            ref = x_half(kc, far, 0)
        elif kind == RELAY_L:
            ref = x_half(kc, far, 1)
        elif kind == FWD_L:
            ref = x_rows(kc, dev(c_left, other))
        elif kind == FWD_R:
            ref = x_rows(kc, dev(c_right, other))
        elif kind == FWD_A:
            ref = x_half(kc, dev(c_far, other), 0)
        else:
            ref = x_half(kc, dev(c_far, other), 1)
        return dcopy(kind, kc, ref, buddy)

    def send_own(kc):
        x_copy(kc).wait()
        for kind in (OWN_R, OWN_L, OWN_P):
            d_sent(kind, kc).start()

    def stage1(kc):
        d_got(OWN_R, kc).wait_recv()
        d_sent(RELAY_R, kc).start()
        d_sent(FWD_L, kc).start()
        d_got(OWN_L, kc).wait_recv()
        d_sent(RELAY_L, kc).start()
        d_sent(FWD_R, kc).start()

    def stage2(kc):
        d_got(RELAY_R, kc).wait_recv()
        d_sent(FWD_A, kc).start()
        d_got(RELAY_L, kc).wait_recv()
        d_sent(FWD_B, kc).start()

    def stage3(kc):
        for kind in (OWN_P, FWD_L, FWD_R, FWD_A, FWD_B):
            d_got(kind, kc).wait_recv()

    with jax.named_scope("own"):
        for kc in range(AHEAD):
            send_own(kc)

    with jax.named_scope("meta_wait"):
        for d in range(1, n):
            for c in meta_copies(d):
                c.wait_recv()

    sub = lax.broadcasted_iota(jnp.int32, (local_e, tokens), 0) + me * local_e
    hit = {}
    for b in range(n):
        for j in range(top_k):
            hit[b, j] = jnp.where(ids_all[b, j:j + 1, :] == sub, 1.0, 0.0).astype(F32)
    hits = jnp.concatenate([hit[b, j] for b in range(n) for j in range(top_k)], axis=0).astype(BF16)
    t_from = lax.broadcasted_iota(jnp.int32, (tokens, tokens), 0)
    t_to = lax.broadcasted_iota(jnp.int32, (tokens, tokens), 1)
    earlier = jnp.where(t_from < t_to, 1.0, 0.0).astype(BF16)
    ones = jnp.full((tokens, tokens), 1.0, BF16)
    within = jnp.dot(hits, earlier, preferred_element_type=F32)
    sums = jnp.dot(hits, ones, preferred_element_type=F32)
    running = jnp.zeros((local_e, tokens), F32)
    rank = [jnp.zeros((local_e, tokens), F32) for _ in range(n)]
    for j in range(top_k):
        for b in range(n):
            at = (b * top_k + j) * local_e
            rank[b] = rank[b] + hit[b, j] * (running + within[at:at + local_e])
            running = running + sums[at:at + local_e]
    slot_row = lax.broadcasted_iota(jnp.int32, (capacity, tokens), 0).astype(F32)
    for b in range(n):
        has = jnp.zeros((local_e, tokens), F32)
        gate = jnp.zeros((local_e, tokens), F32)
        for j in range(top_k):
            has = has + hit[b, j]
            gate = gate + hit[b, j] * gates_all[b, j:j + 1, :]
        slot = jnp.where((has > 0.0) & (rank[b] < capacity), rank[b], -1.0)
        g1 = jnp.minimum(gate, BIG_BF16).astype(BF16).astype(F32)
        g2 = (gate - g1).astype(BF16).astype(F32)
        g3 = gate - g1 - g2
        packed[b] = jnp.concatenate([slot, g1, g2, g3], axis=0)
        for e in range(local_e):
            pick[e * capacity:(e + 1) * capacity, b * tokens:(b + 1) * tokens] = jnp.where(
                slot[e:e + 1, :] == slot_row, 1.0, 0.0).astype(BF16)

    acc[...] = jnp.zeros_like(acc)
    with jax.named_scope("s1"):
        stage1(0)
        send_own(AHEAD)
        stage1(1)
        send_own(AHEAD + 1)

    lane = lax.broadcasted_iota(jnp.int32, (tokens, LANES), 1)

    def mix_rows(b):
        row = pl.multiple_of((lax.rem(b, 2) * chips + b // 2) * tokens, tokens)
        cols = jnp.concatenate(
            [packed[b], jnp.zeros((LANES - 4 * local_e, tokens), F32)], axis=0).T
        for tile in range(slots // LANES):
            first = tile * LANES // capacity
            last = (tile * LANES + LANES - 1) // capacity
            col = lane + tile * LANES

            def per_lane(k):
                out = cols[:, k * local_e + first:k * local_e + first + 1]
                out = jnp.broadcast_to(out, (tokens, LANES))
                for e in range(first + 1, last + 1):
                    nxt = cols[:, k * local_e + e:k * local_e + e + 1]
                    out = jnp.where(col >= e * capacity, nxt, out)
                return out

            rel = col - first * capacity
            for e in range(first + 1, last + 1):
                rel = jnp.where(col >= e * capacity, col - e * capacity, rel)
            sel = per_lane(0) == rel.astype(F32)
            for k in range(3):
                mix[k, pl.ds(row, tokens), tile * LANES:(tile + 1) * LANES] = jnp.where(
                    sel, per_lane(k + 1), 0.0).astype(BF16)

    def gather(kc):
        xg[...] = jnp.dot(pick[...], x_all[kc], preferred_element_type=F32).astype(BF16).reshape(local_e, capacity, kc_n)

    def win_at(e, kc):
        return lax.rem(kc, IN_DEPTH) * local_e + e

    mix_step = n // IN_BLOCKS

    with jax.named_scope("s2"):
        stage2(0)

    @pl.loop(0, IN_BLOCKS - 1)
    def _(kc):
        with jax.named_scope("s1"):
            @pl.when(kc + 2 < IN_BLOCKS)
            def _():
                stage1(kc + 2)

            @pl.when(kc + 2 + AHEAD < IN_BLOCKS)
            def _():
                send_own(kc + 2 + AHEAD)

        with jax.named_scope("mix"):
            for i in range(mix_step):
                mix_rows(kc * mix_step + i)
        with jax.named_scope("s2"):
            stage2(kc + 1)
        with jax.named_scope("s3"):
            stage3(kc)
        with jax.named_scope("up"):
            for e in range(local_e):
                win_copy(e, kc).wait()

            pl.when(chip >= 0)(lambda: gather(kc))

            @alone
            def _():
                for e in range(local_e):
                    acc[e] = acc[e] + jnp.dot(xg[e], win_buf[win_at(e, kc)], preferred_element_type=F32)

            @pl.when(kc + IN_DEPTH < IN_BLOCKS)
            def _():
                for e in range(local_e):
                    win_copy(e, kc + IN_DEPTH).start()

    last = IN_BLOCKS - 1
    with jax.named_scope("mix"):
        for i in range(mix_step):
            mix_rows(last * mix_step + i)
    with jax.named_scope("s3"):
        stage3(last)
    with jax.named_scope("up_last"):
        for e in range(local_e):
            win_copy(e, last).wait()

        pl.when(chip >= 0)(lambda: gather(last))

        @alone
        def _():
            for e in range(local_e):
                up = acc[e] + jnp.dot(xg[e], win_buf[win_at(e, last)], preferred_element_type=F32)
                hid[e] = jax.nn.gelu(up).astype(BF16)

    with jax.named_scope("up_done"):
      for kc in range(IN_BLOCKS):
        for kind in range(9):
            d_sent(kind, kc).wait_send()
    for d in range(1, n):
        for c in meta_copies(d):
            c.wait_send()

    def rcopy(kind, oc, src, dst, to):
        return pltpu.make_async_remote_copy(
            src_ref=src, dst_ref=dst, send_sem=r_ssem.at[kind, oc], recv_sem=r_rsem.at[kind, oc],
            device_id={AXIS: to}, device_id_type=MESH)

    def r_copy(kind, oc):
        if kind == PART:
            return rcopy(kind, oc, part_send.at[lax.rem(oc, 2)], part_recv.at[oc], buddy)
        if kind == FAR_R:
            return rcopy(kind, oc, total.at[oc, c_far, 0], far_recv.at[oc, 0], right)
        if kind == FAR_L:
            return rcopy(kind, oc, total.at[oc, c_far, 1], far_recv.at[oc, 1], left)
        if kind == NEAR_R:
            return rcopy(kind, oc, total.at[oc, c_right, 1], fin_recv.at[oc, 0, 1], right)
        if kind == NEAR_L:
            return rcopy(kind, oc, total.at[oc, c_left, 0], fin_recv.at[oc, 1, 0], left)
        if kind == MIX_R:
            return rcopy(kind, oc, total.at[oc, c_right, 0], fin_recv.at[oc, 0, 0], right)
        return rcopy(kind, oc, total.at[oc, c_left, 1], fin_recv.at[oc, 1, 1], left)

    rows = chips * tokens
    half = OUT_COLS // 2

    def partial(rail, obuf, dst):
        at = pl.multiple_of(rail * rows, rows)
        val = jnp.dot(mix[0, pl.ds(at, rows), :], obuf[...], preferred_element_type=F32)
        val += jnp.dot(mix[1, pl.ds(at, rows), :], obuf[...], preferred_element_type=F32)
        val += jnp.dot(mix[2, pl.ds(at, rows), :], obuf[...], preferred_element_type=F32)
        for t in range(chips):
            for h in range(2):
                dst[t, h] = val[t * tokens:(t + 1) * tokens, h * half:(h + 1) * half]

    def out_copy(oc):
        return pltpu.make_async_copy(
            out_buf.at[oc], out_hbm.at[:, pl.ds(oc * OUT_COLS, OUT_COLS)], out_sem.at[oc])

    def finish_far(oc):
        r_copy(FAR_R, oc).wait_recv()
        total[oc, c_right, 0] = total[oc, c_right, 0] + far_recv[oc, 0]
        r_copy(MIX_R, oc).start()
        r_copy(FAR_L, oc).wait_recv()
        total[oc, c_left, 1] = total[oc, c_left, 1] + far_recv[oc, 1]
        r_copy(MIX_L, oc).start()

    per_in = kc_n // OUT_COLS

    def finish(oc):
        for kind in (NEAR_R, NEAR_L, MIX_R, MIX_L):
            r_copy(kind, oc).wait_recv()
        for h in range(2):
            at = pl.multiple_of(lax.rem(oc, per_in) * OUT_COLS + h * half, half)
            x_own = x_all[oc // per_in, pl.ds(pl.multiple_of(me * tokens, tokens), tokens), pl.ds(at, half)]
            val = total[oc, chip, h] + fin_recv[oc, 0, h] + fin_recv[oc, 1, h]
            out_buf[oc, :, h * half:(h + 1) * half] = (x_own.astype(F32) + val).astype(BF16)
        out_copy(oc).start()

    def down(oc, obuf):
        for e in range(local_e):
            val = jnp.dot(hid[e], wout_buf[lax.rem(oc, OUT_DEPTH) * local_e + e], preferred_element_type=F32)
            obuf[e * capacity:(e + 1) * capacity, :] = val.astype(BF16)

    def refill(oc):
        for e in range(local_e):
            wout_copy(e, oc).start()

    def step(oc, now, nxt, peeled):
        with jax.named_scope("partA"):
            if peeled:
                r_copy(PART, oc - 2).wait_send()
            else:
                @pl.when(oc >= 2)
                def _():
                    r_copy(PART, oc - 2).wait_send()
            alone(lambda: partial(other, now, part_send.at[lax.rem(oc, 2)]))
            r_copy(PART, oc).start()
        if nxt is not None:
            for e in range(local_e):
                wout_copy(e, oc + 1).wait()
        with jax.named_scope("partB"):
            @alone
            def _():
                partial(core, now, total.at[oc])
                if nxt is not None:
                    down(oc + 1, nxt)
            if nxt is not None:
                if not peeled:
                    @pl.when(oc + 1 + OUT_DEPTH < oc_n)
                    def _():
                        refill(oc + 1 + OUT_DEPTH)
        with jax.named_scope("part_wait"):
            r_copy(PART, oc).wait_recv()
        total[oc] = total[oc] + part_recv[oc]
        for kind in (FAR_R, FAR_L, NEAR_R, NEAR_L):
            r_copy(kind, oc).start()
        if peeled:
            with jax.named_scope("far"):
                finish_far(oc - 1)
            with jax.named_scope("fin"):
                finish(oc - 2)
        else:
            @pl.when(oc >= 1)
            def _():
                with jax.named_scope("far"):
                    finish_far(oc - 1)

            @pl.when(oc >= 2)
            def _():
                with jax.named_scope("fin"):
                    finish(oc - 2)

    for e in range(local_e):
        wout_copy(e, 0).wait()
    alone(lambda: down(0, obuf0))
    refill(OUT_DEPTH)

    @pl.loop(0, oc_n // 2 - 1)
    def _(i):
        step(2 * i, obuf0, obuf1, False)
        step(2 * i + 1, obuf1, obuf0, False)

    step(oc_n - 2, obuf0, obuf1, True)
    step(oc_n - 1, obuf1, None, True)

    with jax.named_scope("far_t"):
        finish_far(oc_n - 1)
    with jax.named_scope("fin_t1"):
        finish(oc_n - 2)
    with jax.named_scope("fin_t2"):
        finish(oc_n - 1)
    drain = jax.named_scope("drain")
    drain.__enter__()

    for oc in range(oc_n):
        out_copy(oc).wait()
        for kind in range(7):
            if kind != PART or oc >= oc_n - 2:
                r_copy(kind, oc).wait_send()
    drain.__exit__(None, None, None)


def solution(mesh):
    n = mesh.shape[AXIS]
    row_spec = P(("data", AXIS), None)
    weight_spec = P(AXIS, None, None)

    def device_step(token_rows, expert_ids, gate_weights, w_in, w_out):
        tokens, top_k = expert_ids.shape
        local_e, model, hidden = w_in.shape
        capacity = n * tokens * top_k // (n * local_e)
        slots = local_e * capacity
        chips = n // 2
        kc_n = model // IN_BLOCKS
        oc_n = model // OUT_COLS
        half = OUT_COLS // 2
        hbm = pl.BlockSpec(memory_space=pl.ANY)
        dma = pltpu.SemaphoreType.DMA
        return pl.pallas_call(
            functools.partial(body, n, capacity),
            out_shape=jax.ShapeDtypeStruct((tokens, model), BF16),
            in_specs=[hbm, hbm, hbm, hbm, hbm],
            out_specs=hbm,
            scratch_shapes=[
                pltpu.VMEM((n, top_k, tokens), jnp.int32),
                pltpu.VMEM((n, top_k, tokens), F32),
                pltpu.VMEM((IN_BLOCKS, n * tokens, kc_n), BF16),
                pltpu.VMEM((slots, n * tokens), BF16),
                pltpu.VMEM((n, 4 * local_e, tokens), F32),
                pltpu.VMEM((3, n * tokens, slots), BF16),
                pltpu.VMEM((local_e, capacity, kc_n), BF16),
                pltpu.VMEM((local_e, capacity, hidden), F32),
                pltpu.VMEM((local_e, capacity, hidden), BF16),
                pltpu.VMEM((slots, OUT_COLS), BF16),
                pltpu.VMEM((slots, OUT_COLS), BF16),
                pltpu.VMEM((2, chips, 2, tokens, half), F32),
                pltpu.VMEM((oc_n, chips, 2, tokens, half), F32),
                pltpu.VMEM((oc_n, chips, 2, tokens, half), F32),
                pltpu.VMEM((oc_n, 2, tokens, half), F32),
                pltpu.VMEM((oc_n, 2, 2, tokens, half), F32),
                pltpu.VMEM((oc_n, tokens, OUT_COLS), BF16),
                pltpu.VMEM((IN_DEPTH * local_e, kc_n, hidden), BF16),
                pltpu.VMEM((OUT_DEPTH * local_e, hidden, OUT_COLS), BF16),
                dma((2, n)), dma((2, n)),
                dma((9, IN_BLOCKS)), dma((9, IN_BLOCKS)),
                dma((7, oc_n)), dma((7, oc_n)),
                dma((IN_BLOCKS,)),
                dma((IN_DEPTH * local_e,)),
                dma((OUT_DEPTH * local_e,)),
                dma((oc_n,)),
                dma((2,)),
            ],
            compiler_params=pltpu.CompilerParams(
                collective_id=0, has_side_effects=True, vmem_limit_bytes=67043328),
        )(expert_ids.T, gate_weights.T, token_rows, w_in, w_out)

    return jax.shard_map(device_step, mesh=mesh, in_specs=(row_spec, row_spec, row_spec, weight_spec, weight_spec),
                         out_specs=row_spec, check_vma=False)
```

```python
import functools

import jax
import jax.numpy as jnp
from jax import lax
from jax.experimental import pallas as pl
from jax.experimental.pallas import tpu as pltpu
from jax.sharding import PartitionSpec as P

MESH = pl.DeviceIdType.MESH
F32 = jnp.float32
BF16 = jnp.bfloat16
AXIS = "expert"
LANES = 128
IN_BLOCKS = 8
IN_DEPTH = 3
OUT_COLS = 256
OUT_DEPTH = 2
AHEAD = 3
LAG = 3
VMEM_BYTES = 62 * 2 ** 20
BIG_BF16 = 3.3895313892515355e38

OWN_R, OWN_L, OWN_P, RELAY_R, RELAY_L, FWD_L, FWD_R, FWD_A, FWD_B = range(9)
PART, FAR_R, FAR_L, NEAR_R, NEAR_L, MIX_R, MIX_L = range(7)


def body(n, capacity, ids_hbm, gate_hbm, x_hbm, w_in, w_out, out_ref,
         ids_all, gates_all, x_all, pick, packed, mix, xg, acc, hid, spread, obuf0, obuf1,
         part_send, part_recv, total, far_recv, fin_recv, win_buf, wout_buf,
         meta_ssem, meta_rsem, d_ssem, d_rsem, r_ssem, r_rsem, x_sem, win_sem, wout_sem, own_sem):
    top_k, tokens = ids_hbm.shape
    local_e, model, hidden = w_in.shape
    chips = n // 2
    kc_n = model // IN_BLOCKS
    oc_n = model // OUT_COLS
    slots = local_e * capacity

    me = lax.axis_index(AXIS)
    core = lax.rem(me, 2)
    chip = me // 2
    buddy = me + 1 - 2 * core
    other = 1 - core
    c_right = lax.rem(chip + 1, chips)
    c_far = lax.rem(chip + 2, chips)
    c_left = lax.rem(chip + 3, chips)

    def dev(c, k):
        return 2 * c + k

    right = dev(c_right, core)
    left = dev(c_left, core)

    def alone(fn):
        pl.when(me >= 0)(fn)

    def win_copy(e, kc):
        slot = lax.rem(kc, IN_DEPTH)
        return pltpu.make_async_copy(
            w_in.at[e, pl.ds(kc * kc_n, kc_n), :], win_buf.at[slot, e], win_sem.at[slot])

    def win_wait(kc):
        slot = lax.rem(kc, IN_DEPTH)
        pltpu.make_async_copy(w_in.at[:, pl.ds(0, kc_n), :], win_buf.at[slot], win_sem.at[slot]).wait()

    def wout_copy(e, oc):
        slot = lax.rem(oc, OUT_DEPTH)
        return pltpu.make_async_copy(
            w_out.at[e, :, pl.ds(oc * OUT_COLS, OUT_COLS)], wout_buf.at[slot, e], wout_sem.at[slot])

    def wout_wait(oc):
        slot = lax.rem(oc, OUT_DEPTH)
        pltpu.make_async_copy(w_out.at[:, :, pl.ds(0, OUT_COLS)], wout_buf.at[slot], wout_sem.at[slot]).wait()

    def x_rows(kc, d):
        return x_all.at[kc, pl.ds(d * tokens, tokens), :]

    def x_half(kc, d, h):
        half = tokens // 2
        return x_all.at[kc, pl.ds(d * tokens + h * half, half), :]

    def x_copy(kc):
        return pltpu.make_async_copy(
            x_hbm.at[:, pl.ds(kc * kc_n, kc_n)], x_rows(kc, me), x_sem)

    barrier = pltpu.get_barrier_semaphore()
    for d in range(1, n):
        pl.semaphore_signal(barrier, inc=1, device_id={AXIS: lax.rem(me + d, n)}, device_id_type=MESH)

    own_meta = (
        pltpu.make_async_copy(ids_hbm, ids_all.at[me], own_sem.at[0]),
        pltpu.make_async_copy(gate_hbm, gates_all.at[me], own_sem.at[1]),
    )
    for c in own_meta:
        c.start()
    for kc in range(IN_BLOCKS):
        x_copy(kc).start()

    @pl.loop(0, IN_DEPTH)
    def _(kc):
        for e in range(local_e):
            win_copy(e, kc).start()

    @pl.loop(0, OUT_DEPTH)
    def _(oc):
        for e in range(local_e):
            wout_copy(e, oc).start()

    with jax.named_scope("barrier"):
        pl.semaphore_wait(barrier, n - 1)
        for c in own_meta:
            c.wait()

    def meta_copies(d):
        to = lax.rem(me + d, n)
        return (
            pltpu.make_async_remote_copy(
                src_ref=ids_all.at[me], dst_ref=ids_all.at[me], send_sem=meta_ssem.at[0], recv_sem=meta_rsem.at[0],
                device_id={AXIS: to}, device_id_type=MESH),
            pltpu.make_async_remote_copy(
                src_ref=gates_all.at[me], dst_ref=gates_all.at[me], send_sem=meta_ssem.at[1], recv_sem=meta_rsem.at[1],
                device_id={AXIS: to}, device_id_type=MESH),
        )

    def meta_all():
        ids_part, gates_part = ids_all.at[pl.ds(0, n - 1)], gates_all.at[pl.ds(0, n - 1)]
        return (
            pltpu.make_async_remote_copy(
                src_ref=ids_part, dst_ref=ids_part, send_sem=meta_ssem.at[0], recv_sem=meta_rsem.at[0],
                device_id={AXIS: buddy}, device_id_type=MESH),
            pltpu.make_async_remote_copy(
                src_ref=gates_part, dst_ref=gates_part, send_sem=meta_ssem.at[1], recv_sem=meta_rsem.at[1],
                device_id={AXIS: buddy}, device_id_type=MESH),
        )

    for d in range(1, n):
        for c in meta_copies(d):
            c.start()

    def dcopy(kind, kc, ref, to):
        group = 0 if kind in (OWN_R, OWN_L) else 1 if kind in (RELAY_R, RELAY_L) else 2
        return pltpu.make_async_remote_copy(
            src_ref=ref, dst_ref=ref, send_sem=d_ssem.at[kind], recv_sem=d_rsem.at[group, kc],
            device_id={AXIS: to}, device_id_type=MESH)

    def d_wait(kind, kc, rows):
        dcopy(kind, kc, x_all.at[kc, pl.ds(0, rows), :], buddy).wait_recv()

    def d_flush(kind, rows):
        dcopy(kind, 0, x_all.at[:, pl.ds(0, rows), :], buddy).wait_send()

    far = dev(c_far, core)

    def d_sent(kind, kc):
        if kind == OWN_R:
            return dcopy(kind, kc, x_rows(kc, me), right)
        if kind == OWN_L:
            return dcopy(kind, kc, x_rows(kc, me), left)
        if kind == OWN_P:
            return dcopy(kind, kc, x_rows(kc, me), buddy)
        if kind == RELAY_R:
            return dcopy(kind, kc, x_half(kc, left, 0), right)
        if kind == RELAY_L:
            return dcopy(kind, kc, x_half(kc, right, 1), left)
        if kind == FWD_L:
            return dcopy(kind, kc, x_rows(kc, left), buddy)
        if kind == FWD_R:
            return dcopy(kind, kc, x_rows(kc, right), buddy)
        if kind == FWD_A:
            return dcopy(kind, kc, x_half(kc, far, 0), buddy)
        return dcopy(kind, kc, x_half(kc, far, 1), buddy)

    def send_own(kc):
        for kind in (OWN_R, OWN_L, OWN_P):
            d_sent(kind, kc).start()

    def stage1(kc):
        d_wait(OWN_R, kc, 2 * tokens)
        for kind in (RELAY_R, RELAY_L, FWD_L, FWD_R):
            d_sent(kind, kc).start()

    def stage2(kc):
        d_wait(RELAY_R, kc, tokens)
        for kind in (FWD_A, FWD_B):
            d_sent(kind, kc).start()

    def stage3(kc):
        d_wait(OWN_P, kc, chips * tokens)

    with jax.named_scope("own"):
        mine = x_all.at[:, pl.ds(me * tokens, tokens), :]
        pltpu.make_async_copy(mine, mine, x_sem).wait()
        for kc in range(AHEAD):
            send_own(kc)

    with jax.named_scope("meta_wait"):
        for c in meta_all():
            c.wait_recv()

    sub = lax.broadcasted_iota(jnp.int32, (local_e, tokens), 0) + me * local_e
    hit = {}
    for b in range(n):
        for j in range(top_k):
            hit[b, j] = jnp.where(ids_all[b, j:j + 1, :] == sub, 1.0, 0.0).astype(F32)
    hits = jnp.concatenate([hit[b, j] for b in range(n) for j in range(top_k)], axis=0).astype(BF16)
    t_from = lax.broadcasted_iota(jnp.int32, (tokens, tokens), 0)
    t_to = lax.broadcasted_iota(jnp.int32, (tokens, tokens), 1)
    earlier = jnp.where(t_from < t_to, 1.0, 0.0).astype(BF16)
    ones = jnp.full((tokens, tokens), 1.0, BF16)
    within = jnp.dot(hits, earlier, preferred_element_type=F32)
    sums = jnp.dot(hits, ones, preferred_element_type=F32)
    running = jnp.zeros((local_e, tokens), F32)
    rank = [jnp.zeros((local_e, tokens), F32) for _ in range(n)]
    for j in range(top_k):
        for b in range(n):
            at = (b * top_k + j) * local_e
            rank[b] = rank[b] + hit[b, j] * (running + within[at:at + local_e])
            running = running + sums[at:at + local_e]
    slot_row = lax.broadcasted_iota(jnp.int32, (capacity, tokens), 0).astype(F32)
    for b in range(n):
        has = jnp.zeros((local_e, tokens), F32)
        gate = jnp.zeros((local_e, tokens), F32)
        for j in range(top_k):
            has = has + hit[b, j]
            gate = gate + hit[b, j] * gates_all[b, j:j + 1, :]
        slot = jnp.where((has > 0.0) & (rank[b] < capacity), rank[b], -1.0)
        g1 = jnp.minimum(gate, BIG_BF16).astype(BF16).astype(F32)
        g2 = (gate - g1).astype(BF16).astype(F32)
        g3 = gate - g1 - g2
        packed[b] = jnp.concatenate([slot, g1, g2, g3], axis=0)
        for e in range(local_e):
            pick[e * capacity:(e + 1) * capacity, b * tokens:(b + 1) * tokens] = jnp.where(
                slot[e:e + 1, :] == slot_row, 1.0, 0.0).astype(BF16)

    acc[...] = jnp.zeros_like(acc)

    part_c = 2 * LANES
    for q in range(4):
        at = lax.broadcasted_iota(jnp.int32, (LANES, slots), 1)
        row = lax.broadcasted_iota(jnp.int32, (LANES, slots), 0) - q * local_e
        spread[:, q * slots:(q + 1) * slots] = jnp.where(
            (at >= row * capacity) & (at < (row + 1) * capacity) & (row >= 0) & (row < local_e), 1.0, 0.0).astype(BF16)

    def mix_rows(b):
        row = pl.multiple_of((lax.rem(b, 2) * chips + b // 2) * tokens, tokens)
        cols = jnp.concatenate(
            [packed[b], jnp.zeros((LANES - 4 * local_e, tokens), F32)], axis=0).T.astype(BF16)
        for p in range(slots // part_c):
            at = lax.broadcasted_iota(jnp.int32, (1, part_c), 1) + p * part_c
            rel = at
            for e in range(1, local_e):
                rel = jnp.where(at >= e * capacity, at - e * capacity, rel)
            rel = rel.astype(F32)

            def repeat(q):
                return jnp.dot(cols, spread[:, q * slots + p * part_c:q * slots + (p + 1) * part_c],
                               preferred_element_type=F32)

            slot_at = repeat(0)
            for k in range(3):
                mix[k, pl.ds(row, tokens), p * part_c:(p + 1) * part_c] = jnp.where(
                    slot_at == rel, repeat(k + 1), 0.0).astype(BF16)

    def mix_range(lo, hi):
        with jax.named_scope("mix"):
            pl.loop(lo, hi)(mix_rows)

    with jax.named_scope("s1"):
        stage1(0)
        send_own(AHEAD)
    mix_range(0, n // 2)
    with jax.named_scope("s1"):
        stage1(1)
        send_own(AHEAD + 1)
    mix_range(n // 2, n)

    def gather(kc):
        xg[...] = jnp.dot(pick[...], x_all[kc], preferred_element_type=F32).astype(BF16).reshape(local_e, capacity, kc_n)

    with jax.named_scope("s2"):
        stage2(0)

    @pl.loop(0, IN_BLOCKS - 1)
    def _(kc):
        with jax.named_scope("s1"):
            @pl.when(kc + 2 < IN_BLOCKS)
            def _():
                stage1(kc + 2)

            @pl.when(kc + 2 + AHEAD < IN_BLOCKS)
            def _():
                send_own(kc + 2 + AHEAD)

        with jax.named_scope("s2"):
            stage2(kc + 1)
        with jax.named_scope("s3"):
            stage3(kc)
        with jax.named_scope("up"):
            win_wait(kc)

            pl.when(chip >= 0)(lambda: gather(kc))

            @alone
            def _():
                for e in range(local_e):
                    acc[e] = acc[e] + jnp.dot(xg[e], win_buf[lax.rem(kc, IN_DEPTH), e], preferred_element_type=F32)

            @pl.when(kc + IN_DEPTH < IN_BLOCKS)
            def _():
                for e in range(local_e):
                    win_copy(e, kc + IN_DEPTH).start()

    last = IN_BLOCKS - 1
    with jax.named_scope("s3"):
        stage3(last)
    with jax.named_scope("up_last"):
        win_wait(last)

        pl.when(chip >= 0)(lambda: gather(last))

        @alone
        def _():
            for e in range(local_e):
                up = acc[e] + jnp.dot(xg[e], win_buf[last % IN_DEPTH, e], preferred_element_type=F32)
                hid[e] = jax.nn.gelu(up).astype(BF16)

    def rcopy(kind, oc, src, dst, to):
        ssem = r_ssem.at[lax.rem(oc, 2)] if kind == PART else r_ssem.at[kind + 1]
        group = 0 if kind == PART else 1 if kind in (FAR_R, FAR_L) else 2
        return pltpu.make_async_remote_copy(
            src_ref=src, dst_ref=dst, send_sem=ssem, recv_sem=r_rsem.at[group, oc],
            device_id={AXIS: to}, device_id_type=MESH)

    def r_copy(kind, oc):
        if kind == PART:
            return rcopy(kind, oc, part_send.at[lax.rem(oc, 2)], part_recv.at[oc], buddy)
        if kind == FAR_R:
            return rcopy(kind, oc, total.at[oc, c_far, 0], far_recv.at[oc, 0], right)
        if kind == FAR_L:
            return rcopy(kind, oc, total.at[oc, c_far, 1], far_recv.at[oc, 1], left)
        if kind == NEAR_R:
            return rcopy(kind, oc, total.at[oc, c_right, 1], fin_recv.at[oc, 0, 1], right)
        if kind == NEAR_L:
            return rcopy(kind, oc, total.at[oc, c_left, 0], fin_recv.at[oc, 1, 0], left)
        if kind == MIX_R:
            return rcopy(kind, oc, total.at[oc, c_right, 0], fin_recv.at[oc, 0, 0], right)
        return rcopy(kind, oc, total.at[oc, c_left, 1], fin_recv.at[oc, 1, 1], left)

    rows = chips * tokens
    half = OUT_COLS // 2

    def partial(rail, obuf, dst):
        at = pl.multiple_of(rail * rows, rows)
        val = jnp.dot(mix[0, pl.ds(at, rows), :], obuf[...], preferred_element_type=F32)
        val += jnp.dot(mix[1, pl.ds(at, rows), :], obuf[...], preferred_element_type=F32)
        val += jnp.dot(mix[2, pl.ds(at, rows), :], obuf[...], preferred_element_type=F32)
        for t in range(chips):
            for h in range(2):
                dst[t, h] = val[t * tokens:(t + 1) * tokens, h * half:(h + 1) * half]

    def finish_far(oc):
        rcopy(FAR_R, oc, far_recv.at[oc], far_recv.at[oc], buddy).wait_recv()
        total[oc, c_right, 0] = total[oc, c_right, 0] + far_recv[oc, 0]
        r_copy(MIX_R, oc).start()
        total[oc, c_left, 1] = total[oc, c_left, 1] + far_recv[oc, 1]
        r_copy(MIX_L, oc).start()

    per_in = kc_n // OUT_COLS

    def finish(oc):
        rcopy(NEAR_R, oc, fin_recv.at[oc], fin_recv.at[oc], buddy).wait_recv()
        for h in range(2):
            at = pl.multiple_of(lax.rem(oc, per_in) * OUT_COLS + h * half, half)
            x_own = x_all[oc // per_in, pl.ds(pl.multiple_of(me * tokens, tokens), tokens), pl.ds(at, half)]
            val = total[oc, chip, h] + fin_recv[oc, 0, h] + fin_recv[oc, 1, h]
            to = pl.multiple_of(oc * OUT_COLS + h * half, half)
            out_ref[:, pl.ds(to, half)] = (x_own.astype(F32) + val).astype(BF16)

    def down(oc, obuf):
        for e in range(local_e):
            val = jnp.dot(hid[e], wout_buf[lax.rem(oc, OUT_DEPTH), e], preferred_element_type=F32)
            obuf[e * capacity:(e + 1) * capacity, :] = val.astype(BF16)

    def refill(oc):
        for e in range(local_e):
            wout_copy(e, oc).start()

    def share(oc, now, after):
        @pl.when(oc >= 2)
        def _():
            r_copy(PART, oc - 2).wait_send()

        with jax.named_scope("partA"):
            alone(lambda: partial(other, now, part_send.at[lax.rem(oc, 2)]))
            r_copy(PART, oc).start()
        with jax.named_scope("partB"):
            @alone
            def _():
                partial(core, now, total.at[oc])
                after()
        with jax.named_scope("part_wait"):
            r_copy(PART, oc).wait_recv()
        total[oc] = total[oc] + part_recv[oc]
        for kind in (FAR_R, FAR_L, NEAR_R, NEAR_L):
            r_copy(kind, oc).start()

    def step(oc, now, nxt):
        if nxt is None:
            share(oc, now, lambda: None)
        else:
            wout_wait(oc + 1)
            share(oc, now, lambda: down(oc + 1, nxt))

            @pl.when(oc + 1 + OUT_DEPTH < oc_n)
            def _():
                refill(oc + 1 + OUT_DEPTH)
        with jax.named_scope("far"):
            finish_far(oc - 1)

        @pl.when(oc >= LAG)
        def _():
            with jax.named_scope("fin"):
                finish(oc - LAG)

    wout_wait(0)
    alone(lambda: down(0, obuf0))
    refill(OUT_DEPTH)
    share(0, obuf0, lambda: None)
    wout_wait(1)
    alone(lambda: down(1, obuf1))
    refill(OUT_DEPTH + 1)

    @pl.loop(0, oc_n // 2 - 1)
    def _(i):
        step(2 * i + 1, obuf1, obuf0)
        step(2 * i + 2, obuf0, obuf1)

    step(oc_n - 1, obuf1, None)

    for kind, rows_sent in ((OWN_R, 2), (OWN_L, 2), (OWN_P, 2), (RELAY_R, 1), (RELAY_L, 1),
                            (FWD_L, 2), (FWD_R, 2), (FWD_A, 1), (FWD_B, 1)):
        d_flush(kind, rows_sent * tokens // 2)
    for c in meta_all():
        c.wait_send()

    with jax.named_scope("far_t"):
        finish_far(oc_n - 1)
    for oc in range(oc_n - LAG, oc_n):
        with jax.named_scope("fin_t"):
            finish(oc)

    with jax.named_scope("drain"):
        r_copy(PART, oc_n - 2).wait_send()
        r_copy(PART, oc_n - 1).wait_send()
        for kind in (FAR_R, FAR_L, NEAR_R, NEAR_L, MIX_R, MIX_L):
            sent = total.at[:, 0, 0]
            rcopy(kind, 0, sent, sent, buddy).wait_send()


def solution(mesh):
    n = mesh.shape[AXIS]
    row_spec = P(("data", AXIS), None)
    weight_spec = P(AXIS, None, None)

    def device_step(token_rows, expert_ids, gate_weights, w_in, w_out):
        tokens, top_k = expert_ids.shape
        local_e, model, hidden = w_in.shape
        capacity = n * tokens * top_k // (n * local_e)
        slots = local_e * capacity
        chips = n // 2
        kc_n = model // IN_BLOCKS
        oc_n = model // OUT_COLS
        half = OUT_COLS // 2
        hbm = pl.BlockSpec(memory_space=pl.ANY)
        dma = pltpu.SemaphoreType.DMA
        return pl.pallas_call(
            functools.partial(body, n, capacity),
            out_shape=jax.ShapeDtypeStruct((tokens, model), BF16),
            in_specs=[hbm, hbm, hbm, hbm, hbm],
            out_specs=pl.BlockSpec(memory_space=pltpu.VMEM),
            scratch_shapes=[
                pltpu.VMEM((n, top_k, tokens), jnp.int32),
                pltpu.VMEM((n, top_k, tokens), F32),
                pltpu.VMEM((IN_BLOCKS, n * tokens, kc_n), BF16),
                pltpu.VMEM((slots, n * tokens), BF16),
                pltpu.VMEM((n, 4 * local_e, tokens), F32),
                pltpu.VMEM((3, n * tokens, slots), BF16),
                pltpu.VMEM((local_e, capacity, kc_n), BF16),
                pltpu.VMEM((local_e, capacity, hidden), F32),
                pltpu.VMEM((local_e, capacity, hidden), BF16),
                pltpu.VMEM((LANES, 4 * slots), BF16),
                pltpu.VMEM((slots, OUT_COLS), BF16),
                pltpu.VMEM((slots, OUT_COLS), BF16),
                pltpu.VMEM((2, chips, 2, tokens, half), F32),
                pltpu.VMEM((oc_n, chips, 2, tokens, half), F32),
                pltpu.VMEM((oc_n, chips, 2, tokens, half), F32),
                pltpu.VMEM((oc_n, 2, tokens, half), F32),
                pltpu.VMEM((oc_n, 2, 2, tokens, half), F32),
                pltpu.VMEM((IN_DEPTH, local_e, kc_n, hidden), BF16),
                pltpu.VMEM((OUT_DEPTH, local_e, hidden, OUT_COLS), BF16),
                dma((2,)), dma((2,)),
                dma((9,)), dma((3, IN_BLOCKS)),
                dma((8,)), dma((3, oc_n)),
                dma,
                dma((IN_DEPTH,)),
                dma((OUT_DEPTH,)),
                dma((2,)),
            ],
            compiler_params=pltpu.CompilerParams(
                collective_id=0, has_side_effects=True, vmem_limit_bytes=VMEM_BYTES),
        )(expert_ids.T, gate_weights.T, token_rows, w_in, w_out)

    return jax.shard_map(device_step, mesh=mesh, in_specs=(row_spec, row_spec, row_spec, weight_spec, weight_spec),
                         out_specs=row_spec, check_vma=False)
```

```python
import functools

import jax
import jax.numpy as jnp
from jax import lax
from jax.experimental import pallas as pl
from jax.experimental.pallas import tpu as pltpu
from jax.sharding import PartitionSpec as P

MESH = pl.DeviceIdType.MESH
F32 = jnp.float32
BF16 = jnp.bfloat16
AXIS = "expert"
LANES = 128
IN_BLOCKS = 8
IN_DEPTH = 3
OUT_COLS = 256
OUT_DEPTH = 2
AHEAD = 3
LAG = 3
VMEM_BYTES = 62 * 2 ** 20
GELU_A = 0.7978845608028654
GELU_B = 0.044715 * GELU_A
BIG_BF16 = 3.3895313892515355e38

OWN_R, OWN_L, OWN_P, RELAY_R, RELAY_L, FWD_L, FWD_R, FWD_A, FWD_B = range(9)
PART, FAR_R, FAR_L, NEAR_R, NEAR_L, MIX_R, MIX_L, PART_REST = range(8)


def gelu(x):
    half = 0.5 * x
    return half + half * jnp.tanh(x * (GELU_A + GELU_B * (x * x)))


def body(n, capacity, ids_hbm, gate_hbm, x_hbm, w_in, w_out, out_ref,
         ids_all, gates_all, x_all, pick, packed, mix, xg, acc, hid, spread, obuf0, obuf1,
         part_send, part_recv, total, far_recv, fin_recv, win_buf, wout_buf,
         meta_ssem, meta_rsem, d_ssem, d_rsem, r_ssem, r_rsem, x_sem, win_sem, wout_sem, own_sem):
    top_k, tokens = ids_hbm.shape
    local_e, model, hidden = w_in.shape
    chips = n // 2
    kc_n = model // IN_BLOCKS
    oc_n = model // OUT_COLS
    slots = local_e * capacity

    me = lax.axis_index(AXIS)
    core = lax.rem(me, 2)
    chip = me // 2
    buddy = me + 1 - 2 * core
    other = 1 - core
    c_right = lax.rem(chip + 1, chips)
    c_far = lax.rem(chip + 2, chips)
    c_left = lax.rem(chip + 3, chips)

    def dev(c, k):
        return 2 * c + k

    right = dev(c_right, core)
    left = dev(c_left, core)

    def alone(fn):
        pl.when(me >= 0)(fn)

    def win_copy(e, kc):
        slot = lax.rem(kc, IN_DEPTH)
        return pltpu.make_async_copy(
            w_in.at[e, pl.ds(kc * kc_n, kc_n), :], win_buf.at[slot, e], win_sem.at[slot])

    def win_wait(kc):
        slot = lax.rem(kc, IN_DEPTH)
        pltpu.make_async_copy(w_in.at[:, pl.ds(0, kc_n), :], win_buf.at[slot], win_sem.at[slot]).wait()

    def wout_copy(e, oc):
        slot = lax.rem(oc, OUT_DEPTH)
        return pltpu.make_async_copy(
            w_out.at[e, :, pl.ds(oc * OUT_COLS, OUT_COLS)], wout_buf.at[slot, e], wout_sem.at[slot])

    def wout_wait(oc):
        slot = lax.rem(oc, OUT_DEPTH)
        pltpu.make_async_copy(w_out.at[:, :, pl.ds(0, OUT_COLS)], wout_buf.at[slot], wout_sem.at[slot]).wait()

    def x_rows(kc, d):
        return x_all.at[kc, pl.ds(d * tokens, tokens), :]

    def x_half(kc, d, h):
        half = tokens // 2
        return x_all.at[kc, pl.ds(d * tokens + h * half, half), :]

    def x_copy(kc):
        return pltpu.make_async_copy(
            x_hbm.at[:, pl.ds(kc * kc_n, kc_n)], x_rows(kc, me), x_sem)

    barrier = pltpu.get_barrier_semaphore()
    for d in range(1, n):
        pl.semaphore_signal(barrier, inc=1, device_id={AXIS: lax.rem(me + d, n)}, device_id_type=MESH)

    own_meta = (
        pltpu.make_async_copy(ids_hbm, ids_all.at[me], own_sem.at[0]),
        pltpu.make_async_copy(gate_hbm, gates_all.at[me], own_sem.at[1]),
    )
    for c in own_meta:
        c.start()
    for kc in range(IN_BLOCKS):
        x_copy(kc).start()

    @pl.loop(0, IN_DEPTH)
    def _(kc):
        for e in range(local_e):
            win_copy(e, kc).start()

    @pl.loop(0, OUT_DEPTH)
    def _(oc):
        for e in range(local_e):
            wout_copy(e, oc).start()

    with jax.named_scope("barrier"):
        pl.semaphore_wait(barrier, n - 1)
        for c in own_meta:
            c.wait()

    def meta_copies(d):
        to = lax.rem(me + d, n)
        return (
            pltpu.make_async_remote_copy(
                src_ref=ids_all.at[me], dst_ref=ids_all.at[me], send_sem=meta_ssem.at[0], recv_sem=meta_rsem.at[0],
                device_id={AXIS: to}, device_id_type=MESH),
            pltpu.make_async_remote_copy(
                src_ref=gates_all.at[me], dst_ref=gates_all.at[me], send_sem=meta_ssem.at[1], recv_sem=meta_rsem.at[1],
                device_id={AXIS: to}, device_id_type=MESH),
        )

    def meta_all():
        ids_part, gates_part = ids_all.at[pl.ds(0, n - 1)], gates_all.at[pl.ds(0, n - 1)]
        return (
            pltpu.make_async_remote_copy(
                src_ref=ids_part, dst_ref=ids_part, send_sem=meta_ssem.at[0], recv_sem=meta_rsem.at[0],
                device_id={AXIS: buddy}, device_id_type=MESH),
            pltpu.make_async_remote_copy(
                src_ref=gates_part, dst_ref=gates_part, send_sem=meta_ssem.at[1], recv_sem=meta_rsem.at[1],
                device_id={AXIS: buddy}, device_id_type=MESH),
        )

    for d in range(1, n):
        for c in meta_copies(d):
            c.start()

    def dcopy(kind, kc, ref, to):
        group = 0 if kind in (OWN_R, OWN_L) else 1 if kind in (RELAY_R, RELAY_L) else 2
        return pltpu.make_async_remote_copy(
            src_ref=ref, dst_ref=ref, send_sem=d_ssem.at[kind], recv_sem=d_rsem.at[group, kc],
            device_id={AXIS: to}, device_id_type=MESH)

    def d_wait(kind, kc, rows):
        dcopy(kind, kc, x_all.at[kc, pl.ds(0, rows), :], buddy).wait_recv()

    def d_flush(kind, rows):
        dcopy(kind, 0, x_all.at[:, pl.ds(0, rows), :], buddy).wait_send()

    far = dev(c_far, core)

    def d_sent(kind, kc):
        if kind == OWN_R:
            return dcopy(kind, kc, x_rows(kc, me), right)
        if kind == OWN_L:
            return dcopy(kind, kc, x_rows(kc, me), left)
        if kind == OWN_P:
            return dcopy(kind, kc, x_rows(kc, me), buddy)
        if kind == RELAY_R:
            return dcopy(kind, kc, x_half(kc, left, 0), right)
        if kind == RELAY_L:
            return dcopy(kind, kc, x_half(kc, right, 1), left)
        if kind == FWD_L:
            return dcopy(kind, kc, x_rows(kc, left), buddy)
        if kind == FWD_R:
            return dcopy(kind, kc, x_rows(kc, right), buddy)
        if kind == FWD_A:
            return dcopy(kind, kc, x_half(kc, far, 0), buddy)
        return dcopy(kind, kc, x_half(kc, far, 1), buddy)

    def send_own(kc):
        for kind in (OWN_R, OWN_L, OWN_P):
            d_sent(kind, kc).start()

    def stage1(kc):
        d_wait(OWN_R, kc, 2 * tokens)
        for kind in (RELAY_R, RELAY_L, FWD_L, FWD_R):
            d_sent(kind, kc).start()

    def stage2(kc):
        d_wait(RELAY_R, kc, tokens)
        for kind in (FWD_A, FWD_B):
            d_sent(kind, kc).start()

    def stage3(kc):
        d_wait(OWN_P, kc, chips * tokens)

    with jax.named_scope("own"):
        mine = x_all.at[:, pl.ds(me * tokens, tokens), :]
        pltpu.make_async_copy(mine, mine, x_sem).wait()
        for kc in range(AHEAD):
            send_own(kc)

    with jax.named_scope("meta_wait"):
        for c in meta_all():
            c.wait_recv()

    sub = lax.broadcasted_iota(jnp.int32, (local_e, tokens), 0) + me * local_e
    hit = {}
    for b in range(n):
        for j in range(top_k):
            hit[b, j] = jnp.where(ids_all[b, j:j + 1, :] == sub, 1.0, 0.0).astype(F32)
    hits = jnp.concatenate([hit[b, j] for b in range(n) for j in range(top_k)], axis=0).astype(BF16)
    t_from = lax.broadcasted_iota(jnp.int32, (tokens, tokens), 0)
    t_to = lax.broadcasted_iota(jnp.int32, (tokens, tokens), 1)
    earlier = jnp.where(t_from < t_to, 1.0, 0.0).astype(BF16)
    ones = jnp.full((tokens, tokens), 1.0, BF16)
    within = jnp.dot(hits, earlier, preferred_element_type=F32)
    sums = jnp.dot(hits, ones, preferred_element_type=F32)
    running = jnp.zeros((local_e, tokens), F32)
    rank = [jnp.zeros((local_e, tokens), F32) for _ in range(n)]
    for j in range(top_k):
        for b in range(n):
            at = (b * top_k + j) * local_e
            rank[b] = rank[b] + hit[b, j] * (running + within[at:at + local_e])
            running = running + sums[at:at + local_e]
    slot_row = lax.broadcasted_iota(jnp.int32, (capacity, tokens), 0).astype(F32)
    for b in range(n):
        has = jnp.zeros((local_e, tokens), F32)
        gate = jnp.zeros((local_e, tokens), F32)
        for j in range(top_k):
            has = has + hit[b, j]
            gate = gate + hit[b, j] * gates_all[b, j:j + 1, :]
        slot = jnp.where((has > 0.0) & (rank[b] < capacity), rank[b], -1.0)
        g1 = jnp.minimum(gate, BIG_BF16).astype(BF16).astype(F32)
        g2 = (gate - g1).astype(BF16).astype(F32)
        g3 = gate - g1 - g2
        packed[b] = jnp.concatenate([slot, g1, g2, g3], axis=0)
        for e in range(local_e):
            pick[e * capacity:(e + 1) * capacity, b * tokens:(b + 1) * tokens] = jnp.where(
                slot[e:e + 1, :] == slot_row, 1.0, 0.0).astype(BF16)

    acc[...] = jnp.zeros_like(acc)

    part_c = 2 * LANES
    for q in range(4):
        at = lax.broadcasted_iota(jnp.int32, (LANES, slots), 1)
        row = lax.broadcasted_iota(jnp.int32, (LANES, slots), 0) - q * local_e
        spread[:, q * slots:(q + 1) * slots] = jnp.where(
            (at >= row * capacity) & (at < (row + 1) * capacity) & (row >= 0) & (row < local_e), 1.0, 0.0).astype(BF16)

    def mix_rows(b):
        row = pl.multiple_of((lax.rem(b, 2) * chips + b // 2) * tokens, tokens)
        cols = jnp.concatenate(
            [packed[b], jnp.zeros((LANES - 4 * local_e, tokens), F32)], axis=0).T.astype(BF16)
        for p in range(slots // part_c):
            at = lax.broadcasted_iota(jnp.int32, (1, part_c), 1) + p * part_c
            rel = at
            for e in range(1, local_e):
                rel = jnp.where(at >= e * capacity, at - e * capacity, rel)
            rel = rel.astype(F32)

            def repeat(q):
                return jnp.dot(cols, spread[:, q * slots + p * part_c:q * slots + (p + 1) * part_c],
                               preferred_element_type=F32)

            slot_at = repeat(0)
            for k in range(3):
                mix[k, pl.ds(row, tokens), p * part_c:(p + 1) * part_c] = jnp.where(
                    slot_at == rel, repeat(k + 1), 0.0).astype(BF16)

    def mix_range(lo, hi):
        with jax.named_scope("mix"):
            pl.loop(lo, hi)(mix_rows)

    with jax.named_scope("s1"):
        stage1(0)
        send_own(AHEAD)
    mix_range(0, n // 2)
    with jax.named_scope("s1"):
        stage1(1)
        send_own(AHEAD + 1)
    with jax.named_scope("s2"):
        stage2(0)
    mix_range(n // 2, n - 2)

    def gather(kc):
        xg[...] = jnp.dot(pick[...], x_all[kc], preferred_element_type=F32).astype(BF16).reshape(local_e, capacity, kc_n)

    with jax.named_scope("s1"):
        stage1(2)
        send_own(AHEAD + 2)

    @pl.loop(0, IN_BLOCKS - 1)
    def _(kc):
        with jax.named_scope("s1"):
            @pl.when(kc + 3 < IN_BLOCKS)
            def _():
                stage1(kc + 3)

            @pl.when(kc + 3 + AHEAD < IN_BLOCKS)
            def _():
                send_own(kc + 3 + AHEAD)

        with jax.named_scope("s2"):
            stage2(kc + 1)
        with jax.named_scope("s3"):
            stage3(kc)

        with jax.named_scope("up"):
            win_wait(kc)

            pl.when(chip >= 0)(lambda: gather(kc))

            @alone
            def _():
                for e in range(local_e):
                    acc[e] = acc[e] + jnp.dot(xg[e], win_buf[lax.rem(kc, IN_DEPTH), e], preferred_element_type=F32)

            @pl.when(kc + IN_DEPTH < IN_BLOCKS)
            def _():
                for e in range(local_e):
                    win_copy(e, kc + IN_DEPTH).start()

        @pl.when(kc == 0)
        def _():
            mix_range(n - 2, n)

    last = IN_BLOCKS - 1
    with jax.named_scope("s3"):
        stage3(last)
    with jax.named_scope("up_last"):
        win_wait(last)

        pl.when(chip >= 0)(lambda: gather(last))

        @alone
        def _():
            for e in range(local_e):
                up = acc[e] + jnp.dot(xg[e], win_buf[last % IN_DEPTH, e], preferred_element_type=F32)
                hid[e] = gelu(up).astype(BF16)

    def rcopy(kind, oc, src, dst, to):
        ssem = r_ssem.at[lax.rem(oc, 2)] if kind in (PART, PART_REST) else r_ssem.at[kind + 1]
        group = 0 if kind == PART else 1 if kind in (FAR_R, FAR_L) else 2 if kind != PART_REST else 3
        return pltpu.make_async_remote_copy(
            src_ref=src, dst_ref=dst, send_sem=ssem, recv_sem=r_rsem.at[group, oc],
            device_id={AXIS: to}, device_id_type=MESH)

    def r_copy(kind, oc):
        if kind == PART:
            return rcopy(kind, oc, part_send.at[lax.rem(oc, 2), c_far], part_recv.at[oc, c_far], buddy)
        if kind == FAR_R:
            return rcopy(kind, oc, total.at[oc, c_far, 0], far_recv.at[oc, 0], right)
        if kind == FAR_L:
            return rcopy(kind, oc, total.at[oc, c_far, 1], far_recv.at[oc, 1], left)
        if kind == NEAR_R:
            return rcopy(kind, oc, total.at[oc, c_right, 1], fin_recv.at[oc, 0, 1], right)
        if kind == NEAR_L:
            return rcopy(kind, oc, total.at[oc, c_left, 0], fin_recv.at[oc, 1, 0], left)
        if kind == MIX_R:
            return rcopy(kind, oc, total.at[oc, c_right, 0], fin_recv.at[oc, 0, 0], right)
        return rcopy(kind, oc, total.at[oc, c_left, 1], fin_recv.at[oc, 1, 1], left)

    rows = chips * tokens
    half = OUT_COLS // 2

    def partial(rail, obuf, dst):
        at = pl.multiple_of(rail * rows, rows)
        val = jnp.dot(mix[0, pl.ds(at, rows), :], obuf[...], preferred_element_type=F32)
        val += jnp.dot(mix[1, pl.ds(at, rows), :], obuf[...], preferred_element_type=F32)
        val += jnp.dot(mix[2, pl.ds(at, rows), :], obuf[...], preferred_element_type=F32)
        for t in range(chips):
            for h in range(2):
                dst[t, h] = val[t * tokens:(t + 1) * tokens, h * half:(h + 1) * half]

    def finish_far(oc):
        rcopy(FAR_R, oc, far_recv.at[oc], far_recv.at[oc], buddy).wait_recv()
        total[oc, c_right, 0] = total[oc, c_right, 0] + far_recv[oc, 0]
        r_copy(MIX_R, oc).start()
        total[oc, c_left, 1] = total[oc, c_left, 1] + far_recv[oc, 1]
        r_copy(MIX_L, oc).start()

    per_in = kc_n // OUT_COLS

    def finish(oc):
        rcopy(NEAR_R, oc, fin_recv.at[oc], fin_recv.at[oc], buddy).wait_recv()
        for h in range(2):
            at = pl.multiple_of(lax.rem(oc, per_in) * OUT_COLS + h * half, half)
            x_own = x_all[oc // per_in, pl.ds(pl.multiple_of(me * tokens, tokens), tokens), pl.ds(at, half)]
            val = total[oc, chip, h] + fin_recv[oc, 0, h] + fin_recv[oc, 1, h]
            to = pl.multiple_of(oc * OUT_COLS + h * half, half)
            out_ref[:, pl.ds(to, half)] = (x_own.astype(F32) + val).astype(BF16)

    def down(oc, obuf):
        for e in range(local_e):
            val = jnp.dot(hid[e], wout_buf[lax.rem(oc, OUT_DEPTH), e], preferred_element_type=F32)
            obuf[e * capacity:(e + 1) * capacity, :] = val.astype(BF16)

    def refill(oc):
        for e in range(local_e):
            wout_copy(e, oc).start()

    def part_sent(oc):
        sent = part_send.at[lax.rem(oc, 2)]
        rcopy(PART, oc, sent, sent, buddy).wait_send()

    def share(oc, now, after):
        @pl.when(oc >= 2)
        def _():
            part_sent(oc - 2)

        with jax.named_scope("partA"):
            alone(lambda: partial(other, now, part_send.at[lax.rem(oc, 2)]))
            r_copy(PART, oc).start()
            for t in (c_right, c_left, chip):
                rcopy(PART_REST, oc, part_send.at[lax.rem(oc, 2), t], part_recv.at[oc, t], buddy).start()
        with jax.named_scope("partB"):
            @alone
            def _():
                partial(core, now, total.at[oc])
                after()
        with jax.named_scope("part_wait"):
            r_copy(PART, oc).wait_recv()
        total[oc, c_far] = total[oc, c_far] + part_recv[oc, c_far]
        for kind in (FAR_R, FAR_L):
            r_copy(kind, oc).start()
        with jax.named_scope("rest_wait"):
            rest = part_recv.at[oc, pl.ds(0, chips - 1)]
            rcopy(PART_REST, oc, rest, rest, buddy).wait_recv()
        for t in (c_right, c_left, chip):
            total[oc, t] = total[oc, t] + part_recv[oc, t]
        for kind in (NEAR_R, NEAR_L):
            r_copy(kind, oc).start()

    def step(oc, now, nxt):
        if nxt is None:
            share(oc, now, lambda: None)
        else:
            wout_wait(oc + 1)
            share(oc, now, lambda: down(oc + 1, nxt))

            @pl.when(oc + 1 + OUT_DEPTH < oc_n)
            def _():
                refill(oc + 1 + OUT_DEPTH)
        with jax.named_scope("far"):
            finish_far(oc - 1)

        @pl.when(oc >= LAG)
        def _():
            with jax.named_scope("fin"):
                finish(oc - LAG)

    wout_wait(0)
    alone(lambda: down(0, obuf0))
    refill(OUT_DEPTH)
    share(0, obuf0, lambda: None)
    wout_wait(1)
    alone(lambda: down(1, obuf1))
    refill(OUT_DEPTH + 1)

    @pl.loop(0, oc_n // 2 - 1)
    def _(i):
        step(2 * i + 1, obuf1, obuf0)
        step(2 * i + 2, obuf0, obuf1)

    step(oc_n - 1, obuf1, None)

    for kind, rows_sent in ((OWN_R, 2), (OWN_L, 2), (OWN_P, 2), (RELAY_R, 1), (RELAY_L, 1),
                            (FWD_L, 2), (FWD_R, 2), (FWD_A, 1), (FWD_B, 1)):
        d_flush(kind, rows_sent * tokens // 2)
    for c in meta_all():
        c.wait_send()

    with jax.named_scope("far_t"):
        finish_far(oc_n - 1)
    for oc in range(oc_n - LAG, oc_n):
        with jax.named_scope("fin_t"):
            finish(oc)

    with jax.named_scope("drain"):
        part_sent(oc_n - 2)
        part_sent(oc_n - 1)
        for kind in (FAR_R, FAR_L, NEAR_R, NEAR_L, MIX_R, MIX_L):
            sent = total.at[:, 0, 0]
            rcopy(kind, 0, sent, sent, buddy).wait_send()


def solution(mesh):
    n = mesh.shape[AXIS]
    row_spec = P(("data", AXIS), None)
    weight_spec = P(AXIS, None, None)

    def device_step(token_rows, expert_ids, gate_weights, w_in, w_out):
        tokens, top_k = expert_ids.shape
        local_e, model, hidden = w_in.shape
        capacity = n * tokens * top_k // (n * local_e)
        slots = local_e * capacity
        chips = n // 2
        kc_n = model // IN_BLOCKS
        oc_n = model // OUT_COLS
        half = OUT_COLS // 2
        hbm = pl.BlockSpec(memory_space=pl.ANY)
        dma = pltpu.SemaphoreType.DMA
        return pl.pallas_call(
            functools.partial(body, n, capacity),
            out_shape=jax.ShapeDtypeStruct((tokens, model), BF16),
            in_specs=[hbm, hbm, hbm, hbm, hbm],
            out_specs=pl.BlockSpec(memory_space=pltpu.VMEM),
            scratch_shapes=[
                pltpu.VMEM((n, top_k, tokens), jnp.int32),
                pltpu.VMEM((n, top_k, tokens), F32),
                pltpu.VMEM((IN_BLOCKS, n * tokens, kc_n), BF16),
                pltpu.VMEM((slots, n * tokens), BF16),
                pltpu.VMEM((n, 4 * local_e, tokens), F32),
                pltpu.VMEM((3, n * tokens, slots), BF16),
                pltpu.VMEM((local_e, capacity, kc_n), BF16),
                pltpu.VMEM((local_e, capacity, hidden), F32),
                pltpu.VMEM((local_e, capacity, hidden), BF16),
                pltpu.VMEM((LANES, 4 * slots), BF16),
                pltpu.VMEM((slots, OUT_COLS), BF16),
                pltpu.VMEM((slots, OUT_COLS), BF16),
                pltpu.VMEM((2, chips, 2, tokens, half), F32),
                pltpu.VMEM((oc_n, chips, 2, tokens, half), F32),
                pltpu.VMEM((oc_n, chips, 2, tokens, half), F32),
                pltpu.VMEM((oc_n, 2, tokens, half), F32),
                pltpu.VMEM((oc_n, 2, 2, tokens, half), F32),
                pltpu.VMEM((IN_DEPTH, local_e, kc_n, hidden), BF16),
                pltpu.VMEM((OUT_DEPTH, local_e, hidden, OUT_COLS), BF16),
                dma((2,)), dma((2,)),
                dma((9,)), dma((3, IN_BLOCKS)),
                dma((8,)), dma((4, oc_n)),
                dma,
                dma((IN_DEPTH,)),
                dma((OUT_DEPTH,)),
                dma((2,)),
            ],
            compiler_params=pltpu.CompilerParams(
                collective_id=0, has_side_effects=True, vmem_limit_bytes=VMEM_BYTES),
        )(expert_ids.T, gate_weights.T, token_rows, w_in, w_out)

    return jax.shard_map(device_step, mesh=mesh, in_specs=(row_spec, row_spec, row_spec, weight_spec, weight_spec),
                         out_specs=row_spec, check_vma=False)
```

```python
import functools

import jax
import jax.numpy as jnp
from jax import lax
from jax.experimental import pallas as pl
from jax.experimental.pallas import tpu as pltpu
from jax.sharding import PartitionSpec as P

MESH = pl.DeviceIdType.MESH
F32 = jnp.float32
BF16 = jnp.bfloat16
AXIS = "expert"
LANES = 128
IN_BLOCKS = 8
IN_DEPTH = 3
OUT_COLS = 256
OUT_DEPTH = 2
AHEAD = 3
LAG = 3
VMEM_BYTES = 62 * 2 ** 20
GELU_A = 0.7978845608028654
GELU_B = 0.044715 * GELU_A
PICK_PARTS = 4
BIG_BF16 = 3.3895313892515355e38

OWN_R, OWN_L, OWN_P, RELAY_R, RELAY_L, FWD_L, FWD_R, FWD_A, FWD_B = range(9)
PART, FAR_R, FAR_L, NEAR_R, NEAR_L, MIX_R, MIX_L, PART_REST = range(8)


def gelu(x):
    half = 0.5 * x
    return half + half * jnp.tanh(x * (GELU_A + GELU_B * (x * x)))


def body(n, capacity, ids_hbm, gate_hbm, x_hbm, w_in, w_out, out_ref,
         ids_all, gates_all, x_all, pick, packed, mix, xg, acc, hid, spread, obuf0, obuf1,
         part_send, part_recv, total, far_recv, fin_recv, win_buf, wout_buf,
         meta_ssem, meta_rsem, d_ssem, d_rsem, r_ssem, r_rsem, x_sem, win_sem, wout_sem, own_sem):
    top_k, tokens = ids_hbm.shape
    local_e, model, hidden = w_in.shape
    chips = n // 2
    kc_n = model // IN_BLOCKS
    oc_n = model // OUT_COLS
    slots = local_e * capacity

    me = lax.axis_index(AXIS)
    core = lax.rem(me, 2)
    chip = me // 2
    buddy = me + 1 - 2 * core
    other = 1 - core
    c_right = lax.rem(chip + 1, chips)
    c_far = lax.rem(chip + 2, chips)
    c_left = lax.rem(chip + 3, chips)

    def dev(c, k):
        return 2 * c + k

    right = dev(c_right, core)
    left = dev(c_left, core)

    def alone(fn):
        pl.when(me >= 0)(fn)

    def win_copy(e, kc):
        slot = lax.rem(kc, IN_DEPTH)
        return pltpu.make_async_copy(
            w_in.at[e, pl.ds(kc * kc_n, kc_n), :], win_buf.at[slot, e], win_sem.at[slot])

    def win_wait(kc):
        slot = lax.rem(kc, IN_DEPTH)
        pltpu.make_async_copy(w_in.at[:, pl.ds(0, kc_n), :], win_buf.at[slot], win_sem.at[slot]).wait()

    def wout_copy(e, oc):
        slot = lax.rem(oc, OUT_DEPTH)
        return pltpu.make_async_copy(
            w_out.at[e, :, pl.ds(oc * OUT_COLS, OUT_COLS)], wout_buf.at[slot, e], wout_sem.at[slot])

    def wout_wait(oc):
        slot = lax.rem(oc, OUT_DEPTH)
        pltpu.make_async_copy(w_out.at[:, :, pl.ds(0, OUT_COLS)], wout_buf.at[slot], wout_sem.at[slot]).wait()

    def x_rows(kc, d):
        return x_all.at[kc, pl.ds(d * tokens, tokens), :]

    def x_half(kc, d, h):
        half = tokens // 2
        return x_all.at[kc, pl.ds(d * tokens + h * half, half), :]

    def x_copy(kc):
        return pltpu.make_async_copy(
            x_hbm.at[:, pl.ds(kc * kc_n, kc_n)], x_rows(kc, me), x_sem)

    barrier = pltpu.get_barrier_semaphore()
    for d in range(1, n):
        pl.semaphore_signal(barrier, inc=1, device_id={AXIS: lax.rem(me + d, n)}, device_id_type=MESH)

    own_meta = (
        pltpu.make_async_copy(ids_hbm, ids_all.at[me], own_sem.at[0]),
        pltpu.make_async_copy(gate_hbm, gates_all.at[me], own_sem.at[1]),
    )
    for c in own_meta:
        c.start()
    for kc in range(IN_BLOCKS):
        x_copy(kc).start()

    @pl.loop(0, IN_DEPTH)
    def _(kc):
        for e in range(local_e):
            win_copy(e, kc).start()

    @pl.loop(0, OUT_DEPTH)
    def _(oc):
        for e in range(local_e):
            wout_copy(e, oc).start()

    with jax.named_scope("barrier"):
        pl.semaphore_wait(barrier, n - 1)
        for c in own_meta:
            c.wait()

    def meta_copies(d):
        to = lax.rem(me + d, n)
        return (
            pltpu.make_async_remote_copy(
                src_ref=ids_all.at[me], dst_ref=ids_all.at[me], send_sem=meta_ssem.at[0], recv_sem=meta_rsem.at[0],
                device_id={AXIS: to}, device_id_type=MESH),
            pltpu.make_async_remote_copy(
                src_ref=gates_all.at[me], dst_ref=gates_all.at[me], send_sem=meta_ssem.at[1], recv_sem=meta_rsem.at[1],
                device_id={AXIS: to}, device_id_type=MESH),
        )

    def meta_all():
        ids_part, gates_part = ids_all.at[pl.ds(0, n - 1)], gates_all.at[pl.ds(0, n - 1)]
        return (
            pltpu.make_async_remote_copy(
                src_ref=ids_part, dst_ref=ids_part, send_sem=meta_ssem.at[0], recv_sem=meta_rsem.at[0],
                device_id={AXIS: buddy}, device_id_type=MESH),
            pltpu.make_async_remote_copy(
                src_ref=gates_part, dst_ref=gates_part, send_sem=meta_ssem.at[1], recv_sem=meta_rsem.at[1],
                device_id={AXIS: buddy}, device_id_type=MESH),
        )

    for d in range(1, n):
        for c in meta_copies(d):
            c.start()

    def dcopy(kind, kc, ref, to):
        group = 0 if kind in (OWN_R, OWN_L) else 1 if kind in (RELAY_R, RELAY_L) else 2
        return pltpu.make_async_remote_copy(
            src_ref=ref, dst_ref=ref, send_sem=d_ssem.at[kind], recv_sem=d_rsem.at[group, kc],
            device_id={AXIS: to}, device_id_type=MESH)

    def d_wait(kind, kc, rows):
        dcopy(kind, kc, x_all.at[kc, pl.ds(0, rows), :], buddy).wait_recv()

    def d_flush(kind, rows):
        dcopy(kind, 0, x_all.at[:, pl.ds(0, rows), :], buddy).wait_send()

    far = dev(c_far, core)

    def d_sent(kind, kc):
        if kind == OWN_R:
            return dcopy(kind, kc, x_rows(kc, me), right)
        if kind == OWN_L:
            return dcopy(kind, kc, x_rows(kc, me), left)
        if kind == OWN_P:
            return dcopy(kind, kc, x_rows(kc, me), buddy)
        if kind == RELAY_R:
            return dcopy(kind, kc, x_half(kc, left, 0), right)
        if kind == RELAY_L:
            return dcopy(kind, kc, x_half(kc, right, 1), left)
        if kind == FWD_L:
            return dcopy(kind, kc, x_rows(kc, left), buddy)
        if kind == FWD_R:
            return dcopy(kind, kc, x_rows(kc, right), buddy)
        if kind == FWD_A:
            return dcopy(kind, kc, x_half(kc, far, 0), buddy)
        return dcopy(kind, kc, x_half(kc, far, 1), buddy)

    def send_own(kc):
        for kind in (OWN_R, OWN_L, OWN_P):
            d_sent(kind, kc).start()

    def stage1(kc):
        d_wait(OWN_R, kc, 2 * tokens)
        for kind in (RELAY_R, RELAY_L, FWD_L, FWD_R):
            d_sent(kind, kc).start()

    def stage2(kc):
        d_wait(RELAY_R, kc, tokens)
        for kind in (FWD_A, FWD_B):
            d_sent(kind, kc).start()

    def stage3(kc):
        d_wait(OWN_P, kc, chips * tokens)

    with jax.named_scope("own"):
        mine = x_all.at[:, pl.ds(me * tokens, tokens), :]
        pltpu.make_async_copy(mine, mine, x_sem).wait()
        for kc in range(AHEAD):
            send_own(kc)

    with jax.named_scope("meta_wait"):
        for c in meta_all():
            c.wait_recv()

    sub = lax.broadcasted_iota(jnp.int32, (local_e, tokens), 0) + me * local_e
    hit = {}
    for b in range(n):
        for j in range(top_k):
            hit[b, j] = jnp.where(ids_all[b, j:j + 1, :] == sub, 1.0, 0.0).astype(F32)
    hits = jnp.concatenate([hit[b, j] for b in range(n) for j in range(top_k)], axis=0).astype(BF16)
    t_from = lax.broadcasted_iota(jnp.int32, (tokens, tokens), 0)
    t_to = lax.broadcasted_iota(jnp.int32, (tokens, tokens), 1)
    earlier = jnp.where(t_from < t_to, 1.0, 0.0).astype(BF16)
    ones = jnp.full((tokens, tokens), 1.0, BF16)
    within = jnp.dot(hits, earlier, preferred_element_type=F32)
    sums = jnp.dot(hits, ones, preferred_element_type=F32)
    running = jnp.zeros((local_e, tokens), F32)
    rank = [jnp.zeros((local_e, tokens), F32) for _ in range(n)]
    for j in range(top_k):
        for b in range(n):
            at = (b * top_k + j) * local_e
            rank[b] = rank[b] + hit[b, j] * (running + within[at:at + local_e])
            running = running + sums[at:at + local_e]
    slot_row = lax.broadcasted_iota(jnp.int32, (capacity, tokens), 0).astype(F32)
    for b in range(n):
        has = jnp.zeros((local_e, tokens), F32)
        gate = jnp.zeros((local_e, tokens), F32)
        for j in range(top_k):
            has = has + hit[b, j]
            gate = gate + hit[b, j] * gates_all[b, j:j + 1, :]
        slot = jnp.where((has > 0.0) & (rank[b] < capacity), rank[b], -1.0)
        g1 = jnp.minimum(gate, BIG_BF16).astype(BF16).astype(F32)
        g2 = (gate - g1).astype(BF16).astype(F32)
        g3 = gate - g1 - g2
        packed[b] = jnp.concatenate([slot, g1, g2, g3], axis=0)
        for e in range(local_e):
            pick[e * capacity:(e + 1) * capacity, b * tokens:(b + 1) * tokens] = jnp.where(
                slot[e:e + 1, :] == slot_row, 1.0, 0.0).astype(BF16)

    acc[...] = jnp.zeros_like(acc)

    part_c = 2 * LANES
    for q in range(4):
        at = lax.broadcasted_iota(jnp.int32, (LANES, slots), 1)
        row = lax.broadcasted_iota(jnp.int32, (LANES, slots), 0) - q * local_e
        spread[:, q * slots:(q + 1) * slots] = jnp.where(
            (at >= row * capacity) & (at < (row + 1) * capacity) & (row >= 0) & (row < local_e), 1.0, 0.0).astype(BF16)

    def mix_rows(b):
        row = pl.multiple_of((lax.rem(b, 2) * chips + b // 2) * tokens, tokens)
        cols = jnp.concatenate(
            [packed[b], jnp.zeros((LANES - 4 * local_e, tokens), F32)], axis=0).T.astype(BF16)
        for p in range(slots // part_c):
            at = lax.broadcasted_iota(jnp.int32, (1, part_c), 1) + p * part_c
            rel = at
            for e in range(1, local_e):
                rel = jnp.where(at >= e * capacity, at - e * capacity, rel)
            rel = rel.astype(F32)

            def repeat(q):
                return jnp.dot(cols, spread[:, q * slots + p * part_c:q * slots + (p + 1) * part_c],
                               preferred_element_type=F32)

            slot_at = repeat(0)
            for k in range(3):
                mix[k, pl.ds(row, tokens), p * part_c:(p + 1) * part_c] = jnp.where(
                    slot_at == rel, repeat(k + 1), 0.0).astype(BF16)

    def mix_range(lo, hi):
        with jax.named_scope("mix"):
            pl.loop(lo, hi)(mix_rows)

    with jax.named_scope("s1"):
        stage1(0)
        send_own(AHEAD)
    mix_range(0, n // 2)
    with jax.named_scope("s1"):
        stage1(1)
        send_own(AHEAD + 1)
    with jax.named_scope("s2"):
        stage2(0)
    mix_range(n // 2, n)

    pick_rows = slots // PICK_PARTS

    def gather(kc):
        for i in range(PICK_PARTS):
            val = jnp.dot(pick[i * pick_rows:(i + 1) * pick_rows, :], x_all[kc], preferred_element_type=F32)
            xg[i * pick_rows // capacity:(i + 1) * pick_rows // capacity] = val.astype(BF16).reshape(
                pick_rows // capacity, capacity, kc_n)

    with jax.named_scope("s1"):
        stage1(2)
        send_own(AHEAD + 2)

    @pl.loop(0, IN_BLOCKS - 1)
    def _(kc):
        with jax.named_scope("s1"):
            @pl.when(kc + 3 < IN_BLOCKS)
            def _():
                stage1(kc + 3)

            @pl.when(kc + 3 + AHEAD < IN_BLOCKS)
            def _():
                send_own(kc + 3 + AHEAD)

        with jax.named_scope("s2"):
            stage2(kc + 1)
        with jax.named_scope("s3"):
            stage3(kc)

        with jax.named_scope("up"):
            win_wait(kc)

            @alone
            def _():
                gather(kc)
                for e in range(local_e):
                    acc[e] = acc[e] + jnp.dot(xg[e], win_buf[lax.rem(kc, IN_DEPTH), e], preferred_element_type=F32)

            @pl.when(kc + IN_DEPTH < IN_BLOCKS)
            def _():
                for e in range(local_e):
                    win_copy(e, kc + IN_DEPTH).start()

    last = IN_BLOCKS - 1
    with jax.named_scope("s3"):
        stage3(last)
    def rcopy(kind, oc, src, dst, to):
        ssem = r_ssem.at[lax.rem(oc, 2)] if kind in (PART, PART_REST) else r_ssem.at[kind + 1]
        group = 0 if kind == PART else 1 if kind in (FAR_R, FAR_L) else 2 if kind != PART_REST else 3
        return pltpu.make_async_remote_copy(
            src_ref=src, dst_ref=dst, send_sem=ssem, recv_sem=r_rsem.at[group, oc],
            device_id={AXIS: to}, device_id_type=MESH)

    def r_copy(kind, oc):
        if kind == PART:
            return rcopy(kind, oc, part_send.at[lax.rem(oc, 2), c_far], part_recv.at[oc, c_far], buddy)
        if kind == FAR_R:
            return rcopy(kind, oc, total.at[oc, c_far, 0], far_recv.at[oc, 0], right)
        if kind == FAR_L:
            return rcopy(kind, oc, total.at[oc, c_far, 1], far_recv.at[oc, 1], left)
        if kind == NEAR_R:
            return rcopy(kind, oc, total.at[oc, c_right, 1], fin_recv.at[oc, 0, 1], right)
        if kind == NEAR_L:
            return rcopy(kind, oc, total.at[oc, c_left, 0], fin_recv.at[oc, 1, 0], left)
        if kind == MIX_R:
            return rcopy(kind, oc, total.at[oc, c_right, 0], fin_recv.at[oc, 0, 0], right)
        return rcopy(kind, oc, total.at[oc, c_left, 1], fin_recv.at[oc, 1, 1], left)

    rows = chips * tokens
    half = OUT_COLS // 2

    def partial(rail, obuf, dst):
        at = pl.multiple_of(rail * rows, rows)
        val = jnp.dot(mix[0, pl.ds(at, rows), :], obuf[...], preferred_element_type=F32)
        val += jnp.dot(mix[1, pl.ds(at, rows), :], obuf[...], preferred_element_type=F32)
        val += jnp.dot(mix[2, pl.ds(at, rows), :], obuf[...], preferred_element_type=F32)
        for t in range(chips):
            for h in range(2):
                dst[t, h] = val[t * tokens:(t + 1) * tokens, h * half:(h + 1) * half]

    def partial_of(rail, t, obuf, dst):
        at = pl.multiple_of(rail * rows + t * tokens, tokens)
        val = jnp.dot(mix[0, pl.ds(at, tokens), :], obuf[...], preferred_element_type=F32)
        val += jnp.dot(mix[1, pl.ds(at, tokens), :], obuf[...], preferred_element_type=F32)
        val += jnp.dot(mix[2, pl.ds(at, tokens), :], obuf[...], preferred_element_type=F32)
        for h in range(2):
            dst[t, h] = val[:, h * half:(h + 1) * half]

    def finish_far(oc):
        rcopy(FAR_R, oc, far_recv.at[oc], far_recv.at[oc], buddy).wait_recv()
        total[oc, c_right, 0] = total[oc, c_right, 0] + far_recv[oc, 0]
        r_copy(MIX_R, oc).start()
        total[oc, c_left, 1] = total[oc, c_left, 1] + far_recv[oc, 1]
        r_copy(MIX_L, oc).start()

    per_in = kc_n // OUT_COLS

    def finish(oc):
        rcopy(NEAR_R, oc, fin_recv.at[oc], fin_recv.at[oc], buddy).wait_recv()
        for h in range(2):
            at = pl.multiple_of(lax.rem(oc, per_in) * OUT_COLS + h * half, half)
            x_own = x_all[oc // per_in, pl.ds(pl.multiple_of(me * tokens, tokens), tokens), pl.ds(at, half)]
            val = total[oc, chip, h] + fin_recv[oc, 0, h] + fin_recv[oc, 1, h]
            to = pl.multiple_of(oc * OUT_COLS + h * half, half)
            out_ref[:, pl.ds(to, half)] = (x_own.astype(F32) + val).astype(BF16)

    def down(oc, obuf):
        for e in range(local_e):
            val = jnp.dot(hid[e], wout_buf[lax.rem(oc, OUT_DEPTH), e], preferred_element_type=F32)
            obuf[e * capacity:(e + 1) * capacity, :] = val.astype(BF16)

    def refill(oc):
        for e in range(local_e):
            wout_copy(e, oc).start()

    def part_sent(oc):
        sent = part_send.at[lax.rem(oc, 2)]
        rcopy(PART, oc, sent, sent, buddy).wait_send()

    def share(oc, now, after):
        @pl.when(oc >= 2)
        def _():
            part_sent(oc - 2)

        with jax.named_scope("partA"):
            alone(lambda: partial(other, now, part_send.at[lax.rem(oc, 2)]))
            r_copy(PART, oc).start()
            part_rest(oc)
        with jax.named_scope("partB"):
            @alone
            def _():
                partial(core, now, total.at[oc])
                after()
        send_on(oc)

    def part_rest(oc):
        for t in (c_right, c_left, chip):
            rcopy(PART_REST, oc, part_send.at[lax.rem(oc, 2), t], part_recv.at[oc, t], buddy).start()

    def send_on(oc):
        with jax.named_scope("part_wait"):
            r_copy(PART, oc).wait_recv()
        total[oc, c_far] = total[oc, c_far] + part_recv[oc, c_far]
        for kind in (FAR_R, FAR_L):
            r_copy(kind, oc).start()
        with jax.named_scope("rest_wait"):
            rest = part_recv.at[oc, pl.ds(0, chips - 1)]
            rcopy(PART_REST, oc, rest, rest, buddy).wait_recv()
        for t in (c_right, c_left, chip):
            total[oc, t] = total[oc, t] + part_recv[oc, t]
        for kind in (NEAR_R, NEAR_L):
            r_copy(kind, oc).start()

    def step(oc, now, nxt):
        if nxt is None:
            share(oc, now, lambda: None)
        else:
            wout_wait(oc + 1)
            share(oc, now, lambda: down(oc + 1, nxt))

            @pl.when(oc + 1 + OUT_DEPTH < oc_n)
            def _():
                refill(oc + 1 + OUT_DEPTH)
        with jax.named_scope("far"):
            finish_far(oc - 1)

        @pl.when(oc >= LAG)
        def _():
            with jax.named_scope("fin"):
                finish(oc - LAG)

    with jax.named_scope("up_last"):
        win_wait(last)
        wout_wait(0)

        @alone
        def _():
            gather(last)
            for e in range(local_e):
                up = acc[e] + jnp.dot(xg[e], win_buf[last % IN_DEPTH, e], preferred_element_type=F32)
                hid[e] = gelu(up).astype(BF16)
            down(0, obuf0)

    with jax.named_scope("first"):
        @alone
        def _():
            partial_of(other, c_far, obuf0, part_send.at[0])
            partial_of(core, c_far, obuf0, total.at[0])
        r_copy(PART, 0).start()

        @alone
        def _():
            for t in (c_right, c_left, chip):
                partial_of(other, t, obuf0, part_send.at[0])
        part_rest(0)

        @alone
        def _():
            for t in (c_right, c_left, chip):
                partial_of(core, t, obuf0, total.at[0])
    send_on(0)
    refill(OUT_DEPTH)
    wout_wait(1)
    alone(lambda: down(1, obuf1))
    refill(OUT_DEPTH + 1)

    @pl.loop(0, oc_n // 2 - 1)
    def _(i):
        step(2 * i + 1, obuf1, obuf0)
        step(2 * i + 2, obuf0, obuf1)

    step(oc_n - 1, obuf1, None)

    for kind, rows_sent in ((OWN_R, 2), (OWN_L, 2), (OWN_P, 2), (RELAY_R, 1), (RELAY_L, 1),
                            (FWD_L, 2), (FWD_R, 2), (FWD_A, 1), (FWD_B, 1)):
        d_flush(kind, rows_sent * tokens // 2)
    for c in meta_all():
        c.wait_send()

    with jax.named_scope("far_t"):
        finish_far(oc_n - 1)
    for oc in range(oc_n - LAG, oc_n):
        with jax.named_scope("fin_t"):
            finish(oc)

    with jax.named_scope("drain"):
        part_sent(oc_n - 2)
        part_sent(oc_n - 1)
        for kind in (FAR_R, FAR_L, NEAR_R, NEAR_L, MIX_R, MIX_L):
            sent = total.at[:, 0, 0]
            rcopy(kind, 0, sent, sent, buddy).wait_send()


def solution(mesh):
    n = mesh.shape[AXIS]
    row_spec = P(("data", AXIS), None)
    weight_spec = P(AXIS, None, None)

    def device_step(token_rows, expert_ids, gate_weights, w_in, w_out):
        tokens, top_k = expert_ids.shape
        local_e, model, hidden = w_in.shape
        capacity = n * tokens * top_k // (n * local_e)
        slots = local_e * capacity
        chips = n // 2
        kc_n = model // IN_BLOCKS
        oc_n = model // OUT_COLS
        half = OUT_COLS // 2
        hbm = pl.BlockSpec(memory_space=pl.ANY)
        dma = pltpu.SemaphoreType.DMA
        return pl.pallas_call(
            functools.partial(body, n, capacity),
            out_shape=pltpu.VMEM((tokens, model), BF16),
            in_specs=[hbm, hbm, hbm, hbm, hbm],
            out_specs=pl.BlockSpec(memory_space=pltpu.VMEM),
            scratch_shapes=[
                pltpu.VMEM((n, top_k, tokens), jnp.int32),
                pltpu.VMEM((n, top_k, tokens), F32),
                pltpu.VMEM((IN_BLOCKS, n * tokens, kc_n), BF16),
                pltpu.VMEM((slots, n * tokens), BF16),
                pltpu.VMEM((n, 4 * local_e, tokens), F32),
                pltpu.VMEM((3, n * tokens, slots), BF16),
                pltpu.VMEM((local_e, capacity, kc_n), BF16),
                pltpu.VMEM((local_e, capacity, hidden), F32),
                pltpu.VMEM((local_e, capacity, hidden), BF16),
                pltpu.VMEM((LANES, 4 * slots), BF16),
                pltpu.VMEM((slots, OUT_COLS), BF16),
                pltpu.VMEM((slots, OUT_COLS), BF16),
                pltpu.VMEM((2, chips, 2, tokens, half), F32),
                pltpu.VMEM((oc_n, chips, 2, tokens, half), F32),
                pltpu.VMEM((oc_n, chips, 2, tokens, half), F32),
                pltpu.VMEM((oc_n, 2, tokens, half), F32),
                pltpu.VMEM((oc_n, 2, 2, tokens, half), F32),
                pltpu.VMEM((IN_DEPTH, local_e, kc_n, hidden), BF16),
                pltpu.VMEM((OUT_DEPTH, local_e, hidden, OUT_COLS), BF16),
                dma((2,)), dma((2,)),
                dma((9,)), dma((3, IN_BLOCKS)),
                dma((8,)), dma((4, oc_n)),
                dma,
                dma((IN_DEPTH,)),
                dma((OUT_DEPTH,)),
                dma((2,)),
            ],
            compiler_params=pltpu.CompilerParams(
                collective_id=0, has_side_effects=True, vmem_limit_bytes=VMEM_BYTES),
        )(expert_ids.T, gate_weights.T, token_rows, w_in, w_out)

    return jax.shard_map(device_step, mesh=mesh, in_specs=(row_spec, row_spec, row_spec, weight_spec, weight_spec),
                         out_specs=row_spec, check_vma=False)
```

```python
import functools

import jax
import jax.numpy as jnp
from jax import lax
from jax.experimental import pallas as pl
from jax.experimental.pallas import tpu as pltpu
from jax.sharding import PartitionSpec as P

MESH = pl.DeviceIdType.MESH
F32 = jnp.float32
BF16 = jnp.bfloat16
AXIS = "expert"
LANES = 128
IN_BLOCKS = 8
IN_DEPTH = 3
OUT_COLS = 256
OUT_DEPTH = 2
AHEAD = 3
LAG = 3
VMEM_BYTES = 62 * 2 ** 20
GELU_A = 0.7978845608028654
GELU_B = 0.044715 * GELU_A
PICK_PARTS = 4
BEHIND = 1
BIG_BF16 = 3.3895313892515355e38

OWN_R, OWN_L, OWN_P, RELAY_R, RELAY_L, FWD_L, FWD_R, FWD_A, FWD_B = range(9)
PART, FAR_R, FAR_L, NEAR_R, NEAR_L, MIX_R, MIX_L, PART_REST = range(8)


def gelu(x):
    half = 0.5 * x
    return half + half * jnp.tanh(x * (GELU_A + GELU_B * (x * x)))


def body(n, capacity, ids_hbm, gate_hbm, x_hbm, w_in, w_out, out_ref,
         ids_all, gates_all, x_all, pick, packed, mix, xg, acc, hid, spread, obuf0, obuf1,
         part_send, part_recv, total, far_recv, fin_recv, win_buf, wout_buf,
         meta_ssem, meta_rsem, d_ssem, d_rsem, r_ssem, r_rsem, x_sem, win_sem, wout_sem, own_sem):
    top_k, tokens = ids_hbm.shape
    local_e, model, hidden = w_in.shape
    chips = n // 2
    kc_n = model // IN_BLOCKS
    oc_n = model // OUT_COLS
    slots = local_e * capacity

    me = lax.axis_index(AXIS)
    core = lax.rem(me, 2)
    chip = me // 2
    buddy = me + 1 - 2 * core
    other = 1 - core
    c_right = lax.rem(chip + 1, chips)
    c_far = lax.rem(chip + 2, chips)
    c_left = lax.rem(chip + 3, chips)

    def dev(c, k):
        return 2 * c + k

    right = dev(c_right, core)
    left = dev(c_left, core)

    def alone(fn):
        pl.when(me >= 0)(fn)

    def win_copy(e, kc):
        slot = lax.rem(kc, IN_DEPTH)
        return pltpu.make_async_copy(
            w_in.at[e, pl.ds(kc * kc_n, kc_n), :], win_buf.at[slot, e], win_sem.at[slot])

    def win_wait(kc):
        slot = lax.rem(kc, IN_DEPTH)
        pltpu.make_async_copy(w_in.at[:, pl.ds(0, kc_n), :], win_buf.at[slot], win_sem.at[slot]).wait()

    def wout_copy(e, oc):
        slot = lax.rem(oc, OUT_DEPTH)
        return pltpu.make_async_copy(
            w_out.at[e, :, pl.ds(oc * OUT_COLS, OUT_COLS)], wout_buf.at[slot, e], wout_sem.at[slot])

    def wout_wait(oc):
        slot = lax.rem(oc, OUT_DEPTH)
        pltpu.make_async_copy(w_out.at[:, :, pl.ds(0, OUT_COLS)], wout_buf.at[slot], wout_sem.at[slot]).wait()

    def x_rows(kc, d):
        return x_all.at[kc, pl.ds(d * tokens, tokens), :]

    def x_half(kc, d, h):
        half = tokens // 2
        return x_all.at[kc, pl.ds(d * tokens + h * half, half), :]

    def x_copy(kc):
        return pltpu.make_async_copy(
            x_hbm.at[:, pl.ds(kc * kc_n, kc_n)], x_rows(kc, me), x_sem)

    barrier = pltpu.get_barrier_semaphore()
    for d in range(1, n):
        pl.semaphore_signal(barrier, inc=1, device_id={AXIS: lax.rem(me + d, n)}, device_id_type=MESH)

    own_meta = (
        pltpu.make_async_copy(ids_hbm, ids_all.at[me], own_sem.at[0]),
        pltpu.make_async_copy(gate_hbm, gates_all.at[me], own_sem.at[1]),
    )
    for c in own_meta:
        c.start()
    for kc in range(IN_BLOCKS):
        x_copy(kc).start()

    @pl.loop(0, IN_DEPTH)
    def _(kc):
        for e in range(local_e):
            win_copy(e, kc).start()

    @pl.loop(0, OUT_DEPTH)
    def _(oc):
        for e in range(local_e):
            wout_copy(e, oc).start()

    with jax.named_scope("barrier"):
        pl.semaphore_wait(barrier, n - 1)
        for c in own_meta:
            c.wait()

    def meta_copies(d):
        to = lax.rem(me + d, n)
        return (
            pltpu.make_async_remote_copy(
                src_ref=ids_all.at[me], dst_ref=ids_all.at[me], send_sem=meta_ssem.at[0], recv_sem=meta_rsem.at[0],
                device_id={AXIS: to}, device_id_type=MESH),
            pltpu.make_async_remote_copy(
                src_ref=gates_all.at[me], dst_ref=gates_all.at[me], send_sem=meta_ssem.at[1], recv_sem=meta_rsem.at[1],
                device_id={AXIS: to}, device_id_type=MESH),
        )

    def meta_all():
        ids_part, gates_part = ids_all.at[pl.ds(0, n - 1)], gates_all.at[pl.ds(0, n - 1)]
        return (
            pltpu.make_async_remote_copy(
                src_ref=ids_part, dst_ref=ids_part, send_sem=meta_ssem.at[0], recv_sem=meta_rsem.at[0],
                device_id={AXIS: buddy}, device_id_type=MESH),
            pltpu.make_async_remote_copy(
                src_ref=gates_part, dst_ref=gates_part, send_sem=meta_ssem.at[1], recv_sem=meta_rsem.at[1],
                device_id={AXIS: buddy}, device_id_type=MESH),
        )

    for d in range(1, n):
        for c in meta_copies(d):
            c.start()

    def dcopy(kind, kc, ref, to):
        group = 0 if kind in (OWN_R, OWN_L) else 1 if kind in (RELAY_R, RELAY_L) else 2
        return pltpu.make_async_remote_copy(
            src_ref=ref, dst_ref=ref, send_sem=d_ssem.at[kind], recv_sem=d_rsem.at[group, kc],
            device_id={AXIS: to}, device_id_type=MESH)

    def d_wait(kind, kc, rows):
        dcopy(kind, kc, x_all.at[kc, pl.ds(0, rows), :], buddy).wait_recv()

    def d_flush(kind, rows):
        dcopy(kind, 0, x_all.at[:, pl.ds(0, rows), :], buddy).wait_send()

    far = dev(c_far, core)

    def d_sent(kind, kc):
        if kind == OWN_R:
            return dcopy(kind, kc, x_rows(kc, me), right)
        if kind == OWN_L:
            return dcopy(kind, kc, x_rows(kc, me), left)
        if kind == OWN_P:
            return dcopy(kind, kc, x_rows(kc, me), buddy)
        if kind == RELAY_R:
            return dcopy(kind, kc, x_half(kc, left, 0), right)
        if kind == RELAY_L:
            return dcopy(kind, kc, x_half(kc, right, 1), left)
        if kind == FWD_L:
            return dcopy(kind, kc, x_rows(kc, left), buddy)
        if kind == FWD_R:
            return dcopy(kind, kc, x_rows(kc, right), buddy)
        if kind == FWD_A:
            return dcopy(kind, kc, x_half(kc, far, 0), buddy)
        return dcopy(kind, kc, x_half(kc, far, 1), buddy)

    def send_own(kc):
        for kind in (OWN_R, OWN_L, OWN_P):
            d_sent(kind, kc).start()

    def stage1(kc):
        d_wait(OWN_R, kc, 2 * tokens)
        for kind in (RELAY_R, RELAY_L, FWD_L, FWD_R):
            d_sent(kind, kc).start()

    def stage2(kc):
        d_wait(RELAY_R, kc, tokens)
        for kind in (FWD_A, FWD_B):
            d_sent(kind, kc).start()

    def stage3(kc):
        d_wait(OWN_P, kc, chips * tokens)

    with jax.named_scope("own"):
        mine = x_all.at[:, pl.ds(me * tokens, tokens), :]
        pltpu.make_async_copy(mine, mine, x_sem).wait()
        for kc in range(AHEAD):
            send_own(kc)

    with jax.named_scope("meta_wait"):
        for c in meta_all():
            c.wait_recv()

    sub = lax.broadcasted_iota(jnp.int32, (local_e, tokens), 0) + me * local_e
    hit = {}
    for b in range(n):
        for j in range(top_k):
            hit[b, j] = jnp.where(ids_all[b, j:j + 1, :] == sub, 1.0, 0.0).astype(F32)
    hits = jnp.concatenate([hit[b, j] for b in range(n) for j in range(top_k)], axis=0).astype(BF16)
    t_from = lax.broadcasted_iota(jnp.int32, (tokens, tokens), 0)
    t_to = lax.broadcasted_iota(jnp.int32, (tokens, tokens), 1)
    earlier = jnp.where(t_from < t_to, 1.0, 0.0).astype(BF16)
    ones = jnp.full((tokens, tokens), 1.0, BF16)
    within = jnp.dot(hits, earlier, preferred_element_type=F32)
    sums = jnp.dot(hits, ones, preferred_element_type=F32)
    running = jnp.zeros((local_e, tokens), F32)
    rank = [jnp.zeros((local_e, tokens), F32) for _ in range(n)]
    for j in range(top_k):
        for b in range(n):
            at = (b * top_k + j) * local_e
            rank[b] = rank[b] + hit[b, j] * (running + within[at:at + local_e])
            running = running + sums[at:at + local_e]
    slot_row = lax.broadcasted_iota(jnp.int32, (capacity, tokens), 0).astype(F32)
    for b in range(n):
        has = jnp.zeros((local_e, tokens), F32)
        gate = jnp.zeros((local_e, tokens), F32)
        for j in range(top_k):
            has = has + hit[b, j]
            gate = gate + hit[b, j] * gates_all[b, j:j + 1, :]
        slot = jnp.where((has > 0.0) & (rank[b] < capacity), rank[b], -1.0)
        g1 = jnp.minimum(gate, BIG_BF16).astype(BF16).astype(F32)
        g2 = (gate - g1).astype(BF16).astype(F32)
        g3 = gate - g1 - g2
        packed[b] = jnp.concatenate([slot, g1, g2, g3], axis=0)
        for e in range(local_e):
            pick[e * capacity:(e + 1) * capacity, b * tokens:(b + 1) * tokens] = jnp.where(
                slot[e:e + 1, :] == slot_row, 1.0, 0.0).astype(BF16)

    acc[...] = jnp.zeros_like(acc)

    part_c = 2 * LANES
    for q in range(4):
        at = lax.broadcasted_iota(jnp.int32, (LANES, slots), 1)
        row = lax.broadcasted_iota(jnp.int32, (LANES, slots), 0) - q * local_e
        spread[:, q * slots:(q + 1) * slots] = jnp.where(
            (at >= row * capacity) & (at < (row + 1) * capacity) & (row >= 0) & (row < local_e), 1.0, 0.0).astype(BF16)

    def mix_rows(b):
        row = pl.multiple_of((lax.rem(b, 2) * chips + b // 2) * tokens, tokens)
        cols = jnp.concatenate(
            [packed[b], jnp.zeros((LANES - 4 * local_e, tokens), F32)], axis=0).T.astype(BF16)
        for p in range(slots // part_c):
            at = lax.broadcasted_iota(jnp.int32, (1, part_c), 1) + p * part_c
            rel = at
            for e in range(1, local_e):
                rel = jnp.where(at >= e * capacity, at - e * capacity, rel)
            rel = rel.astype(F32)

            def repeat(q):
                return jnp.dot(cols, spread[:, q * slots + p * part_c:q * slots + (p + 1) * part_c],
                               preferred_element_type=F32)

            slot_at = repeat(0)
            for k in range(3):
                mix[k, pl.ds(row, tokens), p * part_c:(p + 1) * part_c] = jnp.where(
                    slot_at == rel, repeat(k + 1), 0.0).astype(BF16)

    def mix_range(lo, hi):
        with jax.named_scope("mix"):
            pl.loop(lo, hi)(mix_rows)

    with jax.named_scope("s1"):
        stage1(0)
        send_own(AHEAD)
    mix_range(0, n // 2)
    with jax.named_scope("s1"):
        stage1(1)
        send_own(AHEAD + 1)
    with jax.named_scope("s2"):
        stage2(0)

    pick_rows = slots // PICK_PARTS

    def gather(kc):
        for i in range(PICK_PARTS):
            val = jnp.dot(pick[i * pick_rows:(i + 1) * pick_rows, :], x_all[kc], preferred_element_type=F32)
            xg[i * pick_rows // capacity:(i + 1) * pick_rows // capacity] = val.astype(BF16).reshape(
                pick_rows // capacity, capacity, kc_n)

    with jax.named_scope("s1"):
        stage1(2)
        send_own(AHEAD + 2)
    mix_range(n // 2, n)

    @pl.loop(0, IN_BLOCKS - 1)
    def _(kc):
        with jax.named_scope("s1"):
            @pl.when(kc + 3 < IN_BLOCKS)
            def _():
                stage1(kc + 3)

            @pl.when(kc + 3 + AHEAD < IN_BLOCKS)
            def _():
                send_own(kc + 3 + AHEAD)

        with jax.named_scope("s2"):
            stage2(kc + 1)
        with jax.named_scope("s3"):
            stage3(kc)

        with jax.named_scope("up"):
            win_wait(kc)

            @alone
            def _():
                gather(kc)
                for e in range(local_e):
                    acc[e] = acc[e] + jnp.dot(xg[e], win_buf[lax.rem(kc, IN_DEPTH), e], preferred_element_type=F32)

            @pl.when(kc + IN_DEPTH < IN_BLOCKS)
            def _():
                for e in range(local_e):
                    win_copy(e, kc + IN_DEPTH).start()

    last = IN_BLOCKS - 1
    with jax.named_scope("s3"):
        stage3(last)
    def rcopy(kind, oc, src, dst, to):
        ssem = r_ssem.at[lax.rem(oc, 2)] if kind in (PART, PART_REST) else r_ssem.at[kind + 1]
        group = 0 if kind == PART else 1 if kind in (FAR_R, FAR_L) else 2 if kind != PART_REST else 3
        return pltpu.make_async_remote_copy(
            src_ref=src, dst_ref=dst, send_sem=ssem, recv_sem=r_rsem.at[group, oc],
            device_id={AXIS: to}, device_id_type=MESH)

    def r_copy(kind, oc):
        if kind == PART:
            return rcopy(kind, oc, part_send.at[lax.rem(oc, 2), c_far], part_recv.at[oc, c_far], buddy)
        if kind == FAR_R:
            return rcopy(kind, oc, total.at[oc, c_far, 0], far_recv.at[oc, 0], right)
        if kind == FAR_L:
            return rcopy(kind, oc, total.at[oc, c_far, 1], far_recv.at[oc, 1], left)
        if kind == NEAR_R:
            return rcopy(kind, oc, total.at[oc, c_right, 1], fin_recv.at[oc, 0, 1], right)
        if kind == NEAR_L:
            return rcopy(kind, oc, total.at[oc, c_left, 0], fin_recv.at[oc, 1, 0], left)
        if kind == MIX_R:
            return rcopy(kind, oc, total.at[oc, c_right, 0], fin_recv.at[oc, 0, 0], right)
        return rcopy(kind, oc, total.at[oc, c_left, 1], fin_recv.at[oc, 1, 1], left)

    rows = chips * tokens
    half = OUT_COLS // 2

    def partial(rail, obuf, dst):
        at = pl.multiple_of(rail * rows, rows)
        val = jnp.dot(mix[0, pl.ds(at, rows), :], obuf[...], preferred_element_type=F32)
        val += jnp.dot(mix[1, pl.ds(at, rows), :], obuf[...], preferred_element_type=F32)
        val += jnp.dot(mix[2, pl.ds(at, rows), :], obuf[...], preferred_element_type=F32)
        for t in range(chips):
            for h in range(2):
                dst[t, h] = val[t * tokens:(t + 1) * tokens, h * half:(h + 1) * half]

    def partial_of(rail, t, obuf, dst):
        at = pl.multiple_of(rail * rows + t * tokens, tokens)
        val = jnp.dot(mix[0, pl.ds(at, tokens), :], obuf[...], preferred_element_type=F32)
        val += jnp.dot(mix[1, pl.ds(at, tokens), :], obuf[...], preferred_element_type=F32)
        val += jnp.dot(mix[2, pl.ds(at, tokens), :], obuf[...], preferred_element_type=F32)
        for h in range(2):
            dst[t, h] = val[:, h * half:(h + 1) * half]

    def finish_far(oc):
        rcopy(FAR_R, oc, far_recv.at[oc], far_recv.at[oc], buddy).wait_recv()
        total[oc, c_right, 0] = total[oc, c_right, 0] + far_recv[oc, 0]
        r_copy(MIX_R, oc).start()
        total[oc, c_left, 1] = total[oc, c_left, 1] + far_recv[oc, 1]
        r_copy(MIX_L, oc).start()

    per_in = kc_n // OUT_COLS

    def finish(oc):
        rcopy(NEAR_R, oc, fin_recv.at[oc], fin_recv.at[oc], buddy).wait_recv()
        for h in range(2):
            at = pl.multiple_of(lax.rem(oc, per_in) * OUT_COLS + h * half, half)
            x_own = x_all[oc // per_in, pl.ds(pl.multiple_of(me * tokens, tokens), tokens), pl.ds(at, half)]
            val = total[oc, chip, h] + fin_recv[oc, 0, h] + fin_recv[oc, 1, h]
            to = pl.multiple_of(oc * OUT_COLS + h * half, half)
            out_ref[:, pl.ds(to, half)] = (x_own.astype(F32) + val).astype(BF16)

    def down_one(oc, e, obuf):
        val = jnp.dot(hid[e], wout_buf[lax.rem(oc, OUT_DEPTH), e], preferred_element_type=F32)
        obuf[e * capacity:(e + 1) * capacity, :] = val.astype(BF16)

    def down(oc, obuf):
        for e in range(local_e):
            down_one(oc, e, obuf)

    def refill(oc):
        for e in range(local_e):
            wout_copy(e, oc).start()

    def part_sent(oc):
        sent = part_send.at[lax.rem(oc, 2)]
        rcopy(PART, oc, sent, sent, buddy).wait_send()

    def share(oc, now, after, ready):
        @pl.when(oc >= 2)
        def _():
            part_sent(oc - 2)

        with jax.named_scope("partA"):
            alone(lambda: partial(other, now, part_send.at[lax.rem(oc, 2)]))
            r_copy(PART, oc).start()
            part_rest(oc)
            ready()
        with jax.named_scope("partB"):
            @alone
            def _():
                partial(core, now, total.at[oc])
                after()
        send_on(oc)

    def part_rest(oc):
        for t in (c_right, c_left, chip):
            rcopy(PART_REST, oc, part_send.at[lax.rem(oc, 2), t], part_recv.at[oc, t], buddy).start()

    def send_on(oc):
        with jax.named_scope("part_wait"):
            r_copy(PART, oc).wait_recv()
        total[oc, c_far] = total[oc, c_far] + part_recv[oc, c_far]
        for kind in (FAR_R, FAR_L):
            r_copy(kind, oc).start()
        with jax.named_scope("rest_wait"):
            rest = part_recv.at[oc, pl.ds(0, chips - 1)]
            rcopy(PART_REST, oc, rest, rest, buddy).wait_recv()
        for t in (c_right, c_left, chip):
            total[oc, t] = total[oc, t] + part_recv[oc, t]
        for kind in (NEAR_R, NEAR_L):
            r_copy(kind, oc).start()

    def step(oc, now, nxt):
        if nxt is None:
            share(oc, now, lambda: None, lambda: None)
        else:
            share(oc, now, lambda: down(oc + 1, nxt), lambda: wout_wait(oc + 1))

            @pl.when(oc + 1 + OUT_DEPTH < oc_n)
            def _():
                refill(oc + 1 + OUT_DEPTH)
        with jax.named_scope("far"):
            finish_far(oc - 1)

        @pl.when(oc >= LAG)
        def _():
            with jax.named_scope("fin"):
                finish(oc - LAG)

    with jax.named_scope("up_last"):
        win_wait(last)
        wout_wait(0)

        @alone
        def _():
            gather(last)
            for e in range(local_e):
                up = acc[e] + jnp.dot(xg[e], win_buf[last % IN_DEPTH, e], preferred_element_type=F32)
                hid[e] = gelu(up).astype(BF16)
                if e >= BEHIND:
                    down_one(0, e - BEHIND, obuf0)
            for e in range(local_e - BEHIND, local_e):
                down_one(0, e, obuf0)

        refill(OUT_DEPTH)

    with jax.named_scope("first"):
        @alone
        def _():
            partial_of(other, c_far, obuf0, part_send.at[0])
            partial_of(core, c_far, obuf0, total.at[0])
        r_copy(PART, 0).start()

        @alone
        def _():
            for t in (c_right, c_left, chip):
                partial_of(other, t, obuf0, part_send.at[0])
        part_rest(0)

        @alone
        def _():
            for t in (c_right, c_left, chip):
                partial_of(core, t, obuf0, total.at[0])
    send_on(0)
    wout_wait(1)
    alone(lambda: down(1, obuf1))
    refill(OUT_DEPTH + 1)

    @pl.loop(0, oc_n // 2 - 1)
    def _(i):
        step(2 * i + 1, obuf1, obuf0)
        step(2 * i + 2, obuf0, obuf1)

    step(oc_n - 1, obuf1, None)

    for kind, rows_sent in ((OWN_R, 2), (OWN_L, 2), (OWN_P, 2), (RELAY_R, 1), (RELAY_L, 1),
                            (FWD_L, 2), (FWD_R, 2), (FWD_A, 1), (FWD_B, 1)):
        d_flush(kind, rows_sent * tokens // 2)
    for c in meta_all():
        c.wait_send()

    with jax.named_scope("far_t"):
        finish_far(oc_n - 1)
    for oc in range(oc_n - LAG, oc_n):
        with jax.named_scope("fin_t"):
            finish(oc)

    with jax.named_scope("drain"):
        part_sent(oc_n - 2)
        part_sent(oc_n - 1)
        for kind in (FAR_R, FAR_L, NEAR_R, NEAR_L, MIX_R, MIX_L):
            sent = total.at[:, 0, 0]
            rcopy(kind, 0, sent, sent, buddy).wait_send()


def solution(mesh):
    n = mesh.shape[AXIS]
    row_spec = P(("data", AXIS), None)
    weight_spec = P(AXIS, None, None)

    def device_step(token_rows, expert_ids, gate_weights, w_in, w_out):
        tokens, top_k = expert_ids.shape
        local_e, model, hidden = w_in.shape
        capacity = n * tokens * top_k // (n * local_e)
        slots = local_e * capacity
        chips = n // 2
        kc_n = model // IN_BLOCKS
        oc_n = model // OUT_COLS
        half = OUT_COLS // 2
        hbm = pl.BlockSpec(memory_space=pl.ANY)
        dma = pltpu.SemaphoreType.DMA
        return pl.pallas_call(
            functools.partial(body, n, capacity),
            out_shape=pltpu.VMEM((tokens, model), BF16),
            in_specs=[hbm, hbm, hbm, hbm, hbm],
            out_specs=pl.BlockSpec(memory_space=pltpu.VMEM),
            scratch_shapes=[
                pltpu.VMEM((n, top_k, tokens), jnp.int32),
                pltpu.VMEM((n, top_k, tokens), F32),
                pltpu.VMEM((IN_BLOCKS, n * tokens, kc_n), BF16),
                pltpu.VMEM((slots, n * tokens), BF16),
                pltpu.VMEM((n, 4 * local_e, tokens), F32),
                pltpu.VMEM((3, n * tokens, slots), BF16),
                pltpu.VMEM((local_e, capacity, kc_n), BF16),
                pltpu.VMEM((local_e, capacity, hidden), F32),
                pltpu.VMEM((local_e, capacity, hidden), BF16),
                pltpu.VMEM((LANES, 4 * slots), BF16),
                pltpu.VMEM((slots, OUT_COLS), BF16),
                pltpu.VMEM((slots, OUT_COLS), BF16),
                pltpu.VMEM((2, chips, 2, tokens, half), F32),
                pltpu.VMEM((oc_n, chips, 2, tokens, half), F32),
                pltpu.VMEM((oc_n, chips, 2, tokens, half), F32),
                pltpu.VMEM((oc_n, 2, tokens, half), F32),
                pltpu.VMEM((oc_n, 2, 2, tokens, half), F32),
                pltpu.VMEM((IN_DEPTH, local_e, kc_n, hidden), BF16),
                pltpu.VMEM((OUT_DEPTH, local_e, hidden, OUT_COLS), BF16),
                dma((2,)), dma((2,)),
                dma((9,)), dma((3, IN_BLOCKS)),
                dma((8,)), dma((4, oc_n)),
                dma,
                dma((IN_DEPTH,)),
                dma((OUT_DEPTH,)),
                dma((2,)),
            ],
            compiler_params=pltpu.CompilerParams(
                collective_id=0, has_side_effects=True, vmem_limit_bytes=VMEM_BYTES),
        )(expert_ids.T, gate_weights.T, token_rows, w_in, w_out)

    return jax.shard_map(device_step, mesh=mesh, in_specs=(row_spec, row_spec, row_spec, weight_spec, weight_spec),
                         out_specs=row_spec, check_vma=False)
```

```python
import functools

import jax
import jax.numpy as jnp
from jax import lax
from jax.experimental import pallas as pl
from jax.experimental.pallas import tpu as pltpu
from jax.sharding import PartitionSpec as P

MESH = pl.DeviceIdType.MESH
F32 = jnp.float32
BF16 = jnp.bfloat16
AXIS = "expert"
LANES = 128
IN_BLOCKS = 8
IN_DEPTH = 3
OUT_COLS = 256
OUT_DEPTH = 2
AHEAD = 3
LAG = 3
VMEM_BYTES = 62 * 2 ** 20
GELU_A = 0.7978845608028654
GELU_B = 0.044715 * GELU_A
PICK_PARTS = 4
BEHIND = 1
BIG_BF16 = 3.3895313892515355e38

OWN_R, OWN_L, OWN_P, RELAY_R, RELAY_L, FWD_L, FWD_R, FWD_A, FWD_B = range(9)
PART, FAR_R, FAR_L, NEAR_R, NEAR_L, MIX_R, MIX_L, PART_REST = range(8)


def gelu(x):
    half = 0.5 * x
    return half + half * jnp.tanh(x * (GELU_A + GELU_B * (x * x)))


def body(n, capacity, ids_hbm, gate_hbm, x_hbm, w_in, w_out, out_ref,
         ids_all, gates_all, x_all, pick, packed, mix, xg, acc, hid, spread, obuf0, obuf1,
         part_send, part_recv, total, far_recv, fin_recv, win_buf, wout_buf,
         meta_ssem, meta_rsem, d_ssem, d_rsem, r_ssem, r_rsem, x_sem, win_sem, wout_sem, own_sem):
    top_k, tokens = ids_hbm.shape
    local_e, model, hidden = w_in.shape
    chips = n // 2
    kc_n = model // IN_BLOCKS
    oc_n = model // OUT_COLS
    slots = local_e * capacity

    me = lax.axis_index(AXIS)
    core = lax.rem(me, 2)
    chip = me // 2
    buddy = me + 1 - 2 * core
    other = 1 - core
    c_right = lax.rem(chip + 1, chips)
    c_far = lax.rem(chip + 2, chips)
    c_left = lax.rem(chip + 3, chips)

    def dev(c, k):
        return 2 * c + k

    right = dev(c_right, core)
    left = dev(c_left, core)

    def alone(fn):
        pl.when(me >= 0)(fn)

    def win_copy(e, kc):
        slot = lax.rem(kc, IN_DEPTH)
        return pltpu.make_async_copy(
            w_in.at[e, pl.ds(kc * kc_n, kc_n), :], win_buf.at[slot, e], win_sem.at[slot])

    def win_wait(kc):
        slot = lax.rem(kc, IN_DEPTH)
        pltpu.make_async_copy(w_in.at[:, pl.ds(0, kc_n), :], win_buf.at[slot], win_sem.at[slot]).wait()

    def wout_copy(e, oc):
        slot = lax.rem(oc, OUT_DEPTH)
        return pltpu.make_async_copy(
            w_out.at[e, :, pl.ds(oc * OUT_COLS, OUT_COLS)], wout_buf.at[slot, e], wout_sem.at[slot])

    def wout_wait(oc):
        slot = lax.rem(oc, OUT_DEPTH)
        pltpu.make_async_copy(w_out.at[:, :, pl.ds(0, OUT_COLS)], wout_buf.at[slot], wout_sem.at[slot]).wait()

    def x_rows(kc, d):
        return x_all.at[kc, pl.ds(d * tokens, tokens), :]

    def x_half(kc, d, h):
        half = tokens // 2
        return x_all.at[kc, pl.ds(d * tokens + h * half, half), :]

    def x_copy(kc):
        return pltpu.make_async_copy(
            x_hbm.at[:, pl.ds(kc * kc_n, kc_n)], x_rows(kc, me), x_sem)

    barrier = pltpu.get_barrier_semaphore()
    for d in range(1, n):
        pl.semaphore_signal(barrier, inc=1, device_id={AXIS: lax.rem(me + d, n)}, device_id_type=MESH)

    own_meta = (
        pltpu.make_async_copy(ids_hbm, ids_all.at[me], own_sem.at[0]),
        pltpu.make_async_copy(gate_hbm, gates_all.at[me], own_sem.at[1]),
    )
    for c in own_meta:
        c.start()
    for kc in range(IN_BLOCKS):
        x_copy(kc).start()

    @pl.loop(0, IN_DEPTH)
    def _(kc):
        for e in range(local_e):
            win_copy(e, kc).start()

    @pl.loop(0, OUT_DEPTH)
    def _(oc):
        for e in range(local_e):
            wout_copy(e, oc).start()

    with jax.named_scope("barrier"):
        pl.semaphore_wait(barrier, n - 1)
        for c in own_meta:
            c.wait()

    def meta_copies(d):
        to = lax.rem(me + d, n)
        return (
            pltpu.make_async_remote_copy(
                src_ref=ids_all.at[me], dst_ref=ids_all.at[me], send_sem=meta_ssem.at[0], recv_sem=meta_rsem.at[0],
                device_id={AXIS: to}, device_id_type=MESH),
            pltpu.make_async_remote_copy(
                src_ref=gates_all.at[me], dst_ref=gates_all.at[me], send_sem=meta_ssem.at[1], recv_sem=meta_rsem.at[1],
                device_id={AXIS: to}, device_id_type=MESH),
        )

    def meta_all():
        ids_part, gates_part = ids_all.at[pl.ds(0, n - 1)], gates_all.at[pl.ds(0, n - 1)]
        return (
            pltpu.make_async_remote_copy(
                src_ref=ids_part, dst_ref=ids_part, send_sem=meta_ssem.at[0], recv_sem=meta_rsem.at[0],
                device_id={AXIS: buddy}, device_id_type=MESH),
            pltpu.make_async_remote_copy(
                src_ref=gates_part, dst_ref=gates_part, send_sem=meta_ssem.at[1], recv_sem=meta_rsem.at[1],
                device_id={AXIS: buddy}, device_id_type=MESH),
        )

    for d in range(1, n):
        for c in meta_copies(d):
            c.start()

    def dcopy(kind, kc, ref, to):
        group = 0 if kind in (OWN_R, OWN_L) else 1 if kind in (RELAY_R, RELAY_L) else 2
        return pltpu.make_async_remote_copy(
            src_ref=ref, dst_ref=ref, send_sem=d_ssem.at[kind], recv_sem=d_rsem.at[group, kc],
            device_id={AXIS: to}, device_id_type=MESH)

    def d_wait(kind, kc, rows):
        dcopy(kind, kc, x_all.at[kc, pl.ds(0, rows), :], buddy).wait_recv()

    def d_flush(kind, rows):
        dcopy(kind, 0, x_all.at[:, pl.ds(0, rows), :], buddy).wait_send()

    far = dev(c_far, core)

    def d_sent(kind, kc):
        if kind == OWN_R:
            return dcopy(kind, kc, x_rows(kc, me), right)
        if kind == OWN_L:
            return dcopy(kind, kc, x_rows(kc, me), left)
        if kind == OWN_P:
            return dcopy(kind, kc, x_rows(kc, me), buddy)
        if kind == RELAY_R:
            return dcopy(kind, kc, x_half(kc, left, 0), right)
        if kind == RELAY_L:
            return dcopy(kind, kc, x_half(kc, right, 1), left)
        if kind == FWD_L:
            return dcopy(kind, kc, x_rows(kc, left), buddy)
        if kind == FWD_R:
            return dcopy(kind, kc, x_rows(kc, right), buddy)
        if kind == FWD_A:
            return dcopy(kind, kc, x_half(kc, far, 0), buddy)
        return dcopy(kind, kc, x_half(kc, far, 1), buddy)

    def send_own(kc):
        for kind in (OWN_R, OWN_L, OWN_P):
            d_sent(kind, kc).start()

    def stage1(kc):
        d_wait(OWN_R, kc, 2 * tokens)
        for kind in (RELAY_R, RELAY_L, FWD_L, FWD_R):
            d_sent(kind, kc).start()

    def stage2(kc):
        d_wait(RELAY_R, kc, tokens)
        for kind in (FWD_A, FWD_B):
            d_sent(kind, kc).start()

    def stage3(kc):
        d_wait(OWN_P, kc, chips * tokens)

    with jax.named_scope("own"):
        mine = x_all.at[:, pl.ds(me * tokens, tokens), :]
        pltpu.make_async_copy(mine, mine, x_sem).wait()
        for kc in range(AHEAD):
            send_own(kc)

    with jax.named_scope("meta_wait"):
        for c in meta_all():
            c.wait_recv()

    sub = lax.broadcasted_iota(jnp.int32, (local_e, tokens), 0) + me * local_e
    hit = {}
    for b in range(n):
        for j in range(top_k):
            hit[b, j] = jnp.where(ids_all[b, j:j + 1, :] == sub, 1.0, 0.0).astype(F32)
    hits = jnp.concatenate([hit[b, j] for b in range(n) for j in range(top_k)], axis=0).astype(BF16)
    t_from = lax.broadcasted_iota(jnp.int32, (tokens, tokens), 0)
    t_to = lax.broadcasted_iota(jnp.int32, (tokens, tokens), 1)
    earlier = jnp.where(t_from < t_to, 1.0, 0.0).astype(BF16)
    ones = jnp.full((tokens, tokens), 1.0, BF16)
    within = jnp.dot(hits, earlier, preferred_element_type=F32)
    sums = jnp.dot(hits, ones, preferred_element_type=F32)
    running = jnp.zeros((local_e, tokens), F32)
    rank = [jnp.zeros((local_e, tokens), F32) for _ in range(n)]
    for j in range(top_k):
        for b in range(n):
            at = (b * top_k + j) * local_e
            rank[b] = rank[b] + hit[b, j] * (running + within[at:at + local_e])
            running = running + sums[at:at + local_e]
    slot_row = lax.broadcasted_iota(jnp.int32, (capacity, tokens), 0).astype(F32)
    for b in range(n):
        has = jnp.zeros((local_e, tokens), F32)
        gate = jnp.zeros((local_e, tokens), F32)
        for j in range(top_k):
            has = has + hit[b, j]
            gate = gate + hit[b, j] * gates_all[b, j:j + 1, :]
        slot = jnp.where((has > 0.0) & (rank[b] < capacity), rank[b], -1.0)
        g1 = jnp.minimum(gate, BIG_BF16).astype(BF16).astype(F32)
        g2 = (gate - g1).astype(BF16).astype(F32)
        g3 = gate - g1 - g2
        packed[b] = jnp.concatenate([slot, g1, g2, g3], axis=0)
        for e in range(local_e):
            pick[e * capacity:(e + 1) * capacity, b * tokens:(b + 1) * tokens] = jnp.where(
                slot[e:e + 1, :] == slot_row, 1.0, 0.0).astype(BF16)

    acc[...] = jnp.zeros_like(acc)

    part_c = 2 * LANES
    for q in range(4):
        at = lax.broadcasted_iota(jnp.int32, (LANES, slots), 1)
        row = lax.broadcasted_iota(jnp.int32, (LANES, slots), 0) - q * local_e
        spread[:, q * slots:(q + 1) * slots] = jnp.where(
            (at >= row * capacity) & (at < (row + 1) * capacity) & (row >= 0) & (row < local_e), 1.0, 0.0).astype(BF16)

    def mix_rows(b):
        row = pl.multiple_of((lax.rem(b, 2) * chips + b // 2) * tokens, tokens)
        cols = jnp.concatenate(
            [packed[b], jnp.zeros((LANES - 4 * local_e, tokens), F32)], axis=0).T.astype(BF16)
        for p in range(slots // part_c):
            at = lax.broadcasted_iota(jnp.int32, (1, part_c), 1) + p * part_c
            rel = at
            for e in range(1, local_e):
                rel = jnp.where(at >= e * capacity, at - e * capacity, rel)
            rel = rel.astype(F32)

            def repeat(q):
                return jnp.dot(cols, spread[:, q * slots + p * part_c:q * slots + (p + 1) * part_c],
                               preferred_element_type=F32)

            slot_at = repeat(0)
            for k in range(3):
                mix[k, pl.ds(row, tokens), p * part_c:(p + 1) * part_c] = jnp.where(
                    slot_at == rel, repeat(k + 1), 0.0).astype(BF16)

    def mix_range(lo, hi):
        with jax.named_scope("mix"):
            pl.loop(lo, hi)(mix_rows)

    with jax.named_scope("s1"):
        stage1(0)
        send_own(AHEAD)
    mix_range(0, n // 2)
    with jax.named_scope("s1"):
        stage1(1)
        send_own(AHEAD + 1)
    with jax.named_scope("s2"):
        stage2(0)

    pick_rows = slots // PICK_PARTS

    def gather(kc):
        for i in range(PICK_PARTS):
            val = jnp.dot(pick[i * pick_rows:(i + 1) * pick_rows, :], x_all[kc], preferred_element_type=F32)
            xg[i * pick_rows // capacity:(i + 1) * pick_rows // capacity] = val.astype(BF16).reshape(
                pick_rows // capacity, capacity, kc_n)

    with jax.named_scope("s1"):
        stage1(2)
        send_own(AHEAD + 2)
    mix_range(n // 2, n)

    @pl.loop(0, IN_BLOCKS - 1)
    def _(kc):
        with jax.named_scope("s1"):
            @pl.when(kc + 3 < IN_BLOCKS)
            def _():
                stage1(kc + 3)

            @pl.when(kc + 3 + AHEAD < IN_BLOCKS)
            def _():
                send_own(kc + 3 + AHEAD)

        with jax.named_scope("s2"):
            stage2(kc + 1)
        with jax.named_scope("s3"):
            stage3(kc)

        with jax.named_scope("up"):
            win_wait(kc)

            @alone
            def _():
                gather(kc)
                for e in range(local_e):
                    acc[e] = acc[e] + jnp.dot(xg[e], win_buf[lax.rem(kc, IN_DEPTH), e], preferred_element_type=F32)

            @pl.when(kc + IN_DEPTH < IN_BLOCKS)
            def _():
                for e in range(local_e):
                    win_copy(e, kc + IN_DEPTH).start()

    last = IN_BLOCKS - 1
    with jax.named_scope("s3"):
        stage3(last)
    def rcopy(kind, oc, src, dst, to):
        ssem = r_ssem.at[lax.rem(oc, 2)] if kind in (PART, PART_REST) else r_ssem.at[kind + 1]
        group = 0 if kind == PART else 1 if kind in (FAR_R, FAR_L) else 2 if kind != PART_REST else 3
        return pltpu.make_async_remote_copy(
            src_ref=src, dst_ref=dst, send_sem=ssem, recv_sem=r_rsem.at[group, oc],
            device_id={AXIS: to}, device_id_type=MESH)

    def r_copy(kind, oc):
        if kind == PART:
            return rcopy(kind, oc, part_send.at[lax.rem(oc, 2), c_far], part_recv.at[oc, c_far], buddy)
        if kind == FAR_R:
            return rcopy(kind, oc, total.at[oc, c_far, 0], far_recv.at[oc, 0], right)
        if kind == FAR_L:
            return rcopy(kind, oc, total.at[oc, c_far, 1], far_recv.at[oc, 1], left)
        if kind == NEAR_R:
            return rcopy(kind, oc, total.at[oc, c_right, 1], fin_recv.at[oc, 0, 1], right)
        if kind == NEAR_L:
            return rcopy(kind, oc, total.at[oc, c_left, 0], fin_recv.at[oc, 1, 0], left)
        if kind == MIX_R:
            return rcopy(kind, oc, total.at[oc, c_right, 0], fin_recv.at[oc, 0, 0], right)
        return rcopy(kind, oc, total.at[oc, c_left, 1], fin_recv.at[oc, 1, 1], left)

    rows = chips * tokens
    half = OUT_COLS // 2

    def partial_of(rail, t, obuf, dst):
        at = pl.multiple_of(rail * rows + t * tokens, tokens)
        val = jnp.dot(mix[0, pl.ds(at, tokens), :], obuf[...], preferred_element_type=F32)
        val += jnp.dot(mix[1, pl.ds(at, tokens), :], obuf[...], preferred_element_type=F32)
        val += jnp.dot(mix[2, pl.ds(at, tokens), :], obuf[...], preferred_element_type=F32)
        for h in range(2):
            dst[t, h] = val[:, h * half:(h + 1) * half]

    def finish_far(oc):
        rcopy(FAR_R, oc, far_recv.at[oc], far_recv.at[oc], buddy).wait_recv()
        total[oc, c_right, 0] = total[oc, c_right, 0] + far_recv[oc, 0]
        r_copy(MIX_R, oc).start()
        total[oc, c_left, 1] = total[oc, c_left, 1] + far_recv[oc, 1]
        r_copy(MIX_L, oc).start()

    per_in = kc_n // OUT_COLS

    def finish(oc):
        rcopy(NEAR_R, oc, fin_recv.at[oc], fin_recv.at[oc], buddy).wait_recv()
        for h in range(2):
            at = pl.multiple_of(lax.rem(oc, per_in) * OUT_COLS + h * half, half)
            x_own = x_all[oc // per_in, pl.ds(pl.multiple_of(me * tokens, tokens), tokens), pl.ds(at, half)]
            val = total[oc, chip, h] + fin_recv[oc, 0, h] + fin_recv[oc, 1, h]
            to = pl.multiple_of(oc * OUT_COLS + h * half, half)
            out_ref[:, pl.ds(to, half)] = (x_own.astype(F32) + val).astype(BF16)

    def down_one(oc, e, obuf):
        val = jnp.dot(hid[e], wout_buf[lax.rem(oc, OUT_DEPTH), e], preferred_element_type=F32)
        obuf[e * capacity:(e + 1) * capacity, :] = val.astype(BF16)

    def down(oc, obuf):
        for e in range(local_e):
            down_one(oc, e, obuf)

    def refill(oc):
        for e in range(local_e):
            wout_copy(e, oc).start()

    def part_sent(oc):
        sent = part_send.at[lax.rem(oc, 2)]
        rcopy(PART, oc, sent, sent, buddy).wait_send()

    def part_rest(oc):
        for t in (c_right, c_left, chip):
            rcopy(PART_REST, oc, part_send.at[lax.rem(oc, 2), t], part_recv.at[oc, t], buddy).start()

    def step(oc, now, nxt, first=False):
        near = (c_right, c_left, chip)
        slot = lax.rem(oc, 2)
        if not first:
            @pl.when(oc >= 2)
            def _():
                part_sent(oc - 2)

        with jax.named_scope("partF"):
            @alone
            def _():
                partial_of(other, c_far, now, part_send.at[slot])
                partial_of(core, c_far, now, total.at[oc])
            r_copy(PART, oc).start()
        with jax.named_scope("partA"):
            @alone
            def _():
                for t in near:
                    partial_of(other, t, now, part_send.at[slot])
            part_rest(oc)
        with jax.named_scope("part_wait"):
            r_copy(PART, oc).wait_recv()
        total[oc, c_far] = total[oc, c_far] + part_recv[oc, c_far]
        for kind in (FAR_R, FAR_L):
            r_copy(kind, oc).start()
        if not first:
            with jax.named_scope("far"):
                finish_far(oc - 1)
        if nxt is not None:
            wout_wait(oc + 1)
        with jax.named_scope("partB"):
            @alone
            def _():
                for t in near:
                    partial_of(core, t, now, total.at[oc])
                if nxt is not None:
                    down(oc + 1, nxt)
        with jax.named_scope("rest_wait"):
            rest = part_recv.at[oc, pl.ds(0, chips - 1)]
            rcopy(PART_REST, oc, rest, rest, buddy).wait_recv()
        for t in near:
            total[oc, t] = total[oc, t] + part_recv[oc, t]
        for kind in (NEAR_R, NEAR_L):
            r_copy(kind, oc).start()
        if nxt is not None:
            @pl.when(oc + 1 + OUT_DEPTH < oc_n)
            def _():
                refill(oc + 1 + OUT_DEPTH)
        if not first:
            @pl.when(oc >= LAG)
            def _():
                with jax.named_scope("fin"):
                    finish(oc - LAG)

    with jax.named_scope("up_last"):
        win_wait(last)
        wout_wait(0)

        @alone
        def _():
            gather(last)
            for e in range(local_e):
                up = acc[e] + jnp.dot(xg[e], win_buf[last % IN_DEPTH, e], preferred_element_type=F32)
                hid[e] = gelu(up).astype(BF16)
                if e >= BEHIND:
                    down_one(0, e - BEHIND, obuf0)
            for e in range(local_e - BEHIND, local_e):
                down_one(0, e, obuf0)

        refill(OUT_DEPTH)

    step(0, obuf0, obuf1, True)

    @pl.loop(0, oc_n // 2 - 1)
    def _(i):
        step(2 * i + 1, obuf1, obuf0)
        step(2 * i + 2, obuf0, obuf1)

    step(oc_n - 1, obuf1, None)

    for kind, rows_sent in ((OWN_R, 2), (OWN_L, 2), (OWN_P, 2), (RELAY_R, 1), (RELAY_L, 1),
                            (FWD_L, 2), (FWD_R, 2), (FWD_A, 1), (FWD_B, 1)):
        d_flush(kind, rows_sent * tokens // 2)
    for c in meta_all():
        c.wait_send()

    with jax.named_scope("far_t"):
        finish_far(oc_n - 1)
    for oc in range(oc_n - LAG, oc_n):
        with jax.named_scope("fin_t"):
            finish(oc)

    with jax.named_scope("drain"):
        part_sent(oc_n - 2)
        part_sent(oc_n - 1)
        for kind in (FAR_R, FAR_L, NEAR_R, NEAR_L, MIX_R, MIX_L):
            sent = total.at[:, 0, 0]
            rcopy(kind, 0, sent, sent, buddy).wait_send()


def solution(mesh):
    n = mesh.shape[AXIS]
    row_spec = P(("data", AXIS), None)
    weight_spec = P(AXIS, None, None)

    def device_step(token_rows, expert_ids, gate_weights, w_in, w_out):
        tokens, top_k = expert_ids.shape
        local_e, model, hidden = w_in.shape
        capacity = n * tokens * top_k // (n * local_e)
        slots = local_e * capacity
        chips = n // 2
        kc_n = model // IN_BLOCKS
        oc_n = model // OUT_COLS
        half = OUT_COLS // 2
        hbm = pl.BlockSpec(memory_space=pl.ANY)
        dma = pltpu.SemaphoreType.DMA
        return pl.pallas_call(
            functools.partial(body, n, capacity),
            out_shape=pltpu.VMEM((tokens, model), BF16),
            in_specs=[hbm, hbm, hbm, hbm, hbm],
            out_specs=pl.BlockSpec(memory_space=pltpu.VMEM),
            scratch_shapes=[
                pltpu.VMEM((n, top_k, tokens), jnp.int32),
                pltpu.VMEM((n, top_k, tokens), F32),
                pltpu.VMEM((IN_BLOCKS, n * tokens, kc_n), BF16),
                pltpu.VMEM((slots, n * tokens), BF16),
                pltpu.VMEM((n, 4 * local_e, tokens), F32),
                pltpu.VMEM((3, n * tokens, slots), BF16),
                pltpu.VMEM((local_e, capacity, kc_n), BF16),
                pltpu.VMEM((local_e, capacity, hidden), F32),
                pltpu.VMEM((local_e, capacity, hidden), BF16),
                pltpu.VMEM((LANES, 4 * slots), BF16),
                pltpu.VMEM((slots, OUT_COLS), BF16),
                pltpu.VMEM((slots, OUT_COLS), BF16),
                pltpu.VMEM((2, chips, 2, tokens, half), F32),
                pltpu.VMEM((oc_n, chips, 2, tokens, half), F32),
                pltpu.VMEM((oc_n, chips, 2, tokens, half), F32),
                pltpu.VMEM((oc_n, 2, tokens, half), F32),
                pltpu.VMEM((oc_n, 2, 2, tokens, half), F32),
                pltpu.VMEM((IN_DEPTH, local_e, kc_n, hidden), BF16),
                pltpu.VMEM((OUT_DEPTH, local_e, hidden, OUT_COLS), BF16),
                dma((2,)), dma((2,)),
                dma((9,)), dma((3, IN_BLOCKS)),
                dma((8,)), dma((4, oc_n)),
                dma,
                dma((IN_DEPTH,)),
                dma((OUT_DEPTH,)),
                dma((2,)),
            ],
            compiler_params=pltpu.CompilerParams(
                collective_id=0, has_side_effects=True, vmem_limit_bytes=VMEM_BYTES),
        )(expert_ids.T, gate_weights.T, token_rows, w_in, w_out)

    return jax.shard_map(device_step, mesh=mesh, in_specs=(row_spec, row_spec, row_spec, weight_spec, weight_spec),
                         out_specs=row_spec, check_vma=False)
```

```python
import functools

import jax
import jax.numpy as jnp
from jax import lax
from jax.experimental import pallas as pl
from jax.experimental.pallas import tpu as pltpu
from jax.sharding import PartitionSpec as P

MESH = pl.DeviceIdType.MESH
F32 = jnp.float32
BF16 = jnp.bfloat16
AXIS = "expert"
LANES = 128
IN_BLOCKS = 8
IN_DEPTH = 3
OUT_COLS = 256
OUT_DEPTH = 2
AHEAD = 3
LAG = 3
VMEM_BYTES = 62 * 2 ** 20
GELU_A = 0.7978845608028654
GELU_B = 0.044715 * GELU_A
PICK_PARTS = 4
BEHIND = 1
BIG_BF16 = 3.3895313892515355e38

OWN_R, OWN_L, OWN_P, RELAY_R, RELAY_L, FWD_L, FWD_R, FWD_A, FWD_B = range(9)
PART, FAR_R, FAR_L, NEAR_R, NEAR_L, MIX_R, MIX_L, PART_REST = range(8)


def gelu(x):
    half = 0.5 * x
    return half + half * jnp.tanh(x * (GELU_A + GELU_B * (x * x)))


def body(n, capacity, ids_hbm, gate_hbm, x_hbm, w_in, w_out, out_ref,
         ids_all, gates_all, x_all, pick, packed, mix, xg, acc, hid, spread, obuf0, obuf1,
         part_send, part_recv, total, far_recv, fin_recv, win_buf, wout_buf,
         meta_ssem, meta_rsem, d_ssem, d_rsem, r_ssem, r_rsem, p_rsem, x_sem, win_sem, wout_sem, own_sem):
    top_k, tokens = ids_hbm.shape
    local_e, model, hidden = w_in.shape
    chips = n // 2
    kc_n = model // IN_BLOCKS
    oc_n = model // OUT_COLS
    slots = local_e * capacity

    me = lax.axis_index(AXIS)
    core = lax.rem(me, 2)
    chip = me // 2
    buddy = me + 1 - 2 * core
    other = 1 - core
    c_right = lax.rem(chip + 1, chips)
    c_far = lax.rem(chip + 2, chips)
    c_left = lax.rem(chip + 3, chips)

    def dev(c, k):
        return 2 * c + k

    right = dev(c_right, core)
    left = dev(c_left, core)

    def alone(fn):
        pl.when(me >= 0)(fn)

    def win_copy(e, kc):
        slot = lax.rem(kc, IN_DEPTH)
        return pltpu.make_async_copy(
            w_in.at[e, pl.ds(kc * kc_n, kc_n), :], win_buf.at[slot, e], win_sem.at[slot])

    def win_wait(kc):
        slot = lax.rem(kc, IN_DEPTH)
        pltpu.make_async_copy(w_in.at[:, pl.ds(0, kc_n), :], win_buf.at[slot], win_sem.at[slot]).wait()

    def wout_copy(e, oc):
        slot = lax.rem(oc, OUT_DEPTH)
        return pltpu.make_async_copy(
            w_out.at[e, :, pl.ds(oc * OUT_COLS, OUT_COLS)], wout_buf.at[slot, e], wout_sem.at[slot])

    def wout_wait(oc):
        slot = lax.rem(oc, OUT_DEPTH)
        pltpu.make_async_copy(w_out.at[:, :, pl.ds(0, OUT_COLS)], wout_buf.at[slot], wout_sem.at[slot]).wait()

    def x_rows(kc, d):
        return x_all.at[kc, pl.ds(d * tokens, tokens), :]

    def x_half(kc, d, h):
        half = tokens // 2
        return x_all.at[kc, pl.ds(d * tokens + h * half, half), :]

    def x_copy(kc):
        return pltpu.make_async_copy(
            x_hbm.at[:, pl.ds(kc * kc_n, kc_n)], x_rows(kc, me), x_sem)

    barrier = pltpu.get_barrier_semaphore()
    for d in range(1, n):
        pl.semaphore_signal(barrier, inc=1, device_id={AXIS: lax.rem(me + d, n)}, device_id_type=MESH)

    own_meta = (
        pltpu.make_async_copy(ids_hbm, ids_all.at[me], own_sem.at[0]),
        pltpu.make_async_copy(gate_hbm, gates_all.at[me], own_sem.at[1]),
    )
    for c in own_meta:
        c.start()
    for kc in range(IN_BLOCKS):
        x_copy(kc).start()

    @pl.loop(0, IN_DEPTH)
    def _(kc):
        for e in range(local_e):
            win_copy(e, kc).start()

    @pl.loop(0, OUT_DEPTH)
    def _(oc):
        for e in range(local_e):
            wout_copy(e, oc).start()

    with jax.named_scope("barrier"):
        pl.semaphore_wait(barrier, n - 1)
        for c in own_meta:
            c.wait()

    def meta_copies(d):
        to = lax.rem(me + d, n)
        return (
            pltpu.make_async_remote_copy(
                src_ref=ids_all.at[me], dst_ref=ids_all.at[me], send_sem=meta_ssem.at[0], recv_sem=meta_rsem.at[0],
                device_id={AXIS: to}, device_id_type=MESH),
            pltpu.make_async_remote_copy(
                src_ref=gates_all.at[me], dst_ref=gates_all.at[me], send_sem=meta_ssem.at[1], recv_sem=meta_rsem.at[1],
                device_id={AXIS: to}, device_id_type=MESH),
        )

    def meta_all():
        ids_part, gates_part = ids_all.at[pl.ds(0, n - 1)], gates_all.at[pl.ds(0, n - 1)]
        return (
            pltpu.make_async_remote_copy(
                src_ref=ids_part, dst_ref=ids_part, send_sem=meta_ssem.at[0], recv_sem=meta_rsem.at[0],
                device_id={AXIS: buddy}, device_id_type=MESH),
            pltpu.make_async_remote_copy(
                src_ref=gates_part, dst_ref=gates_part, send_sem=meta_ssem.at[1], recv_sem=meta_rsem.at[1],
                device_id={AXIS: buddy}, device_id_type=MESH),
        )

    for d in range(1, n):
        for c in meta_copies(d):
            c.start()

    def dcopy(kind, kc, ref, to):
        group = 0 if kind in (OWN_R, OWN_L) else 1 if kind in (RELAY_R, RELAY_L) else 2
        return pltpu.make_async_remote_copy(
            src_ref=ref, dst_ref=ref, send_sem=d_ssem, recv_sem=d_rsem.at[group, kc],
            device_id={AXIS: to}, device_id_type=MESH)

    def d_wait(kind, kc, rows):
        dcopy(kind, kc, x_all.at[kc, pl.ds(0, rows), :], buddy).wait_recv()

    def d_flush():
        sent = x_all.at[:, pl.ds(0, 7 * tokens), :]
        dcopy(OWN_R, 0, sent, buddy).wait_send()

    far = dev(c_far, core)

    def d_sent(kind, kc):
        if kind == OWN_R:
            return dcopy(kind, kc, x_rows(kc, me), right)
        if kind == OWN_L:
            return dcopy(kind, kc, x_rows(kc, me), left)
        if kind == OWN_P:
            return dcopy(kind, kc, x_rows(kc, me), buddy)
        if kind == RELAY_R:
            return dcopy(kind, kc, x_half(kc, left, 0), right)
        if kind == RELAY_L:
            return dcopy(kind, kc, x_half(kc, right, 1), left)
        if kind == FWD_L:
            return dcopy(kind, kc, x_rows(kc, left), buddy)
        if kind == FWD_R:
            return dcopy(kind, kc, x_rows(kc, right), buddy)
        if kind == FWD_A:
            return dcopy(kind, kc, x_half(kc, far, 0), buddy)
        return dcopy(kind, kc, x_half(kc, far, 1), buddy)

    def send_own(kc):
        for kind in (OWN_R, OWN_L, OWN_P):
            d_sent(kind, kc).start()

    def stage1(kc):
        d_wait(OWN_R, kc, 2 * tokens)
        for kind in (RELAY_R, RELAY_L, FWD_L, FWD_R):
            d_sent(kind, kc).start()

    def stage2(kc):
        d_wait(RELAY_R, kc, tokens)
        for kind in (FWD_A, FWD_B):
            d_sent(kind, kc).start()

    def stage3(kc):
        d_wait(OWN_P, kc, chips * tokens)

    with jax.named_scope("own"):
        mine = x_all.at[:, pl.ds(me * tokens, tokens), :]
        pltpu.make_async_copy(mine, mine, x_sem).wait()
        for kc in range(AHEAD):
            send_own(kc)

    with jax.named_scope("meta_wait"):
        for c in meta_all():
            c.wait_recv()

    sub = lax.broadcasted_iota(jnp.int32, (local_e, tokens), 0) + me * local_e
    hit = {}
    for b in range(n):
        for j in range(top_k):
            hit[b, j] = jnp.where(ids_all[b, j:j + 1, :] == sub, 1.0, 0.0).astype(F32)
    hits = jnp.concatenate([hit[b, j] for b in range(n) for j in range(top_k)], axis=0).astype(BF16)
    t_from = lax.broadcasted_iota(jnp.int32, (tokens, tokens), 0)
    t_to = lax.broadcasted_iota(jnp.int32, (tokens, tokens), 1)
    earlier = jnp.where(t_from < t_to, 1.0, 0.0).astype(BF16)
    ones = jnp.full((tokens, tokens), 1.0, BF16)
    within = jnp.dot(hits, earlier, preferred_element_type=F32)
    sums = jnp.dot(hits, ones, preferred_element_type=F32)
    running = jnp.zeros((local_e, tokens), F32)
    rank = [jnp.zeros((local_e, tokens), F32) for _ in range(n)]
    for j in range(top_k):
        for b in range(n):
            at = (b * top_k + j) * local_e
            rank[b] = rank[b] + hit[b, j] * (running + within[at:at + local_e])
            running = running + sums[at:at + local_e]
    slot_row = lax.broadcasted_iota(jnp.int32, (capacity, tokens), 0).astype(F32)
    for b in range(n):
        has = jnp.zeros((local_e, tokens), F32)
        gate = jnp.zeros((local_e, tokens), F32)
        for j in range(top_k):
            has = has + hit[b, j]
            gate = gate + hit[b, j] * gates_all[b, j:j + 1, :]
        slot = jnp.where((has > 0.0) & (rank[b] < capacity), rank[b], -1.0)
        g1 = jnp.minimum(gate, BIG_BF16).astype(BF16).astype(F32)
        g2 = (gate - g1).astype(BF16).astype(F32)
        g3 = gate - g1 - g2
        packed[b] = jnp.concatenate([slot, g1, g2, g3], axis=0)
        for e in range(local_e):
            pick[e * capacity:(e + 1) * capacity, b * tokens:(b + 1) * tokens] = jnp.where(
                slot[e:e + 1, :] == slot_row, 1.0, 0.0).astype(BF16)

    acc[...] = jnp.zeros_like(acc)

    part_c = 2 * LANES
    for q in range(4):
        at = lax.broadcasted_iota(jnp.int32, (LANES, slots), 1)
        row = lax.broadcasted_iota(jnp.int32, (LANES, slots), 0) - q * local_e
        spread[:, q * slots:(q + 1) * slots] = jnp.where(
            (at >= row * capacity) & (at < (row + 1) * capacity) & (row >= 0) & (row < local_e), 1.0, 0.0).astype(BF16)

    def mix_rows(b):
        row = pl.multiple_of((lax.rem(b, 2) * chips + b // 2) * tokens, tokens)
        cols = jnp.concatenate(
            [packed[b], jnp.zeros((LANES - 4 * local_e, tokens), F32)], axis=0).T.astype(BF16)
        for p in range(slots // part_c):
            at = lax.broadcasted_iota(jnp.int32, (1, part_c), 1) + p * part_c
            rel = at
            for e in range(1, local_e):
                rel = jnp.where(at >= e * capacity, at - e * capacity, rel)
            rel = rel.astype(F32)

            def repeat(q):
                return jnp.dot(cols, spread[:, q * slots + p * part_c:q * slots + (p + 1) * part_c],
                               preferred_element_type=F32)

            slot_at = repeat(0)
            for k in range(3):
                mix[k, pl.ds(row, tokens), p * part_c:(p + 1) * part_c] = jnp.where(
                    slot_at == rel, repeat(k + 1), 0.0).astype(BF16)

    def mix_range(lo, hi):
        with jax.named_scope("mix"):
            pl.loop(lo, hi)(mix_rows)

    with jax.named_scope("s1"):
        stage1(0)
        send_own(AHEAD)
    mix_range(0, n // 2)
    with jax.named_scope("s1"):
        stage1(1)
        send_own(AHEAD + 1)
    with jax.named_scope("s2"):
        stage2(0)

    pick_rows = slots // PICK_PARTS

    def gather(kc):
        for i in range(PICK_PARTS):
            val = jnp.dot(pick[i * pick_rows:(i + 1) * pick_rows, :], x_all[kc], preferred_element_type=F32)
            xg[i * pick_rows // capacity:(i + 1) * pick_rows // capacity] = val.astype(BF16).reshape(
                pick_rows // capacity, capacity, kc_n)

    with jax.named_scope("s1"):
        stage1(2)
        send_own(AHEAD + 2)
    mix_range(n // 2, n)

    @pl.loop(0, IN_BLOCKS - 1)
    def _(kc):
        with jax.named_scope("s1"):
            @pl.when(kc + 3 < IN_BLOCKS)
            def _():
                stage1(kc + 3)

            @pl.when(kc + 3 + AHEAD < IN_BLOCKS)
            def _():
                send_own(kc + 3 + AHEAD)

        with jax.named_scope("s2"):
            stage2(kc + 1)
        with jax.named_scope("s3"):
            stage3(kc)

        with jax.named_scope("up"):
            win_wait(kc)

            @alone
            def _():
                gather(kc)
                for e in range(local_e):
                    acc[e] = acc[e] + jnp.dot(xg[e], win_buf[lax.rem(kc, IN_DEPTH), e], preferred_element_type=F32)

            @pl.when(kc + IN_DEPTH < IN_BLOCKS)
            def _():
                for e in range(local_e):
                    win_copy(e, kc + IN_DEPTH).start()

    last = IN_BLOCKS - 1
    with jax.named_scope("s3"):
        stage3(last)
    def rcopy(kind, oc, src, dst, to):
        ssem = r_ssem.at[lax.rem(oc, 2)] if kind in (PART, PART_REST) else r_ssem.at[2]
        if kind in (PART, PART_REST):
            rsem = p_rsem.at[int(kind == PART_REST), lax.rem(oc, 2)]
        else:
            rsem = r_rsem.at[int(kind not in (FAR_R, FAR_L)), oc]
        return pltpu.make_async_remote_copy(
            src_ref=src, dst_ref=dst, send_sem=ssem, recv_sem=rsem,
            device_id={AXIS: to}, device_id_type=MESH)

    def r_copy(kind, oc):
        if kind == PART:
            return rcopy(kind, oc, part_send.at[lax.rem(oc, 2), c_far], part_recv.at[oc, c_far], buddy)
        if kind == FAR_R:
            return rcopy(kind, oc, total.at[oc, c_far, 0], far_recv.at[oc, 0], right)
        if kind == FAR_L:
            return rcopy(kind, oc, total.at[oc, c_far, 1], far_recv.at[oc, 1], left)
        if kind == NEAR_R:
            return rcopy(kind, oc, total.at[oc, c_right, 1], fin_recv.at[oc, 0, 1], right)
        if kind == NEAR_L:
            return rcopy(kind, oc, total.at[oc, c_left, 0], fin_recv.at[oc, 1, 0], left)
        if kind == MIX_R:
            return rcopy(kind, oc, total.at[oc, c_right, 0], fin_recv.at[oc, 0, 0], right)
        return rcopy(kind, oc, total.at[oc, c_left, 1], fin_recv.at[oc, 1, 1], left)

    rows = chips * tokens
    half = OUT_COLS // 2

    def partial_of(rail, t, obuf, dst):
        at = pl.multiple_of(rail * rows + t * tokens, tokens)
        val = jnp.dot(mix[0, pl.ds(at, tokens), :], obuf[...], preferred_element_type=F32)
        val += jnp.dot(mix[1, pl.ds(at, tokens), :], obuf[...], preferred_element_type=F32)
        val += jnp.dot(mix[2, pl.ds(at, tokens), :], obuf[...], preferred_element_type=F32)
        for h in range(2):
            dst[t, h] = val[:, h * half:(h + 1) * half]

    def finish_far(oc):
        rcopy(FAR_R, oc, far_recv.at[oc], far_recv.at[oc], buddy).wait_recv()
        total[oc, c_right, 0] = total[oc, c_right, 0] + far_recv[oc, 0]
        r_copy(MIX_R, oc).start()
        total[oc, c_left, 1] = total[oc, c_left, 1] + far_recv[oc, 1]
        r_copy(MIX_L, oc).start()

    per_in = kc_n // OUT_COLS

    def finish(oc):
        rcopy(NEAR_R, oc, fin_recv.at[oc], fin_recv.at[oc], buddy).wait_recv()
        for h in range(2):
            at = pl.multiple_of(lax.rem(oc, per_in) * OUT_COLS + h * half, half)
            x_own = x_all[oc // per_in, pl.ds(pl.multiple_of(me * tokens, tokens), tokens), pl.ds(at, half)]
            val = total[oc, chip, h] + fin_recv[oc, 0, h] + fin_recv[oc, 1, h]
            to = pl.multiple_of(oc * OUT_COLS + h * half, half)
            out_ref[:, pl.ds(to, half)] = (x_own.astype(F32) + val).astype(BF16)

    def down_one(oc, e, obuf):
        val = jnp.dot(hid[e], wout_buf[lax.rem(oc, OUT_DEPTH), e], preferred_element_type=F32)
        obuf[e * capacity:(e + 1) * capacity, :] = val.astype(BF16)

    def down(oc, obuf):
        for e in range(local_e):
            down_one(oc, e, obuf)

    def refill(oc):
        for e in range(local_e):
            wout_copy(e, oc).start()

    def part_sent(oc):
        sent = part_send.at[lax.rem(oc, 2)]
        rcopy(PART, oc, sent, sent, buddy).wait_send()

    def part_rest(oc):
        for t in (c_right, c_left, chip):
            rcopy(PART_REST, oc, part_send.at[lax.rem(oc, 2), t], part_recv.at[oc, t], buddy).start()

    def far_rows(oc, now):
        partial_of(other, c_far, now, part_send.at[lax.rem(oc, 2)])
        partial_of(core, c_far, now, total.at[oc])

    def step(oc, now, nxt, first=False):
        near = (c_right, c_left, chip)
        slot = lax.rem(oc, 2)
        if not first:
            @pl.when(oc >= 2)
            def _():
                part_sent(oc - 2)

        with jax.named_scope("partF"):
            if not first:
                alone(lambda: far_rows(oc, now))
            r_copy(PART, oc).start()
        with jax.named_scope("partA"):
            @alone
            def _():
                for t in near:
                    partial_of(other, t, now, part_send.at[slot])
            part_rest(oc)
        with jax.named_scope("part_wait"):
            r_copy(PART, oc).wait_recv()
        total[oc, c_far] = total[oc, c_far] + part_recv[oc, c_far]
        for kind in (FAR_R, FAR_L):
            r_copy(kind, oc).start()
        if not first:
            with jax.named_scope("far"):
                finish_far(oc - 1)
        if nxt is not None:
            wout_wait(oc + 1)
        with jax.named_scope("partB"):
            @alone
            def _():
                for t in near:
                    partial_of(core, t, now, total.at[oc])
                if nxt is not None:
                    down(oc + 1, nxt)
        with jax.named_scope("rest_wait"):
            rest = part_recv.at[oc, pl.ds(0, chips - 1)]
            rcopy(PART_REST, oc, rest, rest, buddy).wait_recv()
        for t in near:
            total[oc, t] = total[oc, t] + part_recv[oc, t]
        for kind in (NEAR_R, NEAR_L):
            r_copy(kind, oc).start()
        if nxt is not None:
            @pl.when(oc + 1 + OUT_DEPTH < oc_n)
            def _():
                refill(oc + 1 + OUT_DEPTH)
        if not first:
            @pl.when(oc >= LAG)
            def _():
                with jax.named_scope("fin"):
                    finish(oc - LAG)

    with jax.named_scope("up_last"):
        win_wait(last)
        wout_wait(0)

        @alone
        def _():
            gather(last)
            for e in range(local_e):
                up = acc[e] + jnp.dot(xg[e], win_buf[last % IN_DEPTH, e], preferred_element_type=F32)
                hid[e] = gelu(up).astype(BF16)
                if e >= BEHIND:
                    down_one(0, e - BEHIND, obuf0)
            for e in range(local_e - BEHIND, local_e):
                down_one(0, e, obuf0)
            far_rows(0, obuf0)

        refill(OUT_DEPTH)

    step(0, obuf0, obuf1, True)

    @pl.loop(0, oc_n // 2 - 1)
    def _(i):
        step(2 * i + 1, obuf1, obuf0)
        step(2 * i + 2, obuf0, obuf1)

    step(oc_n - 1, obuf1, None)

    d_flush()
    for c in meta_all():
        c.wait_send()

    with jax.named_scope("far_t"):
        finish_far(oc_n - 1)
    for oc in range(oc_n - LAG, oc_n):
        with jax.named_scope("fin_t"):
            finish(oc)

    with jax.named_scope("drain"):
        part_sent(oc_n - 2)
        part_sent(oc_n - 1)
        sent = total.at[:, pl.ds(0, 3)]
        rcopy(FAR_R, 0, sent, sent, buddy).wait_send()


def solution(mesh):
    n = mesh.shape[AXIS]
    row_spec = P(("data", AXIS), None)
    weight_spec = P(AXIS, None, None)

    def device_step(token_rows, expert_ids, gate_weights, w_in, w_out):
        tokens, top_k = expert_ids.shape
        local_e, model, hidden = w_in.shape
        capacity = n * tokens * top_k // (n * local_e)
        slots = local_e * capacity
        chips = n // 2
        kc_n = model // IN_BLOCKS
        oc_n = model // OUT_COLS
        half = OUT_COLS // 2
        hbm = pl.BlockSpec(memory_space=pl.ANY)
        dma = pltpu.SemaphoreType.DMA
        return pl.pallas_call(
            functools.partial(body, n, capacity),
            out_shape=pltpu.VMEM((tokens, model), BF16),
            in_specs=[hbm, hbm, hbm, hbm, hbm],
            out_specs=pl.BlockSpec(memory_space=pltpu.VMEM),
            scratch_shapes=[
                pltpu.VMEM((n, top_k, tokens), jnp.int32),
                pltpu.VMEM((n, top_k, tokens), F32),
                pltpu.VMEM((IN_BLOCKS, n * tokens, kc_n), BF16),
                pltpu.VMEM((slots, n * tokens), BF16),
                pltpu.VMEM((n, 4 * local_e, tokens), F32),
                pltpu.VMEM((3, n * tokens, slots), BF16),
                pltpu.VMEM((local_e, capacity, kc_n), BF16),
                pltpu.VMEM((local_e, capacity, hidden), F32),
                pltpu.VMEM((local_e, capacity, hidden), BF16),
                pltpu.VMEM((LANES, 4 * slots), BF16),
                pltpu.VMEM((slots, OUT_COLS), BF16),
                pltpu.VMEM((slots, OUT_COLS), BF16),
                pltpu.VMEM((2, chips, 2, tokens, half), F32),
                pltpu.VMEM((oc_n, chips, 2, tokens, half), F32),
                pltpu.VMEM((oc_n, chips, 2, tokens, half), F32),
                pltpu.VMEM((oc_n, 2, tokens, half), F32),
                pltpu.VMEM((oc_n, 2, 2, tokens, half), F32),
                pltpu.VMEM((IN_DEPTH, local_e, kc_n, hidden), BF16),
                pltpu.VMEM((OUT_DEPTH, local_e, hidden, OUT_COLS), BF16),
                dma((2,)), dma((2,)),
                dma, dma((3, IN_BLOCKS)),
                dma((3,)), dma((2, oc_n)), dma((2, 2)),
                dma,
                dma((IN_DEPTH,)),
                dma((OUT_DEPTH,)),
                dma((2,)),
            ],
            compiler_params=pltpu.CompilerParams(
                collective_id=0, has_side_effects=True, vmem_limit_bytes=VMEM_BYTES),
        )(expert_ids.T, gate_weights.T, token_rows, w_in, w_out)

    return jax.shard_map(device_step, mesh=mesh, in_specs=(row_spec, row_spec, row_spec, weight_spec, weight_spec),
                         out_specs=row_spec, check_vma=False)
```

```python
import functools

import jax
import jax.numpy as jnp
from jax import lax
from jax.experimental import pallas as pl
from jax.experimental.pallas import tpu as pltpu
from jax.sharding import PartitionSpec as P

MESH = pl.DeviceIdType.MESH
F32 = jnp.float32
BF16 = jnp.bfloat16
AXIS = "expert"
LANES = 128
IN_BLOCKS = 8
IN_DEPTH = 3
OUT_COLS = 256
OUT_DEPTH = 2
AHEAD = 2
LAG = 3
VMEM_BYTES = 62 * 2 ** 20
GELU_A = 0.7978845608028654
GELU_B = 0.044715 * GELU_A
PICK_PARTS = 4
BEHIND = 1
BIG_BF16 = 3.3895313892515355e38

PART, FAR_R, FAR_L, NEAR_R, NEAR_L, MIX_R, MIX_L, PART_REST = range(8)


def gelu(x):
    half = 0.5 * x
    return half + half * jnp.tanh(x * (GELU_A + GELU_B * (x * x)))


def body(n, capacity, ids_hbm, gate_hbm, x_hbm, w_in, w_out, out_ref,
         ids_all, gates_all, x_all, pick, packed, mix, xg, acc, hid, spread, obuf0, obuf1,
         part_send, part_recv, total, far_recv, fin_recv, win_buf, wout_buf,
         meta_ssem, meta_rsem, d_ssem, d_rsem, r_ssem, r_rsem, p_rsem, x_sem, win_sem, wout_sem, own_sem):
    top_k, tokens = ids_hbm.shape
    local_e, model, hidden = w_in.shape
    chips = n // 2
    kc_n = model // IN_BLOCKS
    oc_n = model // OUT_COLS
    slots = local_e * capacity

    me = lax.axis_index(AXIS)
    core = lax.rem(me, 2)
    chip = me // 2
    buddy = me + 1 - 2 * core
    other = 1 - core
    c_right = lax.rem(chip + 1, chips)
    c_far = lax.rem(chip + 2, chips)
    c_left = lax.rem(chip + 3, chips)

    def dev(c, k):
        return 2 * c + k

    right = dev(c_right, core)
    left = dev(c_left, core)

    def alone(fn):
        pl.when(me >= 0)(fn)

    def win_copy(e, kc):
        slot = lax.rem(kc, IN_DEPTH)
        return pltpu.make_async_copy(
            w_in.at[e, pl.ds(kc * kc_n, kc_n), :], win_buf.at[slot, e], win_sem.at[slot])

    def win_wait(kc):
        slot = lax.rem(kc, IN_DEPTH)
        pltpu.make_async_copy(w_in.at[:, pl.ds(0, kc_n), :], win_buf.at[slot], win_sem.at[slot]).wait()

    def wout_copy(e, oc):
        slot = lax.rem(oc, OUT_DEPTH)
        return pltpu.make_async_copy(
            w_out.at[e, :, pl.ds(oc * OUT_COLS, OUT_COLS)], wout_buf.at[slot, e], wout_sem.at[slot])

    def wout_wait(oc):
        slot = lax.rem(oc, OUT_DEPTH)
        pltpu.make_async_copy(w_out.at[:, :, pl.ds(0, OUT_COLS)], wout_buf.at[slot], wout_sem.at[slot]).wait()

    def x_rows(kc, d):
        return x_all.at[kc, pl.ds(d * tokens, tokens), :]

    def x_half(kc, d, h):
        half = tokens // 2
        return x_all.at[kc, pl.ds(d * tokens + h * half, half), :]

    def x_copy(kc):
        return pltpu.make_async_copy(
            x_hbm.at[:, pl.ds(kc * kc_n, kc_n)], x_rows(kc, me), x_sem)

    barrier = pltpu.get_barrier_semaphore()
    for d in range(1, n):
        pl.semaphore_signal(barrier, inc=1, device_id={AXIS: lax.rem(me + d, n)}, device_id_type=MESH)

    own_meta = (
        pltpu.make_async_copy(ids_hbm, ids_all.at[me], own_sem.at[0]),
        pltpu.make_async_copy(gate_hbm, gates_all.at[me], own_sem.at[1]),
    )
    for c in own_meta:
        c.start()
    for kc in range(IN_BLOCKS):
        x_copy(kc).start()

    @pl.loop(0, IN_DEPTH)
    def _(kc):
        for e in range(local_e):
            win_copy(e, kc).start()

    @pl.loop(0, OUT_DEPTH)
    def _(oc):
        for e in range(local_e):
            wout_copy(e, oc).start()

    with jax.named_scope("barrier"):
        pl.semaphore_wait(barrier, n - 1)
        for c in own_meta:
            c.wait()

    def meta_copies(d):
        to = lax.rem(me + d, n)
        return (
            pltpu.make_async_remote_copy(
                src_ref=ids_all.at[me], dst_ref=ids_all.at[me], send_sem=meta_ssem.at[0], recv_sem=meta_rsem.at[0],
                device_id={AXIS: to}, device_id_type=MESH),
            pltpu.make_async_remote_copy(
                src_ref=gates_all.at[me], dst_ref=gates_all.at[me], send_sem=meta_ssem.at[1], recv_sem=meta_rsem.at[1],
                device_id={AXIS: to}, device_id_type=MESH),
        )

    def meta_all():
        ids_part, gates_part = ids_all.at[pl.ds(0, n - 1)], gates_all.at[pl.ds(0, n - 1)]
        return (
            pltpu.make_async_remote_copy(
                src_ref=ids_part, dst_ref=ids_part, send_sem=meta_ssem.at[0], recv_sem=meta_rsem.at[0],
                device_id={AXIS: buddy}, device_id_type=MESH),
            pltpu.make_async_remote_copy(
                src_ref=gates_part, dst_ref=gates_part, send_sem=meta_ssem.at[1], recv_sem=meta_rsem.at[1],
                device_id={AXIS: buddy}, device_id_type=MESH),
        )

    for d in range(1, n):
        for c in meta_copies(d):
            c.start()

    RELAYED, RELAYS, CORE, OTHER = range(4)

    def dcopy(group, kc, ref, to):
        return pltpu.make_async_remote_copy(
            src_ref=ref, dst_ref=ref, send_sem=d_ssem, recv_sem=d_rsem.at[group, kc],
            device_id={AXIS: to}, device_id_type=MESH)

    def d_wait(group, kc, rows):
        dcopy(group, kc, x_all.at[kc, pl.ds(0, rows), :], buddy).wait_recv()

    def d_flush():
        sent = x_all.at[:, pl.ds(0, 7 * tokens), :]
        dcopy(CORE, 0, sent, buddy).wait_send()

    far = dev(c_far, core)

    def send_own(kc):
        dcopy(RELAYED, kc, x_half(kc, me, 0), right).start()
        dcopy(RELAYED, kc, x_half(kc, me, 1), left).start()
        dcopy(OTHER, kc, x_half(kc, me, 1), right).start()
        dcopy(OTHER, kc, x_half(kc, me, 0), left).start()
        dcopy(CORE, kc, x_rows(kc, me), buddy).start()

    def stage1(kc):
        d_wait(RELAYED, kc, tokens)
        dcopy(RELAYS, kc, x_half(kc, left, 0), right).start()
        dcopy(RELAYS, kc, x_half(kc, right, 1), left).start()

    def stage1b(kc):
        d_wait(OTHER, kc, tokens)
        dcopy(CORE, kc, x_rows(kc, left), buddy).start()
        dcopy(CORE, kc, x_rows(kc, right), buddy).start()

    def stage2(kc):
        d_wait(RELAYS, kc, tokens)
        dcopy(CORE, kc, x_rows(kc, far), buddy).start()

    def stage3(kc):
        d_wait(CORE, kc, chips * tokens)

    with jax.named_scope("own"):
        mine = x_all.at[:, pl.ds(me * tokens, tokens), :]
        pltpu.make_async_copy(mine, mine, x_sem).wait()
        for kc in range(AHEAD):
            send_own(kc)

    with jax.named_scope("meta_wait"):
        for c in meta_all():
            c.wait_recv()
    with jax.named_scope("s1"):
        stage1(0)
        send_own(AHEAD)

    sub = lax.broadcasted_iota(jnp.int32, (local_e, tokens), 0) + me * local_e
    hit = {}
    for b in range(n):
        for j in range(top_k):
            hit[b, j] = jnp.where(ids_all[b, j:j + 1, :] == sub, 1.0, 0.0).astype(F32)
    hits = jnp.concatenate([hit[b, j] for b in range(n) for j in range(top_k)], axis=0).astype(BF16)
    t_from = lax.broadcasted_iota(jnp.int32, (tokens, tokens), 0)
    t_to = lax.broadcasted_iota(jnp.int32, (tokens, tokens), 1)
    earlier = jnp.where(t_from < t_to, 1.0, 0.0).astype(BF16)
    ones = jnp.full((tokens, tokens), 1.0, BF16)
    within = jnp.dot(hits, earlier, preferred_element_type=F32)
    sums = jnp.dot(hits, ones, preferred_element_type=F32)
    running = jnp.zeros((local_e, tokens), F32)
    rank = [jnp.zeros((local_e, tokens), F32) for _ in range(n)]
    for j in range(top_k):
        for b in range(n):
            at = (b * top_k + j) * local_e
            rank[b] = rank[b] + hit[b, j] * (running + within[at:at + local_e])
            running = running + sums[at:at + local_e]
    slot_row = lax.broadcasted_iota(jnp.int32, (capacity, tokens), 0).astype(F32)
    for b in range(n):
        has = jnp.zeros((local_e, tokens), F32)
        gate = jnp.zeros((local_e, tokens), F32)
        for j in range(top_k):
            has = has + hit[b, j]
            gate = gate + hit[b, j] * gates_all[b, j:j + 1, :]
        slot = jnp.where((has > 0.0) & (rank[b] < capacity), rank[b], -1.0)
        g1 = jnp.minimum(gate, BIG_BF16).astype(BF16).astype(F32)
        g2 = (gate - g1).astype(BF16).astype(F32)
        g3 = gate - g1 - g2
        packed[b] = jnp.concatenate([slot, g1, g2, g3], axis=0)
        for e in range(local_e):
            pick[e * capacity:(e + 1) * capacity, b * tokens:(b + 1) * tokens] = jnp.where(
                slot[e:e + 1, :] == slot_row, 1.0, 0.0).astype(BF16)

    acc[...] = jnp.zeros_like(acc)

    part_c = 2 * LANES
    for q in range(4):
        at = lax.broadcasted_iota(jnp.int32, (LANES, slots), 1)
        row = lax.broadcasted_iota(jnp.int32, (LANES, slots), 0) - q * local_e
        spread[:, q * slots:(q + 1) * slots] = jnp.where(
            (at >= row * capacity) & (at < (row + 1) * capacity) & (row >= 0) & (row < local_e), 1.0, 0.0).astype(BF16)

    def mix_rows(b):
        row = pl.multiple_of((lax.rem(b, 2) * chips + b // 2) * tokens, tokens)
        cols = jnp.concatenate(
            [packed[b], jnp.zeros((LANES - 4 * local_e, tokens), F32)], axis=0).T.astype(BF16)
        for p in range(slots // part_c):
            at = lax.broadcasted_iota(jnp.int32, (1, part_c), 1) + p * part_c
            rel = at
            for e in range(1, local_e):
                rel = jnp.where(at >= e * capacity, at - e * capacity, rel)
            rel = rel.astype(F32)

            def repeat(q):
                return jnp.dot(cols, spread[:, q * slots + p * part_c:q * slots + (p + 1) * part_c],
                               preferred_element_type=F32)

            slot_at = repeat(0)
            for k in range(3):
                mix[k, pl.ds(row, tokens), p * part_c:(p + 1) * part_c] = jnp.where(
                    slot_at == rel, repeat(k + 1), 0.0).astype(BF16)

    def mix_range(lo, hi):
        with jax.named_scope("mix"):
            pl.loop(lo, hi)(mix_rows)

    with jax.named_scope("s1"):
        stage1(1)
        send_own(AHEAD + 1)
        stage1b(0)
    mix_range(0, n // 2)
    with jax.named_scope("s2"):
        stage2(0)

    pick_rows = slots // PICK_PARTS

    def gather(kc):
        for i in range(PICK_PARTS):
            val = jnp.dot(pick[i * pick_rows:(i + 1) * pick_rows, :], x_all[kc], preferred_element_type=F32)
            xg[i * pick_rows // capacity:(i + 1) * pick_rows // capacity] = val.astype(BF16).reshape(
                pick_rows // capacity, capacity, kc_n)

    with jax.named_scope("s1"):
        stage1(2)
        send_own(AHEAD + 2)
    mix_range(n // 2, n)

    stage1b(1)

    @pl.loop(0, IN_BLOCKS - 1)
    def _(kc):
        with jax.named_scope("s1"):
            @pl.when(kc + 3 < IN_BLOCKS)
            def _():
                stage1(kc + 3)

            @pl.when(kc + 3 + AHEAD < IN_BLOCKS)
            def _():
                send_own(kc + 3 + AHEAD)

            @pl.when(kc + 2 < IN_BLOCKS)
            def _():
                stage1b(kc + 2)

        with jax.named_scope("s2"):
            stage2(kc + 1)
        with jax.named_scope("s3"):
            stage3(kc)

        with jax.named_scope("up"):
            win_wait(kc)

            @alone
            def _():
                gather(kc)
                for e in range(local_e):
                    acc[e] = acc[e] + jnp.dot(xg[e], win_buf[lax.rem(kc, IN_DEPTH), e], preferred_element_type=F32)

            @pl.when(kc + IN_DEPTH < IN_BLOCKS)
            def _():
                for e in range(local_e):
                    win_copy(e, kc + IN_DEPTH).start()

    last = IN_BLOCKS - 1
    with jax.named_scope("s3"):
        stage3(last)
    def rcopy(kind, oc, src, dst, to):
        ssem = r_ssem.at[lax.rem(oc, 2)] if kind in (PART, PART_REST) else r_ssem.at[2]
        if kind in (PART, PART_REST):
            rsem = p_rsem.at[int(kind == PART_REST), lax.rem(oc, 2)]
        else:
            rsem = r_rsem.at[int(kind not in (FAR_R, FAR_L)), oc]
        return pltpu.make_async_remote_copy(
            src_ref=src, dst_ref=dst, send_sem=ssem, recv_sem=rsem,
            device_id={AXIS: to}, device_id_type=MESH)

    def r_copy(kind, oc):
        if kind == PART:
            return rcopy(kind, oc, part_send.at[lax.rem(oc, 2), c_far], part_recv.at[oc, c_far], buddy)
        if kind == FAR_R:
            return rcopy(kind, oc, total.at[oc, c_far, 0], far_recv.at[oc, 0], right)
        if kind == FAR_L:
            return rcopy(kind, oc, total.at[oc, c_far, 1], far_recv.at[oc, 1], left)
        if kind == NEAR_R:
            return rcopy(kind, oc, total.at[oc, c_right, 1], fin_recv.at[oc, 0, 1], right)
        if kind == NEAR_L:
            return rcopy(kind, oc, total.at[oc, c_left, 0], fin_recv.at[oc, 1, 0], left)
        if kind == MIX_R:
            return rcopy(kind, oc, total.at[oc, c_right, 0], fin_recv.at[oc, 0, 0], right)
        return rcopy(kind, oc, total.at[oc, c_left, 1], fin_recv.at[oc, 1, 1], left)

    rows = chips * tokens
    half = OUT_COLS // 2

    def partial_of(rail, t, obuf, dst):
        at = pl.multiple_of(rail * rows + t * tokens, tokens)
        val = jnp.dot(mix[0, pl.ds(at, tokens), :], obuf[...], preferred_element_type=F32)
        val += jnp.dot(mix[1, pl.ds(at, tokens), :], obuf[...], preferred_element_type=F32)
        val += jnp.dot(mix[2, pl.ds(at, tokens), :], obuf[...], preferred_element_type=F32)
        for h in range(2):
            dst[t, h] = val[:, h * half:(h + 1) * half]

    def finish_far(oc):
        rcopy(FAR_R, oc, far_recv.at[oc], far_recv.at[oc], buddy).wait_recv()
        total[oc, c_right, 0] = total[oc, c_right, 0] + far_recv[oc, 0]
        r_copy(MIX_R, oc).start()
        total[oc, c_left, 1] = total[oc, c_left, 1] + far_recv[oc, 1]
        r_copy(MIX_L, oc).start()

    per_in = kc_n // OUT_COLS

    def finish(oc):
        rcopy(NEAR_R, oc, fin_recv.at[oc], fin_recv.at[oc], buddy).wait_recv()
        for h in range(2):
            at = pl.multiple_of(lax.rem(oc, per_in) * OUT_COLS + h * half, half)
            x_own = x_all[oc // per_in, pl.ds(pl.multiple_of(me * tokens, tokens), tokens), pl.ds(at, half)]
            val = total[oc, chip, h] + fin_recv[oc, 0, h] + fin_recv[oc, 1, h]
            to = pl.multiple_of(oc * OUT_COLS + h * half, half)
            out_ref[:, pl.ds(to, half)] = (x_own.astype(F32) + val).astype(BF16)

    def down_one(oc, e, obuf):
        val = jnp.dot(hid[e], wout_buf[lax.rem(oc, OUT_DEPTH), e], preferred_element_type=F32)
        obuf[e * capacity:(e + 1) * capacity, :] = val.astype(BF16)

    def down(oc, obuf):
        for e in range(local_e):
            down_one(oc, e, obuf)

    def refill(oc):
        for e in range(local_e):
            wout_copy(e, oc).start()

    def part_sent(oc):
        sent = part_send.at[lax.rem(oc, 2)]
        rcopy(PART, oc, sent, sent, buddy).wait_send()

    def part_rest(oc):
        for t in (c_right, c_left, chip):
            rcopy(PART_REST, oc, part_send.at[lax.rem(oc, 2), t], part_recv.at[oc, t], buddy).start()

    def far_rows(oc, now):
        partial_of(other, c_far, now, part_send.at[lax.rem(oc, 2)])
        partial_of(core, c_far, now, total.at[oc])

    def step(oc, now, nxt, first=False):
        near = (c_right, c_left, chip)
        slot = lax.rem(oc, 2)
        if not first:
            @pl.when(oc >= 2)
            def _():
                part_sent(oc - 2)

        with jax.named_scope("partF"):
            if not first:
                alone(lambda: far_rows(oc, now))
            r_copy(PART, oc).start()
        with jax.named_scope("partA"):
            @alone
            def _():
                for t in near:
                    partial_of(other, t, now, part_send.at[slot])
            part_rest(oc)
        with jax.named_scope("part_wait"):
            r_copy(PART, oc).wait_recv()
        total[oc, c_far] = total[oc, c_far] + part_recv[oc, c_far]
        for kind in (FAR_R, FAR_L):
            r_copy(kind, oc).start()
        if not first:
            with jax.named_scope("far"):
                finish_far(oc - 1)
        if nxt is not None:
            wout_wait(oc + 1)
        with jax.named_scope("partB"):
            @alone
            def _():
                for t in near:
                    partial_of(core, t, now, total.at[oc])
                if nxt is not None:
                    down(oc + 1, nxt)
        with jax.named_scope("rest_wait"):
            rest = part_recv.at[oc, pl.ds(0, chips - 1)]
            rcopy(PART_REST, oc, rest, rest, buddy).wait_recv()
        for t in near:
            total[oc, t] = total[oc, t] + part_recv[oc, t]
        for kind in (NEAR_R, NEAR_L):
            r_copy(kind, oc).start()
        if nxt is not None:
            @pl.when(oc + 1 + OUT_DEPTH < oc_n)
            def _():
                refill(oc + 1 + OUT_DEPTH)
        if not first:
            @pl.when(oc >= LAG)
            def _():
                with jax.named_scope("fin"):
                    finish(oc - LAG)

    with jax.named_scope("up_last"):
        win_wait(last)
        wout_wait(0)

        @alone
        def _():
            gather(last)
            for e in range(local_e):
                up = acc[e] + jnp.dot(xg[e], win_buf[last % IN_DEPTH, e], preferred_element_type=F32)
                hid[e] = gelu(up).astype(BF16)
                if e >= BEHIND:
                    down_one(0, e - BEHIND, obuf0)
            for e in range(local_e - BEHIND, local_e):
                down_one(0, e, obuf0)
            far_rows(0, obuf0)

        refill(OUT_DEPTH)

    step(0, obuf0, obuf1, True)

    @pl.loop(0, oc_n // 2 - 1)
    def _(i):
        step(2 * i + 1, obuf1, obuf0)
        step(2 * i + 2, obuf0, obuf1)

    step(oc_n - 1, obuf1, None)

    d_flush()
    for c in meta_all():
        c.wait_send()

    with jax.named_scope("far_t"):
        finish_far(oc_n - 1)
    for oc in range(oc_n - LAG, oc_n):
        with jax.named_scope("fin_t"):
            finish(oc)

    with jax.named_scope("drain"):
        part_sent(oc_n - 2)
        part_sent(oc_n - 1)
        sent = total.at[:, pl.ds(0, 3)]
        rcopy(FAR_R, 0, sent, sent, buddy).wait_send()


def solution(mesh):
    n = mesh.shape[AXIS]
    row_spec = P(("data", AXIS), None)
    weight_spec = P(AXIS, None, None)

    def device_step(token_rows, expert_ids, gate_weights, w_in, w_out):
        tokens, top_k = expert_ids.shape
        local_e, model, hidden = w_in.shape
        capacity = n * tokens * top_k // (n * local_e)
        slots = local_e * capacity
        chips = n // 2
        kc_n = model // IN_BLOCKS
        oc_n = model // OUT_COLS
        half = OUT_COLS // 2
        hbm = pl.BlockSpec(memory_space=pl.ANY)
        dma = pltpu.SemaphoreType.DMA
        return pl.pallas_call(
            functools.partial(body, n, capacity),
            out_shape=pltpu.VMEM((tokens, model), BF16),
            in_specs=[hbm, hbm, hbm, hbm, hbm],
            out_specs=pl.BlockSpec(memory_space=pltpu.VMEM),
            scratch_shapes=[
                pltpu.VMEM((n, top_k, tokens), jnp.int32),
                pltpu.VMEM((n, top_k, tokens), F32),
                pltpu.VMEM((IN_BLOCKS, n * tokens, kc_n), BF16),
                pltpu.VMEM((slots, n * tokens), BF16),
                pltpu.VMEM((n, 4 * local_e, tokens), F32),
                pltpu.VMEM((3, n * tokens, slots), BF16),
                pltpu.VMEM((local_e, capacity, kc_n), BF16),
                pltpu.VMEM((local_e, capacity, hidden), F32),
                pltpu.VMEM((local_e, capacity, hidden), BF16),
                pltpu.VMEM((LANES, 4 * slots), BF16),
                pltpu.VMEM((slots, OUT_COLS), BF16),
                pltpu.VMEM((slots, OUT_COLS), BF16),
                pltpu.VMEM((2, chips, 2, tokens, half), F32),
                pltpu.VMEM((oc_n, chips, 2, tokens, half), F32),
                pltpu.VMEM((oc_n, chips, 2, tokens, half), F32),
                pltpu.VMEM((oc_n, 2, tokens, half), F32),
                pltpu.VMEM((oc_n, 2, 2, tokens, half), F32),
                pltpu.VMEM((IN_DEPTH, local_e, kc_n, hidden), BF16),
                pltpu.VMEM((OUT_DEPTH, local_e, hidden, OUT_COLS), BF16),
                dma((2,)), dma((2,)),
                dma, dma((4, IN_BLOCKS)),
                dma((3,)), dma((2, oc_n)), dma((2, 2)),
                dma,
                dma((IN_DEPTH,)),
                dma((OUT_DEPTH,)),
                dma((2,)),
            ],
            compiler_params=pltpu.CompilerParams(
                collective_id=0, has_side_effects=True, vmem_limit_bytes=VMEM_BYTES),
        )(expert_ids.T, gate_weights.T, token_rows, w_in, w_out)

    return jax.shard_map(device_step, mesh=mesh, in_specs=(row_spec, row_spec, row_spec, weight_spec, weight_spec),
                         out_specs=row_spec, check_vma=False)
```

```python
import functools

import jax
import jax.numpy as jnp
from jax import lax
from jax.experimental import pallas as pl
from jax.experimental.pallas import tpu as pltpu
from jax.sharding import PartitionSpec as P

MESH = pl.DeviceIdType.MESH
F32 = jnp.float32
BF16 = jnp.bfloat16
AXIS = "expert"
LANES = 128
IN_BLOCKS = 8
IN_DEPTH = 3
OUT_COLS = 256
OUT_DEPTH = 2
AHEAD = 3
LAG = 3
VMEM_BYTES = 62 * 2 ** 20
GELU_A = 0.7978845608028654
GELU_B = 0.044715 * GELU_A
PICK_PARTS = 4
BEHIND = 1
PICK_COLS = 256
BIG_BF16 = 3.3895313892515355e38

OWN_R, OWN_L, OWN_P, RELAY_R, RELAY_L, FWD_L, FWD_R, FWD_A, FWD_B = range(9)
PART, FAR_R, FAR_L, NEAR_R, NEAR_L, MIX_R, MIX_L, PART_REST = range(8)


def gelu(x):
    half = 0.5 * x
    return half + half * jnp.tanh(x * (GELU_A + GELU_B * (x * x)))


def body(n, capacity, ids_hbm, gate_hbm, x_hbm, w_in, w_out, out_ref,
         ids_all, gates_all, x_all, pick, packed, mix, xg, acc, hid, spread, obuf0, obuf1,
         part_send, part_recv, total, far_recv, fin_recv, win_buf, wout_buf,
         meta_ssem, meta_rsem, d_ssem, d_rsem, r_ssem, r_rsem, p_rsem, x_sem, win_sem, wout_sem, own_sem):
    top_k, tokens = ids_hbm.shape
    local_e, model, hidden = w_in.shape
    chips = n // 2
    kc_n = model // IN_BLOCKS
    oc_n = model // OUT_COLS
    slots = local_e * capacity

    me = lax.axis_index(AXIS)
    core = lax.rem(me, 2)
    chip = me // 2
    buddy = me + 1 - 2 * core
    other = 1 - core
    c_right = lax.rem(chip + 1, chips)
    c_far = lax.rem(chip + 2, chips)
    c_left = lax.rem(chip + 3, chips)

    def dev(c, k):
        return 2 * c + k

    right = dev(c_right, core)
    left = dev(c_left, core)

    def alone(fn):
        pl.when(me >= 0)(fn)

    def win_copy(e, kc):
        slot = lax.rem(kc, IN_DEPTH)
        return pltpu.make_async_copy(
            w_in.at[e, pl.ds(kc * kc_n, kc_n), :], win_buf.at[slot, e], win_sem.at[slot])

    def win_wait(kc):
        slot = lax.rem(kc, IN_DEPTH)
        pltpu.make_async_copy(w_in.at[:, pl.ds(0, kc_n), :], win_buf.at[slot], win_sem.at[slot]).wait()

    def wout_copy(e, oc):
        slot = lax.rem(oc, OUT_DEPTH)
        return pltpu.make_async_copy(
            w_out.at[e, :, pl.ds(oc * OUT_COLS, OUT_COLS)], wout_buf.at[slot, e], wout_sem.at[slot])

    def wout_wait(oc):
        slot = lax.rem(oc, OUT_DEPTH)
        pltpu.make_async_copy(w_out.at[:, :, pl.ds(0, OUT_COLS)], wout_buf.at[slot], wout_sem.at[slot]).wait()

    def x_rows(kc, d):
        return x_all.at[kc, pl.ds(d * tokens, tokens), :]

    def x_half(kc, d, h):
        half = tokens // 2
        return x_all.at[kc, pl.ds(d * tokens + h * half, half), :]

    def x_copy(kc):
        return pltpu.make_async_copy(
            x_hbm.at[:, pl.ds(kc * kc_n, kc_n)], x_rows(kc, me), x_sem)

    barrier = pltpu.get_barrier_semaphore()
    for d in range(1, n):
        pl.semaphore_signal(barrier, inc=1, device_id={AXIS: lax.rem(me + d, n)}, device_id_type=MESH)

    own_meta = (
        pltpu.make_async_copy(ids_hbm, ids_all.at[me], own_sem.at[0]),
        pltpu.make_async_copy(gate_hbm, gates_all.at[me], own_sem.at[1]),
    )
    for c in own_meta:
        c.start()
    for kc in range(IN_BLOCKS):
        x_copy(kc).start()

    @pl.loop(0, IN_DEPTH)
    def _(kc):
        for e in range(local_e):
            win_copy(e, kc).start()

    @pl.loop(0, OUT_DEPTH)
    def _(oc):
        for e in range(local_e):
            wout_copy(e, oc).start()

    with jax.named_scope("barrier"):
        pl.semaphore_wait(barrier, n - 1)
        for c in own_meta:
            c.wait()

    def meta_copies(d):
        to = lax.rem(me + d, n)
        return (
            pltpu.make_async_remote_copy(
                src_ref=ids_all.at[me], dst_ref=ids_all.at[me], send_sem=meta_ssem.at[0], recv_sem=meta_rsem.at[0],
                device_id={AXIS: to}, device_id_type=MESH),
            pltpu.make_async_remote_copy(
                src_ref=gates_all.at[me], dst_ref=gates_all.at[me], send_sem=meta_ssem.at[1], recv_sem=meta_rsem.at[1],
                device_id={AXIS: to}, device_id_type=MESH),
        )

    def meta_all():
        ids_part, gates_part = ids_all.at[pl.ds(0, n - 1)], gates_all.at[pl.ds(0, n - 1)]
        return (
            pltpu.make_async_remote_copy(
                src_ref=ids_part, dst_ref=ids_part, send_sem=meta_ssem.at[0], recv_sem=meta_rsem.at[0],
                device_id={AXIS: buddy}, device_id_type=MESH),
            pltpu.make_async_remote_copy(
                src_ref=gates_part, dst_ref=gates_part, send_sem=meta_ssem.at[1], recv_sem=meta_rsem.at[1],
                device_id={AXIS: buddy}, device_id_type=MESH),
        )

    for d in range(1, n):
        for c in meta_copies(d):
            c.start()

    def dcopy(kind, kc, ref, to):
        group = 0 if kind in (OWN_R, OWN_L) else 1 if kind in (RELAY_R, RELAY_L) else 2
        return pltpu.make_async_remote_copy(
            src_ref=ref, dst_ref=ref, send_sem=d_ssem, recv_sem=d_rsem.at[group, kc],
            device_id={AXIS: to}, device_id_type=MESH)

    def d_wait(kind, kc, rows):
        dcopy(kind, kc, x_all.at[kc, pl.ds(0, rows), :], buddy).wait_recv()

    def d_flush():
        sent = x_all.at[:, pl.ds(0, 7 * tokens), :]
        dcopy(OWN_R, 0, sent, buddy).wait_send()

    far = dev(c_far, core)

    def d_sent(kind, kc):
        if kind == OWN_R:
            return dcopy(kind, kc, x_rows(kc, me), right)
        if kind == OWN_L:
            return dcopy(kind, kc, x_rows(kc, me), left)
        if kind == OWN_P:
            return dcopy(kind, kc, x_rows(kc, me), buddy)
        if kind == RELAY_R:
            return dcopy(kind, kc, x_half(kc, left, 0), right)
        if kind == RELAY_L:
            return dcopy(kind, kc, x_half(kc, right, 1), left)
        if kind == FWD_L:
            return dcopy(kind, kc, x_rows(kc, left), buddy)
        if kind == FWD_R:
            return dcopy(kind, kc, x_rows(kc, right), buddy)
        if kind == FWD_A:
            return dcopy(kind, kc, x_half(kc, far, 0), buddy)
        return dcopy(kind, kc, x_half(kc, far, 1), buddy)

    def send_own(kc):
        for kind in (OWN_R, OWN_L, OWN_P):
            d_sent(kind, kc).start()

    def stage1(kc):
        d_wait(OWN_R, kc, 2 * tokens)
        for kind in (RELAY_R, RELAY_L, FWD_L, FWD_R):
            d_sent(kind, kc).start()

    def stage2(kc):
        d_wait(RELAY_R, kc, tokens)
        for kind in (FWD_A, FWD_B):
            d_sent(kind, kc).start()

    def stage3(kc):
        d_wait(OWN_P, kc, chips * tokens)

    with jax.named_scope("own"):
        mine = x_all.at[:, pl.ds(me * tokens, tokens), :]
        pltpu.make_async_copy(mine, mine, x_sem).wait()
        for kc in range(AHEAD):
            send_own(kc)

    with jax.named_scope("meta_wait"):
        for c in meta_all():
            c.wait_recv()

    sub = lax.broadcasted_iota(jnp.int32, (local_e, tokens), 0) + me * local_e
    hit = {}
    for b in range(n):
        for j in range(top_k):
            hit[b, j] = jnp.where(ids_all[b, j:j + 1, :] == sub, 1.0, 0.0).astype(F32)
    hits = jnp.concatenate([hit[b, j] for b in range(n) for j in range(top_k)], axis=0).astype(BF16)
    t_from = lax.broadcasted_iota(jnp.int32, (tokens, tokens), 0)
    t_to = lax.broadcasted_iota(jnp.int32, (tokens, tokens), 1)
    earlier = jnp.where(t_from < t_to, 1.0, 0.0).astype(BF16)
    ones = jnp.full((tokens, tokens), 1.0, BF16)
    within = jnp.dot(hits, earlier, preferred_element_type=F32)
    sums = jnp.dot(hits, ones, preferred_element_type=F32)
    running = jnp.zeros((local_e, tokens), F32)
    rank = [jnp.zeros((local_e, tokens), F32) for _ in range(n)]
    for j in range(top_k):
        for b in range(n):
            at = (b * top_k + j) * local_e
            rank[b] = rank[b] + hit[b, j] * (running + within[at:at + local_e])
            running = running + sums[at:at + local_e]
    slot_row = lax.broadcasted_iota(jnp.int32, (capacity, tokens), 0).astype(F32)
    for b in range(n):
        has = jnp.zeros((local_e, tokens), F32)
        gate = jnp.zeros((local_e, tokens), F32)
        for j in range(top_k):
            has = has + hit[b, j]
            gate = gate + hit[b, j] * gates_all[b, j:j + 1, :]
        slot = jnp.where((has > 0.0) & (rank[b] < capacity), rank[b], -1.0)
        g1 = jnp.minimum(gate, BIG_BF16).astype(BF16).astype(F32)
        g2 = (gate - g1).astype(BF16).astype(F32)
        g3 = gate - g1 - g2
        packed[b] = jnp.concatenate([slot, g1, g2, g3], axis=0)
        for e in range(local_e):
            at = b * tokens % PICK_COLS
            pick[b * tokens // PICK_COLS, e * capacity:(e + 1) * capacity, at:at + tokens] = jnp.where(
                slot[e:e + 1, :] == slot_row, 1.0, 0.0).astype(BF16)

    acc[...] = jnp.zeros_like(acc)

    part_c = 2 * LANES
    for q in range(4):
        at = lax.broadcasted_iota(jnp.int32, (LANES, slots), 1)
        row = lax.broadcasted_iota(jnp.int32, (LANES, slots), 0) - q * local_e
        spread[:, q * slots:(q + 1) * slots] = jnp.where(
            (at >= row * capacity) & (at < (row + 1) * capacity) & (row >= 0) & (row < local_e), 1.0, 0.0).astype(BF16)

    def mix_rows(b):
        row = pl.multiple_of((lax.rem(b, 2) * chips + b // 2) * tokens, tokens)
        cols = jnp.concatenate(
            [packed[b], jnp.zeros((LANES - 4 * local_e, tokens), F32)], axis=0).T.astype(BF16)
        for p in range(slots // part_c):
            at = lax.broadcasted_iota(jnp.int32, (1, part_c), 1) + p * part_c
            rel = at
            for e in range(1, local_e):
                rel = jnp.where(at >= e * capacity, at - e * capacity, rel)
            rel = rel.astype(F32)

            def repeat(q):
                return jnp.dot(cols, spread[:, q * slots + p * part_c:q * slots + (p + 1) * part_c],
                               preferred_element_type=F32)

            slot_at = repeat(0)
            for k in range(3):
                mix[k, pl.ds(row, tokens), p * part_c:(p + 1) * part_c] = jnp.where(
                    slot_at == rel, repeat(k + 1), 0.0).astype(BF16)

    def mix_range(lo, hi):
        with jax.named_scope("mix"):
            pl.loop(lo, hi)(mix_rows)

    with jax.named_scope("s1"):
        stage1(0)
        send_own(AHEAD)
    mix_range(0, n // 2)
    with jax.named_scope("s1"):
        stage1(1)
        send_own(AHEAD + 1)
    with jax.named_scope("s2"):
        stage2(0)

    pick_rows = slots // PICK_PARTS

    def gather(kc):
        for i in range(PICK_PARTS):
            val = None
            for p in range(n * tokens // PICK_COLS):
                term = jnp.dot(pick[p, i * pick_rows:(i + 1) * pick_rows, :],
                               x_all[kc, p * PICK_COLS:(p + 1) * PICK_COLS, :], preferred_element_type=F32)
                val = term if val is None else val + term
            xg[i * pick_rows // capacity:(i + 1) * pick_rows // capacity] = val.astype(BF16).reshape(
                pick_rows // capacity, capacity, kc_n)

    with jax.named_scope("s1"):
        stage1(2)
        send_own(AHEAD + 2)
    mix_range(n // 2, n)

    @pl.loop(0, IN_BLOCKS - 1)
    def _(kc):
        with jax.named_scope("s1"):
            @pl.when(kc + 3 < IN_BLOCKS)
            def _():
                stage1(kc + 3)

            @pl.when(kc + 3 + AHEAD < IN_BLOCKS)
            def _():
                send_own(kc + 3 + AHEAD)

        with jax.named_scope("s2"):
            stage2(kc + 1)
        with jax.named_scope("s3"):
            stage3(kc)

        with jax.named_scope("up"):
            win_wait(kc)

            @alone
            def _():
                gather(kc)
                for e in range(local_e):
                    acc[e] = acc[e] + jnp.dot(xg[e], win_buf[lax.rem(kc, IN_DEPTH), e], preferred_element_type=F32)

            @pl.when(kc + IN_DEPTH < IN_BLOCKS)
            def _():
                for e in range(local_e):
                    win_copy(e, kc + IN_DEPTH).start()

    last = IN_BLOCKS - 1
    with jax.named_scope("s3"):
        stage3(last)
    def rcopy(kind, oc, src, dst, to):
        ssem = r_ssem.at[lax.rem(oc, 2)] if kind in (PART, PART_REST) else r_ssem.at[2]
        if kind in (PART, PART_REST):
            rsem = p_rsem.at[int(kind == PART_REST), lax.rem(oc, 2)]
        else:
            rsem = r_rsem.at[int(kind not in (FAR_R, FAR_L)), oc]
        return pltpu.make_async_remote_copy(
            src_ref=src, dst_ref=dst, send_sem=ssem, recv_sem=rsem,
            device_id={AXIS: to}, device_id_type=MESH)

    def r_copy(kind, oc):
        if kind == PART:
            return rcopy(kind, oc, part_send.at[lax.rem(oc, 2), c_far], part_recv.at[oc, c_far], buddy)
        if kind == FAR_R:
            return rcopy(kind, oc, total.at[oc, c_far, 0], far_recv.at[oc, 0], right)
        if kind == FAR_L:
            return rcopy(kind, oc, total.at[oc, c_far, 1], far_recv.at[oc, 1], left)
        if kind == NEAR_R:
            return rcopy(kind, oc, total.at[oc, c_right, 1], fin_recv.at[oc, 0, 1], right)
        if kind == NEAR_L:
            return rcopy(kind, oc, total.at[oc, c_left, 0], fin_recv.at[oc, 1, 0], left)
        if kind == MIX_R:
            return rcopy(kind, oc, total.at[oc, c_right, 0], fin_recv.at[oc, 0, 0], right)
        return rcopy(kind, oc, total.at[oc, c_left, 1], fin_recv.at[oc, 1, 1], left)

    rows = chips * tokens
    half = OUT_COLS // 2

    def partial_of(rail, t, obuf, dst):
        at = pl.multiple_of(rail * rows + t * tokens, tokens)
        val = jnp.dot(mix[0, pl.ds(at, tokens), :], obuf[...], preferred_element_type=F32)
        val += jnp.dot(mix[1, pl.ds(at, tokens), :], obuf[...], preferred_element_type=F32)
        val += jnp.dot(mix[2, pl.ds(at, tokens), :], obuf[...], preferred_element_type=F32)
        for h in range(2):
            dst[t, h] = val[:, h * half:(h + 1) * half]

    def finish_far(oc):
        rcopy(FAR_R, oc, far_recv.at[oc], far_recv.at[oc], buddy).wait_recv()
        total[oc, c_right, 0] = total[oc, c_right, 0] + far_recv[oc, 0]
        r_copy(MIX_R, oc).start()
        total[oc, c_left, 1] = total[oc, c_left, 1] + far_recv[oc, 1]
        r_copy(MIX_L, oc).start()

    per_in = kc_n // OUT_COLS

    def finish(oc):
        rcopy(NEAR_R, oc, fin_recv.at[oc], fin_recv.at[oc], buddy).wait_recv()
        for h in range(2):
            at = pl.multiple_of(lax.rem(oc, per_in) * OUT_COLS + h * half, half)
            x_own = x_all[oc // per_in, pl.ds(pl.multiple_of(me * tokens, tokens), tokens), pl.ds(at, half)]
            val = total[oc, chip, h] + fin_recv[oc, 0, h] + fin_recv[oc, 1, h]
            to = pl.multiple_of(oc * OUT_COLS + h * half, half)
            out_ref[:, pl.ds(to, half)] = (x_own.astype(F32) + val).astype(BF16)

    def down_one(oc, e, obuf):
        val = jnp.dot(hid[e], wout_buf[lax.rem(oc, OUT_DEPTH), e], preferred_element_type=F32)
        obuf[e * capacity:(e + 1) * capacity, :] = val.astype(BF16)

    def down(oc, obuf):
        for e in range(local_e):
            down_one(oc, e, obuf)

    def refill(oc):
        for e in range(local_e):
            wout_copy(e, oc).start()

    def part_sent(oc):
        sent = part_send.at[lax.rem(oc, 2)]
        rcopy(PART, oc, sent, sent, buddy).wait_send()

    def part_rest(oc):
        for t in (c_right, c_left, chip):
            rcopy(PART_REST, oc, part_send.at[lax.rem(oc, 2), t], part_recv.at[oc, t], buddy).start()

    def far_rows(oc, now):
        partial_of(other, c_far, now, part_send.at[lax.rem(oc, 2)])
        partial_of(core, c_far, now, total.at[oc])

    def step(oc, now, nxt, first=False):
        near = (c_right, c_left, chip)
        slot = lax.rem(oc, 2)
        if not first:
            @pl.when(oc >= 2)
            def _():
                part_sent(oc - 2)

        with jax.named_scope("partF"):
            if not first:
                alone(lambda: far_rows(oc, now))
            r_copy(PART, oc).start()
        with jax.named_scope("partA"):
            @alone
            def _():
                for t in near:
                    partial_of(other, t, now, part_send.at[slot])
            part_rest(oc)
        with jax.named_scope("part_wait"):
            r_copy(PART, oc).wait_recv()
        total[oc, c_far] = total[oc, c_far] + part_recv[oc, c_far]
        for kind in (FAR_R, FAR_L):
            r_copy(kind, oc).start()
        if not first:
            with jax.named_scope("far"):
                finish_far(oc - 1)
        if nxt is not None:
            wout_wait(oc + 1)
        with jax.named_scope("partB"):
            @alone
            def _():
                for t in near:
                    partial_of(core, t, now, total.at[oc])
                if nxt is not None:
                    down(oc + 1, nxt)
        with jax.named_scope("rest_wait"):
            rest = part_recv.at[oc, pl.ds(0, chips - 1)]
            rcopy(PART_REST, oc, rest, rest, buddy).wait_recv()
        for t in near:
            total[oc, t] = total[oc, t] + part_recv[oc, t]
        for kind in (NEAR_R, NEAR_L):
            r_copy(kind, oc).start()
        if nxt is not None:
            @pl.when(oc + 1 + OUT_DEPTH < oc_n)
            def _():
                refill(oc + 1 + OUT_DEPTH)
        if not first:
            @pl.when(oc >= LAG)
            def _():
                with jax.named_scope("fin"):
                    finish(oc - LAG)

    with jax.named_scope("up_last"):
        win_wait(last)
        wout_wait(0)

        @alone
        def _():
            gather(last)
            for e in range(local_e):
                up = acc[e] + jnp.dot(xg[e], win_buf[last % IN_DEPTH, e], preferred_element_type=F32)
                hid[e] = gelu(up).astype(BF16)
                if e >= BEHIND:
                    down_one(0, e - BEHIND, obuf0)
            for e in range(local_e - BEHIND, local_e):
                down_one(0, e, obuf0)
            far_rows(0, obuf0)

        refill(OUT_DEPTH)

    step(0, obuf0, obuf1, True)

    @pl.loop(0, oc_n // 2 - 1)
    def _(i):
        step(2 * i + 1, obuf1, obuf0)
        step(2 * i + 2, obuf0, obuf1)

    step(oc_n - 1, obuf1, None)

    d_flush()
    for c in meta_all():
        c.wait_send()

    with jax.named_scope("far_t"):
        finish_far(oc_n - 1)
    for oc in range(oc_n - LAG, oc_n):
        with jax.named_scope("fin_t"):
            finish(oc)

    with jax.named_scope("drain"):
        part_sent(oc_n - 2)
        part_sent(oc_n - 1)
        sent = total.at[:, pl.ds(0, 3)]
        rcopy(FAR_R, 0, sent, sent, buddy).wait_send()


def solution(mesh):
    n = mesh.shape[AXIS]
    row_spec = P(("data", AXIS), None)
    weight_spec = P(AXIS, None, None)

    def device_step(token_rows, expert_ids, gate_weights, w_in, w_out):
        tokens, top_k = expert_ids.shape
        local_e, model, hidden = w_in.shape
        capacity = n * tokens * top_k // (n * local_e)
        slots = local_e * capacity
        chips = n // 2
        kc_n = model // IN_BLOCKS
        oc_n = model // OUT_COLS
        half = OUT_COLS // 2
        hbm = pl.BlockSpec(memory_space=pl.ANY)
        dma = pltpu.SemaphoreType.DMA
        return pl.pallas_call(
            functools.partial(body, n, capacity),
            out_shape=pltpu.VMEM((tokens, model), BF16),
            in_specs=[hbm, hbm, hbm, hbm, hbm],
            out_specs=pl.BlockSpec(memory_space=pltpu.VMEM),
            scratch_shapes=[
                pltpu.VMEM((n, top_k, tokens), jnp.int32),
                pltpu.VMEM((n, top_k, tokens), F32),
                pltpu.VMEM((IN_BLOCKS, n * tokens, kc_n), BF16),
                pltpu.VMEM((n * tokens // PICK_COLS, slots, PICK_COLS), BF16),
                pltpu.VMEM((n, 4 * local_e, tokens), F32),
                pltpu.VMEM((3, n * tokens, slots), BF16),
                pltpu.VMEM((local_e, capacity, kc_n), BF16),
                pltpu.VMEM((local_e, capacity, hidden), F32),
                pltpu.VMEM((local_e, capacity, hidden), BF16),
                pltpu.VMEM((LANES, 4 * slots), BF16),
                pltpu.VMEM((slots, OUT_COLS), BF16),
                pltpu.VMEM((slots, OUT_COLS), BF16),
                pltpu.VMEM((2, chips, 2, tokens, half), F32),
                pltpu.VMEM((oc_n, chips, 2, tokens, half), F32),
                pltpu.VMEM((oc_n, chips, 2, tokens, half), F32),
                pltpu.VMEM((oc_n, 2, tokens, half), F32),
                pltpu.VMEM((oc_n, 2, 2, tokens, half), F32),
                pltpu.VMEM((IN_DEPTH, local_e, kc_n, hidden), BF16),
                pltpu.VMEM((OUT_DEPTH, local_e, hidden, OUT_COLS), BF16),
                dma((2,)), dma((2,)),
                dma, dma((3, IN_BLOCKS)),
                dma((3,)), dma((2, oc_n)), dma((2, 2)),
                dma,
                dma((IN_DEPTH,)),
                dma((OUT_DEPTH,)),
                dma((2,)),
            ],
            compiler_params=pltpu.CompilerParams(
                collective_id=0, has_side_effects=True, vmem_limit_bytes=VMEM_BYTES),
        )(expert_ids.T, gate_weights.T, token_rows, w_in, w_out)

    return jax.shard_map(device_step, mesh=mesh, in_specs=(row_spec, row_spec, row_spec, weight_spec, weight_spec),
                         out_specs=row_spec, check_vma=False)
```

```python
import functools

import jax
import jax.numpy as jnp
from jax import lax
from jax.experimental import pallas as pl
from jax.experimental.pallas import tpu as pltpu
from jax.sharding import PartitionSpec as P

MESH = pl.DeviceIdType.MESH
F32 = jnp.float32
BF16 = jnp.bfloat16
AXIS = "expert"
LANES = 128
IN_BLOCKS = 8
IN_DEPTH = 3
OUT_COLS = 256
OUT_DEPTH = 2
AHEAD = 3
LAG = 3
VMEM_BYTES = 62 * 2 ** 20
GELU_A = 0.7978845608028654
GELU_B = 0.044715 * GELU_A
PICK_PARTS = 4
BEHIND = 1
PICK_COLS = 256
BIG_BF16 = 3.3895313892515355e38

OWN_R, OWN_L, OWN_P, RELAY_R, RELAY_L, FWD_L, FWD_R, FWD_A, FWD_B = range(9)
PART, FAR_R, FAR_L, NEAR_R, NEAR_L, MIX_R, MIX_L, PART_REST = range(8)


def gelu(x):
    half = 0.5 * x
    return half + half * jnp.tanh(x * (GELU_A + GELU_B * (x * x)))


def body(n, capacity, ids_hbm, gate_hbm, x_hbm, w_in, w_out, out_ref,
         ids_all, gates_all, x_all, pick, packed, mix, xg, acc, hid, spread, obuf0, obuf1,
         part_send, part_recv, total, far_recv, fin_recv, win_buf, wout_buf,
         meta_ssem, meta_rsem, d_ssem, d_rsem, r_ssem, r_rsem, p_rsem, x_sem, win_sem, wout_sem, own_sem):
    top_k, tokens = ids_hbm.shape
    local_e, model, hidden = w_in.shape
    chips = n // 2
    kc_n = model // IN_BLOCKS
    oc_n = model // OUT_COLS
    slots = local_e * capacity

    me = lax.axis_index(AXIS)
    core = lax.rem(me, 2)
    chip = me // 2
    buddy = me + 1 - 2 * core
    other = 1 - core
    c_right = lax.rem(chip + 1, chips)
    c_far = lax.rem(chip + 2, chips)
    c_left = lax.rem(chip + 3, chips)

    def dev(c, k):
        return 2 * c + k

    right = dev(c_right, core)
    left = dev(c_left, core)

    def alone(fn):
        pl.when(me >= 0)(fn)

    def win_copy(e, kc):
        slot = lax.rem(kc, IN_DEPTH)
        return pltpu.make_async_copy(
            w_in.at[e, pl.ds(kc * kc_n, kc_n), :], win_buf.at[slot, e], win_sem.at[slot])

    def win_wait(kc):
        slot = lax.rem(kc, IN_DEPTH)
        pltpu.make_async_copy(w_in.at[:, pl.ds(0, kc_n), :], win_buf.at[slot], win_sem.at[slot]).wait()

    def wout_copy(e, oc):
        slot = lax.rem(oc, OUT_DEPTH)
        return pltpu.make_async_copy(
            w_out.at[e, :, pl.ds(oc * OUT_COLS, OUT_COLS)], wout_buf.at[slot, e], wout_sem.at[slot])

    def wout_wait(oc):
        slot = lax.rem(oc, OUT_DEPTH)
        pltpu.make_async_copy(w_out.at[:, :, pl.ds(0, OUT_COLS)], wout_buf.at[slot], wout_sem.at[slot]).wait()

    def x_rows(kc, d):
        return x_all.at[kc, pl.ds(d * tokens, tokens), :]

    def x_half(kc, d, h):
        half = tokens // 2
        return x_all.at[kc, pl.ds(d * tokens + h * half, half), :]

    def x_copy(kc):
        return pltpu.make_async_copy(
            x_hbm.at[:, pl.ds(kc * kc_n, kc_n)], x_rows(kc, me), x_sem)

    barrier = pltpu.get_barrier_semaphore()
    for d in range(1, n):
        pl.semaphore_signal(barrier, inc=1, device_id={AXIS: lax.rem(me + d, n)}, device_id_type=MESH)

    own_meta = (
        pltpu.make_async_copy(ids_hbm, ids_all.at[me], own_sem.at[0]),
        pltpu.make_async_copy(gate_hbm, gates_all.at[me], own_sem.at[1]),
    )
    for c in own_meta:
        c.start()
    for kc in range(IN_BLOCKS):
        x_copy(kc).start()

    @pl.loop(0, IN_DEPTH)
    def _(kc):
        for e in range(local_e):
            win_copy(e, kc).start()

    @pl.loop(0, OUT_DEPTH)
    def _(oc):
        for e in range(local_e):
            wout_copy(e, oc).start()

    with jax.named_scope("barrier"):
        pl.semaphore_wait(barrier, n - 1)
        for c in own_meta:
            c.wait()

    def meta_copies(d):
        to = lax.rem(me + d, n)
        return (
            pltpu.make_async_remote_copy(
                src_ref=ids_all.at[me], dst_ref=ids_all.at[me], send_sem=meta_ssem.at[0], recv_sem=meta_rsem.at[0],
                device_id={AXIS: to}, device_id_type=MESH),
            pltpu.make_async_remote_copy(
                src_ref=gates_all.at[me], dst_ref=gates_all.at[me], send_sem=meta_ssem.at[1], recv_sem=meta_rsem.at[1],
                device_id={AXIS: to}, device_id_type=MESH),
        )

    def meta_all():
        ids_part, gates_part = ids_all.at[pl.ds(0, n - 1)], gates_all.at[pl.ds(0, n - 1)]
        return (
            pltpu.make_async_remote_copy(
                src_ref=ids_part, dst_ref=ids_part, send_sem=meta_ssem.at[0], recv_sem=meta_rsem.at[0],
                device_id={AXIS: buddy}, device_id_type=MESH),
            pltpu.make_async_remote_copy(
                src_ref=gates_part, dst_ref=gates_part, send_sem=meta_ssem.at[1], recv_sem=meta_rsem.at[1],
                device_id={AXIS: buddy}, device_id_type=MESH),
        )

    for d in range(1, n):
        for c in meta_copies(d):
            c.start()

    def dcopy(kind, kc, ref, to):
        group = 0 if kind in (OWN_R, OWN_L) else 1 if kind in (RELAY_R, RELAY_L) else 2
        return pltpu.make_async_remote_copy(
            src_ref=ref, dst_ref=ref, send_sem=d_ssem, recv_sem=d_rsem.at[group, kc],
            device_id={AXIS: to}, device_id_type=MESH)

    def d_wait(kind, kc, rows):
        dcopy(kind, kc, x_all.at[kc, pl.ds(0, rows), :], buddy).wait_recv()

    def d_flush():
        sent = x_all.at[:, pl.ds(0, 7 * tokens), :]
        dcopy(OWN_R, 0, sent, buddy).wait_send()

    far = dev(c_far, core)

    def d_sent(kind, kc):
        if kind == OWN_R:
            return dcopy(kind, kc, x_rows(kc, me), right)
        if kind == OWN_L:
            return dcopy(kind, kc, x_rows(kc, me), left)
        if kind == OWN_P:
            return dcopy(kind, kc, x_rows(kc, me), buddy)
        if kind == RELAY_R:
            return dcopy(kind, kc, x_half(kc, left, 0), right)
        if kind == RELAY_L:
            return dcopy(kind, kc, x_half(kc, right, 1), left)
        if kind == FWD_L:
            return dcopy(kind, kc, x_rows(kc, left), buddy)
        if kind == FWD_R:
            return dcopy(kind, kc, x_rows(kc, right), buddy)
        if kind == FWD_A:
            return dcopy(kind, kc, x_half(kc, far, 0), buddy)
        return dcopy(kind, kc, x_half(kc, far, 1), buddy)

    def send_own(kc):
        for kind in (OWN_R, OWN_L, OWN_P):
            d_sent(kind, kc).start()

    def stage1(kc):
        d_wait(OWN_R, kc, 2 * tokens)
        for kind in (RELAY_R, RELAY_L, FWD_L, FWD_R):
            d_sent(kind, kc).start()

    def stage2(kc):
        d_wait(RELAY_R, kc, tokens)
        for kind in (FWD_A, FWD_B):
            d_sent(kind, kc).start()

    def stage3(kc):
        d_wait(OWN_P, kc, chips * tokens)

    with jax.named_scope("own"):
        mine = x_all.at[:, pl.ds(me * tokens, tokens), :]
        pltpu.make_async_copy(mine, mine, x_sem).wait()
        for kc in range(AHEAD):
            send_own(kc)

    acc[...] = jnp.zeros_like(acc)
    for q in range(4):
        at = lax.broadcasted_iota(jnp.int32, (LANES, slots), 1)
        row = lax.broadcasted_iota(jnp.int32, (LANES, slots), 0) - q * local_e
        spread[:, q * slots:(q + 1) * slots] = jnp.where(
            (at >= row * capacity) & (at < (row + 1) * capacity) & (row >= 0) & (row < local_e), 1.0, 0.0).astype(BF16)

    with jax.named_scope("meta_wait"):
        for c in meta_all():
            c.wait_recv()

    sub = lax.broadcasted_iota(jnp.int32, (local_e, tokens), 0) + me * local_e
    hit = {}
    for b in range(n):
        for j in range(top_k):
            hit[b, j] = jnp.where(ids_all[b, j:j + 1, :] == sub, 1.0, 0.0).astype(F32)
    hits = jnp.concatenate([hit[b, j] for b in range(n) for j in range(top_k)], axis=0).astype(BF16)
    t_from = lax.broadcasted_iota(jnp.int32, (tokens, tokens), 0)
    t_to = lax.broadcasted_iota(jnp.int32, (tokens, tokens), 1)
    earlier = jnp.where(t_from < t_to, 1.0, 0.0).astype(BF16)
    ones = jnp.full((tokens, tokens), 1.0, BF16)
    within = jnp.dot(hits, earlier, preferred_element_type=F32)
    sums = jnp.dot(hits, ones, preferred_element_type=F32)
    running = jnp.zeros((local_e, tokens), F32)
    rank = [jnp.zeros((local_e, tokens), F32) for _ in range(n)]
    for j in range(top_k):
        for b in range(n):
            at = (b * top_k + j) * local_e
            rank[b] = rank[b] + hit[b, j] * (running + within[at:at + local_e])
            running = running + sums[at:at + local_e]
    slot_row = lax.broadcasted_iota(jnp.int32, (capacity, tokens), 0).astype(F32)
    for b in range(n):
        has = jnp.zeros((local_e, tokens), F32)
        gate = jnp.zeros((local_e, tokens), F32)
        for j in range(top_k):
            has = has + hit[b, j]
            gate = gate + hit[b, j] * gates_all[b, j:j + 1, :]
        slot = jnp.where((has > 0.0) & (rank[b] < capacity), rank[b], -1.0)
        g1 = jnp.minimum(gate, BIG_BF16).astype(BF16).astype(F32)
        g2 = (gate - g1).astype(BF16).astype(F32)
        g3 = gate - g1 - g2
        packed[b] = jnp.concatenate([slot, g1, g2, g3], axis=0)
        for e in range(local_e):
            at = b * tokens % PICK_COLS
            pick[b * tokens // PICK_COLS, e * capacity:(e + 1) * capacity, at:at + tokens] = jnp.where(
                slot[e:e + 1, :] == slot_row, 1.0, 0.0).astype(BF16)

    part_c = 2 * LANES
    def mix_rows(b):
        row = pl.multiple_of((lax.rem(b, 2) * chips + b // 2) * tokens, tokens)
        cols = jnp.concatenate(
            [packed[b], jnp.zeros((LANES - 4 * local_e, tokens), F32)], axis=0).T.astype(BF16)
        for p in range(slots // part_c):
            at = lax.broadcasted_iota(jnp.int32, (1, part_c), 1) + p * part_c
            rel = at
            for e in range(1, local_e):
                rel = jnp.where(at >= e * capacity, at - e * capacity, rel)
            rel = rel.astype(F32)

            def repeat(q):
                return jnp.dot(cols, spread[:, q * slots + p * part_c:q * slots + (p + 1) * part_c],
                               preferred_element_type=F32)

            slot_at = repeat(0)
            for k in range(3):
                mix[k, pl.ds(row, tokens), p * part_c:(p + 1) * part_c] = jnp.where(
                    slot_at == rel, repeat(k + 1), 0.0).astype(BF16)

    def mix_range(lo, hi):
        with jax.named_scope("mix"):
            pl.loop(lo, hi)(mix_rows)

    with jax.named_scope("s1"):
        stage1(0)
        send_own(AHEAD)
    mix_range(0, n // 2)
    with jax.named_scope("s1"):
        stage1(1)
        send_own(AHEAD + 1)
    with jax.named_scope("s2"):
        stage2(0)

    pick_rows = slots // PICK_PARTS

    def gather(kc):
        for i in range(PICK_PARTS):
            val = None
            for p in range(n * tokens // PICK_COLS):
                term = jnp.dot(pick[p, i * pick_rows:(i + 1) * pick_rows, :],
                               x_all[kc, p * PICK_COLS:(p + 1) * PICK_COLS, :], preferred_element_type=F32)
                val = term if val is None else val + term
            xg[i * pick_rows // capacity:(i + 1) * pick_rows // capacity] = val.astype(BF16).reshape(
                pick_rows // capacity, capacity, kc_n)

    with jax.named_scope("s1"):
        stage1(2)
        send_own(AHEAD + 2)
    mix_range(n // 2, n)

    @pl.loop(0, IN_BLOCKS - 1)
    def _(kc):
        with jax.named_scope("s1"):
            @pl.when(kc + 3 < IN_BLOCKS)
            def _():
                stage1(kc + 3)

            @pl.when(kc + 3 + AHEAD < IN_BLOCKS)
            def _():
                send_own(kc + 3 + AHEAD)

        with jax.named_scope("s2"):
            stage2(kc + 1)
        with jax.named_scope("s3"):
            stage3(kc)

        with jax.named_scope("up"):
            win_wait(kc)

            @alone
            def _():
                gather(kc)
                for e in range(local_e):
                    acc[e] = acc[e] + jnp.dot(xg[e], win_buf[lax.rem(kc, IN_DEPTH), e], preferred_element_type=F32)

            @pl.when(kc + IN_DEPTH < IN_BLOCKS)
            def _():
                for e in range(local_e):
                    win_copy(e, kc + IN_DEPTH).start()

    last = IN_BLOCKS - 1
    with jax.named_scope("s3"):
        stage3(last)
    def rcopy(kind, oc, src, dst, to):
        ssem = r_ssem.at[lax.rem(oc, 2)] if kind in (PART, PART_REST) else r_ssem.at[2]
        if kind in (PART, PART_REST):
            rsem = p_rsem.at[int(kind == PART_REST), lax.rem(oc, 2)]
        else:
            rsem = r_rsem.at[int(kind not in (FAR_R, FAR_L)), oc]
        return pltpu.make_async_remote_copy(
            src_ref=src, dst_ref=dst, send_sem=ssem, recv_sem=rsem,
            device_id={AXIS: to}, device_id_type=MESH)

    def r_copy(kind, oc):
        if kind == PART:
            return rcopy(kind, oc, part_send.at[lax.rem(oc, 2), c_far], part_recv.at[oc, c_far], buddy)
        if kind == FAR_R:
            return rcopy(kind, oc, total.at[oc, c_far, 0], far_recv.at[oc, 0], right)
        if kind == FAR_L:
            return rcopy(kind, oc, total.at[oc, c_far, 1], far_recv.at[oc, 1], left)
        if kind == NEAR_R:
            return rcopy(kind, oc, total.at[oc, c_right, 1], fin_recv.at[oc, 0, 1], right)
        if kind == NEAR_L:
            return rcopy(kind, oc, total.at[oc, c_left, 0], fin_recv.at[oc, 1, 0], left)
        if kind == MIX_R:
            return rcopy(kind, oc, total.at[oc, c_right, 0], fin_recv.at[oc, 0, 0], right)
        return rcopy(kind, oc, total.at[oc, c_left, 1], fin_recv.at[oc, 1, 1], left)

    rows = chips * tokens
    half = OUT_COLS // 2

    def partial_of(rail, t, obuf, dst):
        at = pl.multiple_of(rail * rows + t * tokens, tokens)
        val = jnp.dot(mix[0, pl.ds(at, tokens), :], obuf[...], preferred_element_type=F32)
        val += jnp.dot(mix[1, pl.ds(at, tokens), :], obuf[...], preferred_element_type=F32)
        val += jnp.dot(mix[2, pl.ds(at, tokens), :], obuf[...], preferred_element_type=F32)
        for h in range(2):
            dst[t, h] = val[:, h * half:(h + 1) * half]

    def finish_far(oc):
        rcopy(FAR_R, oc, far_recv.at[oc], far_recv.at[oc], buddy).wait_recv()
        total[oc, c_right, 0] = total[oc, c_right, 0] + far_recv[oc, 0]
        r_copy(MIX_R, oc).start()
        total[oc, c_left, 1] = total[oc, c_left, 1] + far_recv[oc, 1]
        r_copy(MIX_L, oc).start()

    per_in = kc_n // OUT_COLS

    def finish(oc):
        rcopy(NEAR_R, oc, fin_recv.at[oc], fin_recv.at[oc], buddy).wait_recv()
        for h in range(2):
            at = pl.multiple_of(lax.rem(oc, per_in) * OUT_COLS + h * half, half)
            x_own = x_all[oc // per_in, pl.ds(pl.multiple_of(me * tokens, tokens), tokens), pl.ds(at, half)]
            val = total[oc, chip, h] + fin_recv[oc, 0, h] + fin_recv[oc, 1, h]
            to = pl.multiple_of(oc * OUT_COLS + h * half, half)
            out_ref[:, pl.ds(to, half)] = (x_own.astype(F32) + val).astype(BF16)

    def down_one(oc, e, obuf):
        val = jnp.dot(hid[e], wout_buf[lax.rem(oc, OUT_DEPTH), e], preferred_element_type=F32)
        obuf[e * capacity:(e + 1) * capacity, :] = val.astype(BF16)

    def down(oc, obuf):
        for e in range(local_e):
            down_one(oc, e, obuf)

    def refill(oc):
        for e in range(local_e):
            wout_copy(e, oc).start()

    def part_sent(oc):
        sent = part_send.at[lax.rem(oc, 2)]
        rcopy(PART, oc, sent, sent, buddy).wait_send()

    def part_rest(oc):
        for t in (c_right, c_left, chip):
            rcopy(PART_REST, oc, part_send.at[lax.rem(oc, 2), t], part_recv.at[oc, t], buddy).start()

    def far_rows(oc, now):
        partial_of(other, c_far, now, part_send.at[lax.rem(oc, 2)])
        partial_of(core, c_far, now, total.at[oc])

    def step(oc, now, nxt, first=False):
        near = (c_right, c_left, chip)
        slot = lax.rem(oc, 2)
        if not first:
            @pl.when(oc >= 2)
            def _():
                part_sent(oc - 2)

        with jax.named_scope("partF"):
            if not first:
                alone(lambda: far_rows(oc, now))
            r_copy(PART, oc).start()
            if first:
                refill(OUT_DEPTH)
        with jax.named_scope("partA"):
            @alone
            def _():
                for t in near:
                    partial_of(other, t, now, part_send.at[slot])
            part_rest(oc)
        with jax.named_scope("part_wait"):
            r_copy(PART, oc).wait_recv()
        total[oc, c_far] = total[oc, c_far] + part_recv[oc, c_far]
        for kind in (FAR_R, FAR_L):
            r_copy(kind, oc).start()
        if not first:
            with jax.named_scope("far"):
                finish_far(oc - 1)
        if nxt is not None:
            wout_wait(oc + 1)
        with jax.named_scope("partB"):
            @alone
            def _():
                for t in near:
                    partial_of(core, t, now, total.at[oc])
                if nxt is not None:
                    down(oc + 1, nxt)
        with jax.named_scope("rest_wait"):
            rest = part_recv.at[oc, pl.ds(0, chips - 1)]
            rcopy(PART_REST, oc, rest, rest, buddy).wait_recv()
        for t in near:
            total[oc, t] = total[oc, t] + part_recv[oc, t]
        for kind in (NEAR_R, NEAR_L):
            r_copy(kind, oc).start()
        if nxt is not None:
            @pl.when(oc + 1 + OUT_DEPTH < oc_n)
            def _():
                refill(oc + 1 + OUT_DEPTH)
        if not first:
            @pl.when(oc >= LAG)
            def _():
                with jax.named_scope("fin"):
                    finish(oc - LAG)

    with jax.named_scope("up_last"):
        win_wait(last)
        wout_wait(0)

        @alone
        def _():
            gather(last)
            for e in range(local_e):
                up = acc[e] + jnp.dot(xg[e], win_buf[last % IN_DEPTH, e], preferred_element_type=F32)
                hid[e] = gelu(up).astype(BF16)
                if e >= BEHIND:
                    down_one(0, e - BEHIND, obuf0)
            for e in range(local_e - BEHIND, local_e):
                down_one(0, e, obuf0)
            far_rows(0, obuf0)

    step(0, obuf0, obuf1, True)

    @pl.loop(0, oc_n // 2 - 1)
    def _(i):
        step(2 * i + 1, obuf1, obuf0)
        step(2 * i + 2, obuf0, obuf1)

    step(oc_n - 1, obuf1, None)

    d_flush()
    for c in meta_all():
        c.wait_send()

    with jax.named_scope("far_t"):
        finish_far(oc_n - 1)
    for oc in range(oc_n - LAG, oc_n):
        with jax.named_scope("fin_t"):
            finish(oc)

    with jax.named_scope("drain"):
        part_sent(oc_n - 2)
        part_sent(oc_n - 1)
        sent = total.at[:, pl.ds(0, 3)]
        rcopy(FAR_R, 0, sent, sent, buddy).wait_send()


def solution(mesh):
    n = mesh.shape[AXIS]
    row_spec = P(("data", AXIS), None)
    weight_spec = P(AXIS, None, None)

    def device_step(token_rows, expert_ids, gate_weights, w_in, w_out):
        tokens, top_k = expert_ids.shape
        local_e, model, hidden = w_in.shape
        capacity = n * tokens * top_k // (n * local_e)
        slots = local_e * capacity
        chips = n // 2
        kc_n = model // IN_BLOCKS
        oc_n = model // OUT_COLS
        half = OUT_COLS // 2
        hbm = pl.BlockSpec(memory_space=pl.ANY)
        dma = pltpu.SemaphoreType.DMA
        return pl.pallas_call(
            functools.partial(body, n, capacity),
            out_shape=pltpu.VMEM((tokens, model), BF16),
            in_specs=[hbm, hbm, hbm, hbm, hbm],
            out_specs=pl.BlockSpec(memory_space=pltpu.VMEM),
            scratch_shapes=[
                pltpu.VMEM((n, top_k, tokens), jnp.int32),
                pltpu.VMEM((n, top_k, tokens), F32),
                pltpu.VMEM((IN_BLOCKS, n * tokens, kc_n), BF16),
                pltpu.VMEM((n * tokens // PICK_COLS, slots, PICK_COLS), BF16),
                pltpu.VMEM((n, 4 * local_e, tokens), F32),
                pltpu.VMEM((3, n * tokens, slots), BF16),
                pltpu.VMEM((local_e, capacity, kc_n), BF16),
                pltpu.VMEM((local_e, capacity, hidden), F32),
                pltpu.VMEM((local_e, capacity, hidden), BF16),
                pltpu.VMEM((LANES, 4 * slots), BF16),
                pltpu.VMEM((slots, OUT_COLS), BF16),
                pltpu.VMEM((slots, OUT_COLS), BF16),
                pltpu.VMEM((2, chips, 2, tokens, half), F32),
                pltpu.VMEM((oc_n, chips, 2, tokens, half), F32),
                pltpu.VMEM((oc_n, chips, 2, tokens, half), F32),
                pltpu.VMEM((oc_n, 2, tokens, half), F32),
                pltpu.VMEM((oc_n, 2, 2, tokens, half), F32),
                pltpu.VMEM((IN_DEPTH, local_e, kc_n, hidden), BF16),
                pltpu.VMEM((OUT_DEPTH, local_e, hidden, OUT_COLS), BF16),
                dma((2,)), dma((2,)),
                dma, dma((3, IN_BLOCKS)),
                dma((3,)), dma((2, oc_n)), dma((2, 2)),
                dma,
                dma((IN_DEPTH,)),
                dma((OUT_DEPTH,)),
                dma((2,)),
            ],
            compiler_params=pltpu.CompilerParams(
                collective_id=0, has_side_effects=True, vmem_limit_bytes=VMEM_BYTES),
        )(expert_ids.T, gate_weights.T, token_rows, w_in, w_out)

    return jax.shard_map(device_step, mesh=mesh, in_specs=(row_spec, row_spec, row_spec, weight_spec, weight_spec),
                         out_specs=row_spec, check_vma=False)
```
